256 devices in a mesh: row: 8 (over z), col: 32 (over x, y, core).
Axes of the slice: x: 4, y: 4, z: 8, core: 2. Of those that a mesh axis runs over, the one named last changes fastest.
Arguments:
- rhs: float32 [64, 131072], P(None, ('row', 'col')), may hold values from -6 to 6
- pivots: int32 [4096], replicated, may hold values from 0 to 131071, as said below
- factor: float32 [4096, 1, 32, 128], P('row', None, 'col'), as said below
- diag_inv: float32 [8, 512, 512], P('row'), as said below
Outputs:
- solution: float32 [64, 1, 32, 128], P(None, None, 'col')
The draws below stay inside these ranges and needn't reach their ends.
Inputs may be any that keep to these rules, and one draw needn't show every extreme that they name: `pivots`: distinct column numbers, the first 4096 entries of a permutation of 0 .. 131071. `factor`: entry (row i, column q) is zero where q >= 512 * (i // 512). `diag_inv`: each block is unit lower triangular.
All inputs are finite; a program needn't handle non-finite values.
Results may differ from the reference program's by a relative error of at most 0.0001.
Values sent between devices are 32-bit elements; how exact they have to be, the bound alone decides.
A program may use at most 64 MiB of HBM per device.

```python
import math
import jax
import jax.numpy as jnp
from jax import lax

N = 131072
BLK = 512
CB = 128
NRHS = 64
NB = 8
N_COL = 32


def draw_pivots(key, part):
    order = jax.random.permutation(jax.random.fold_in(key, 11), N)
    return order[:NB * BLK].astype(jnp.int32)


def draw_factor(key, part):
    width = NB * BLK
    rounds = NB * (BLK // CB) // N_COL
    shape = (width, rounds, N_COL, CB)
    row_block = lax.broadcasted_iota(jnp.int32, shape, 0) // BLK
    column = (lax.broadcasted_iota(jnp.int32, shape, 1) * N_COL + lax.broadcasted_iota(jnp.int32, shape, 2)) * CB + lax.broadcasted_iota(jnp.int32, shape, 3)
    col_block = column // BLK
    subkey = jax.random.fold_in(key, 23)
    values = jax.random.normal(subkey, shape, jnp.float32)
    values = values * (0.6 / math.sqrt(width))
    return jnp.where(col_block < row_block, values, 0.0).astype(jnp.float32)


def draw_diag_inv(key, part):
    shape = (NB, BLK, BLK)
    inner = lax.broadcasted_iota(jnp.int32, shape, 1)
    outer = lax.broadcasted_iota(jnp.int32, shape, 2)
    subkey = jax.random.fold_in(key, 37)
    values = jax.random.normal(subkey, shape, jnp.float32)
    values = values * (0.5 / math.sqrt(BLK))
    lower_part = jnp.where(outer < inner, values, 0.0)
    return (lower_part + jnp.where(outer == inner, 1.0, 0.0)).astype(jnp.float32)


def shard_levels(key, shape, cuts, smallest, largest):
    def one(axis_at, shards_of):
        draws = jax.random.uniform(jax.random.fold_in(jax.random.fold_in(key, 6), axis_at), (shards_of,), jnp.float32, smallest / len(cuts), largest / len(cuts))
        return jnp.repeat(jnp.exp(draws), shape[axis_at] // shards_of).reshape((-1,) + (1,) * (len(shape) - axis_at - 1))

    loudness = one(*cuts[0])
    for cut in cuts[1:]:
        loudness = loudness * one(*cut)
    return loudness


def gaussian(own_key, dims, scale, bound, cuts=(), dtype=jnp.bfloat16):
    loudness = shard_levels(own_key, dims, cuts, -0.22, 0.18) if cuts else 1.0
    drawn = jax.random.normal(own_key, dims, jnp.float32) * scale * loudness
    return jnp.minimum(jnp.maximum(drawn, -bound), bound).astype(dtype)


def setup_inputs(seed: int = 0) -> dict:
    key_list = jax.random.split(jax.random.key(seed), 5)
    rhs = gaussian(key_list[0], (NRHS, N), 1.0, 6.0, ((1, 256),), jnp.float32)
    pivots = draw_pivots(jax.random.fold_in(key_list[4], 71), 0)
    factor = draw_factor(jax.random.fold_in(key_list[4], 71), 0)
    diag_inv = draw_diag_inv(jax.random.fold_in(key_list[4], 71), 0)
    return dict(rhs=rhs, pivots=pivots, factor=factor, diag_inv=diag_inv)


def reference(rhs, pivots, factor, diag_inv):
    width = NB * BLK
    permuted = jnp.take(rhs, pivots, axis=1)
    full_lower = factor.reshape(width, width)

    def advance(number, solved):
        offset = (number * BLK).astype(jnp.int32)
        block_rows = lax.dynamic_slice_in_dim(full_lower, offset, BLK, 0)
        summed = lax.dot_general(solved, block_rows, (((1,), (1,)), ((), ())), precision=lax.Precision.HIGHEST, preferred_element_type=jnp.float32)
        own_rhs = lax.dynamic_slice_in_dim(permuted, offset, BLK, 1)
        block_inv = lax.dynamic_index_in_dim(diag_inv, number.astype(jnp.int32), 0, keepdims=False)
        fresh = lax.dot_general(own_rhs - summed, block_inv, (((1,), (1,)), ((), ())), precision=lax.Precision.HIGHEST, preferred_element_type=jnp.float32)
        return lax.dynamic_update_slice_in_dim(solved, fresh, offset, 1)

    solved = lax.fori_loop(jnp.int32(0), jnp.int32(NB), advance, jnp.zeros((NRHS, width), jnp.float32))
    return solved.reshape(NRHS, NB * (BLK // CB) // N_COL, N_COL, CB)
```

```python
import functools

import jax
import jax.numpy as jnp
from jax import lax
from jax.experimental import pallas as pl
from jax.experimental.pallas import tpu as pltpu
from jax.sharding import PartitionSpec as P

MESH = pl.DeviceIdType.MESH
NX, NY = 4, 4
CHIPS = NX * NY
COLS = 2 * CHIPS
ROWS = 8
BLK = 512
CB = 128
NRHS = 64
G = NRHS // CHIPS
CHAIN, GATHER = 1, 0
BF16, F32 = jnp.bfloat16, jnp.float32


def split(v):
    hi = v.astype(BF16)
    lo = (v - hi.astype(F32)).astype(BF16)
    return hi, lo


def packed(v):
    return jnp.concatenate([v[:, : BLK // 2], v[:, BLK // 2 :]], axis=0)


def unpacked(v):
    return jnp.concatenate([v[:G], v[G:]], axis=1)


def times_t(v, hi_ref, lo_ref):
    hi, lo = split(v)
    lhs = jnp.concatenate([hi.astype(F32), lo.astype(F32)], axis=0).astype(BF16)
    dims = (((1,), (1,)), ((), ()))
    o = lax.dot_general(lhs, hi_ref[...], dims, preferred_element_type=F32)
    o = o + lax.dot_general(lhs, lo_ref[...], dims, preferred_element_type=F32)
    return o[:G] + o[G:]


def kernel(
    rhs_ref, piv_ref, l_ref, d_ref, out_ref,
    s1_send, s1_recv, s2_send, s2_recv, e2, x2, ybuf, acc, pbuf, orecv, lall, bhi, blo, dhi, dlo,
    s1_ssem, s1_rsem, s2_ssem, s2_rsem, y_ssem, y_rsem, o_ssem, o_rsem, g_ssem, g_rsem, b_ssem,
):
    row = lax.axis_index("row")
    col = lax.axis_index("col")
    chip, core = col // 2, col % 2
    x, y = chip // NY, chip % NY
    is_chain = core == CHAIN
    is_gather = core == GATHER

    def chain_col(c):
        return 2 * c + CHAIN

    def remote(src, dst, ssem, rsem, dev):
        return pltpu.make_async_remote_copy(
            src_ref=src, dst_ref=dst, send_sem=ssem, recv_sem=rsem, device_id=dev, device_id_type=MESH
        )

    barrier = pltpu.get_barrier_semaphore()

    def greet_plane(i, _):
        pl.semaphore_signal(barrier, inc=1, device_id=(row, lax.rem(col + i, COLS)), device_id_type=MESH)
        return 0

    def greet_z(i, _):
        pl.semaphore_signal(barrier, inc=1, device_id=(lax.rem(row + i, ROWS), col), device_id_type=MESH)
        return 0

    lax.fori_loop(1, COLS, greet_plane, 0)

    @pl.when(is_chain)
    def _():
        lax.fori_loop(1, ROWS, greet_z, 0)

    for c in range(CHIPS):
        for q in range(4):
            s1_send[c, G * q : G * q + G, :] = rhs_ref[G * c : G * c + G, CB * q : CB * q + CB]

    @pl.when(is_chain)
    def _():
        pl.semaphore_wait(barrier, COLS - 1 + ROWS - 1)

    @pl.when(is_gather)
    def _():
        pl.semaphore_wait(barrier, COLS - 1)

    def send_s1(i, _):
        c = lax.rem(chip + i, CHIPS)
        remote(s1_send.at[c], s1_recv.at[col], s1_ssem, s1_rsem, (row, chain_col(c))).start()
        return 0

    @pl.when(is_gather)
    def _():
        lax.fori_loop(0, CHIPS, send_s1, 0)

    @pl.when(is_chain)
    def _():
        s1_recv[col] = s1_send[chip]
        lax.fori_loop(1, CHIPS, send_s1, 0)

    me_chain = (row, chain_col(chip))

    def flow_cols(f, du, dv):
        dx, dy = (du, dv) if f == 0 else (dv, du)
        return lax.rem(x + dx, NX) * NY + lax.rem(y + dy, NY)

    def gather_plan(f):
        up, un, vp, vn = (1, 0), (3, 0), (0, 1), (0, 3)
        own = [(up, True), (un, True), (vp, True), (vn, False)]
        return [
            ((0, 0), own),
            ((1, 0), [(up, True), (vp, True), (vn, False)]),
            ((3, 0), [(vn, True), (vp, False)]),
            ((0, 1), [(vp, False)]),
            ((2, 0), [(vn, True), (vp, False)]),
            ((1, 1), [(vp, False)]),
            ((3, 3), [(vn, False)]),
            ((2, 3), [(vn, False)]),
        ]

    def gather_events(do):
        plans = [gather_plan(0), gather_plan(1)]
        n = 0
        for e in range(len(plans[0])):
            for f in (0, 1):
                (su, sv), sends = plans[f][e]
                src_chip = flow_cols(f, (4 - su) % 4, (4 - sv) % 4)
                live = src_chip < 2 * row
                do(f, e, src_chip, live, sends, n)
                n += 1 + len(sends)

    def copies_of(f, e, src_chip, sends, n):
        src = l_ref if (f == GATHER and e == 0) else lall.at[src_chip, f]
        out = []
        for k, ((du, dv), to_gather) in enumerate(sends):
            dest = flow_cols(f, du, dv) * 2 + (GATHER if to_gather else CHAIN)
            out.append(remote(src, lall.at[src_chip, f], g_ssem.at[n + k], g_rsem.at[src_chip, f], (row, dest)))
        out.append(remote(src, lall.at[src_chip, f], g_ssem.at[n + len(sends)], g_rsem.at[src_chip, f], me_chain))
        return out

    def l_piece_wait(a, f):
        remote(lall.at[a, f], lall.at[a, f], b_ssem, g_rsem.at[a, f], me_chain).wait_recv()

    @pl.when(is_gather)
    def _():
        def do(f, e, src_chip, live, sends, n):
            @pl.when(live)
            def _():
                if not (f == GATHER and e == 0):
                    l_piece_wait(src_chip, f)
                for c in copies_of(f, e, src_chip, sends, n):
                    c.start()

        gather_events(do)

        def done(f, e, src_chip, live, sends, n):
            @pl.when(live)
            def _():
                for c in copies_of(f, e, src_chip, sends, n):
                    c.wait_send()

        gather_events(done)
        remote(s1_send, s1_send, s1_ssem, s1_rsem, me_chain).wait_send()
        remote(orecv, orecv, b_ssem, o_rsem, me_chain).wait_recv()

    @pl.when(is_chain)
    def _():
        partner = (row, 2 * chip + GATHER)
        own_live = chip < 2 * row

        @pl.when(own_live)
        def _():
            remote(l_ref, lall.at[chip, CHAIN], b_ssem, g_rsem.at[chip, CHAIN], partner).start()

        d = d_ref[...]
        hi, lo = split(d)
        dhi[...] = hi
        dlo[...] = lo

        width = COLS * BLK
        piv = piv_ref[...] - row * width
        low = jnp.broadcast_to(piv & (CB - 1), (CB, ROWS * BLK))
        hot = (lax.broadcasted_iota(jnp.int32, (CB, ROWS * BLK), 0) == low).astype(F32).astype(BF16)
        e2[0:CB, :] = hot
        e2[CB:, :] = hot

        remote(s1_recv.at[pl.ds(0, COLS - 1)], s1_recv.at[pl.ds(0, COLS - 1)], b_ssem, s1_rsem, partner).wait_recv()
        v = s1_recv[...].reshape(COLS * 4 * G, CB)
        hi, lo = split(v)
        x2[:, 0:CB] = hi
        x2[:, CB:] = lo

        def select(j, _):
            off = pl.multiple_of(j * BLK, BLK)
            t = jnp.dot(x2[...], e2[:, pl.ds(off, BLK)], preferred_element_type=F32)
            high = jnp.right_shift(piv_ref[:, pl.ds(off, BLK)] - row * width, 7)
            rows_hi = jnp.right_shift(lax.broadcasted_iota(jnp.int32, (COLS * 4 * G, BLK), 0), 2)
            t = jnp.where(rows_hi == jnp.broadcast_to(high, rows_hi.shape), t, 0.0)
            t = jnp.sum(t.reshape(COLS * 4 * G // 8, 8, BLK), axis=0)
            tile = packed(t[:G] + t[G:])

            @pl.when(j == row)
            def _():
                s2_recv[row] = tile

            @pl.when(j != row)
            def _():
                s2_send[j] = tile
                remote(s2_send.at[j], s2_recv.at[row], s2_ssem, s2_rsem, (j, col)).start()

            return 0

        lax.fori_loop(0, ROWS, select, 0)
        remote(s2_recv.at[pl.ds(0, ROWS - 1)], s2_recv.at[pl.ds(0, ROWS - 1)], b_ssem, s2_rsem, partner).wait_recv()
        pbuf[...] = unpacked(jnp.sum(s2_recv[...], axis=0))
        acc[...] = jnp.zeros_like(acc)

        def finish():
            fresh = times_t(pbuf[...] - acc[...], dhi, dlo)
            ybuf[row] = packed(fresh)
            for i in range(1, ROWS):
                remote(ybuf.at[row], ybuf.at[row], y_ssem, y_rsem.at[row], (lax.rem(row + i, ROWS), col)).start()

        @pl.when(row == 0)
        def _():
            finish()

        def step(m, _):
            @pl.when(m < row)
            def _():
                for t in range(4):
                    l_piece_wait(2 * m + t // 2, t % 2)
                for t in range(4):
                    hi, lo = split(lall[2 * m + t // 2, t % 2])
                    bhi[:, CB * t : CB * t + CB] = hi
                    blo[:, CB * t : CB * t + CB] = lo

            @pl.when(m != row)
            def _():
                remote(ybuf.at[m], ybuf.at[m], b_ssem, y_rsem.at[m], partner).wait_recv()

            @pl.when(m < row)
            def _():
                acc[...] += times_t(unpacked(ybuf[m]), bhi, blo)

            @pl.when(m + 1 == row)
            def _():
                finish()

            for t in range(4):
                lanes = pl.ds(CB * (t % 2), CB)
                dest = 4 * m + t

                @pl.when(dest == col)
                def _():
                    orecv[chip] = ybuf[m, :, lanes]

                @pl.when(dest != col)
                def _():
                    remote(ybuf.at[m, :, lanes], orecv.at[chip], o_ssem.at[m], o_rsem, (row, dest)).start()

            return 0

        lax.fori_loop(0, ROWS, step, 0)

        @pl.when(own_live)
        def _():
            remote(l_ref, lall.at[chip, CHAIN], b_ssem, g_rsem.at[chip, CHAIN], partner).wait_send()

        remote(s1_send.at[pl.ds(0, CHIPS - 1)], s1_send.at[pl.ds(0, CHIPS - 1)], s1_ssem, s1_rsem, partner).wait_send()
        remote(s2_send.at[pl.ds(0, ROWS - 1)], s2_send.at[pl.ds(0, ROWS - 1)], s2_ssem, s2_rsem, partner).wait_send()
        remote(ybuf.at[pl.ds(0, ROWS - 1)], ybuf.at[pl.ds(0, ROWS - 1)], y_ssem, y_rsem.at[row], partner).wait_send()

        def drain(m, _):
            @pl.when(m == col // 4)
            def _():
                remote(orecv.at[pl.ds(0, 3)], orecv.at[pl.ds(0, 3)], o_ssem.at[m], o_rsem, partner).wait_send()

            @pl.when(m != col // 4)
            def _():
                remote(orecv.at[pl.ds(0, 4)], orecv.at[pl.ds(0, 4)], o_ssem.at[m], o_rsem, partner).wait_send()

            return 0

        lax.fori_loop(0, ROWS, drain, 0)
        remote(
            orecv.at[pl.ds(0, CHIPS - 1)], orecv.at[pl.ds(0, CHIPS - 1)], b_ssem, o_rsem, partner
        ).wait_recv()

    upper = lax.rem(chip, 2) == 0
    for c in range(CHIPS):
        tile = orecv[c]
        out_ref[G * c : G * c + G, :] = jnp.where(upper, tile[:G], tile[G:])


def per_device(rhs, pivots, factor, diag_inv):
    vmem = pl.BlockSpec(memory_space=pltpu.VMEM)
    dma = pltpu.SemaphoreType.DMA
    out = pl.pallas_call(
        kernel,
        out_shape=jax.ShapeDtypeStruct((NRHS, CB), F32),
        in_specs=[vmem] * 4,
        out_specs=vmem,
        scratch_shapes=[
            pltpu.VMEM((CHIPS, 4 * G, CB), F32),
            pltpu.VMEM((COLS, 4 * G, CB), F32),
            pltpu.VMEM((ROWS, 8, BLK // 2), F32),
            pltpu.VMEM((ROWS, 8, BLK // 2), F32),
            pltpu.VMEM((2 * CB, ROWS * BLK), BF16),
            pltpu.VMEM((COLS * 4 * G, 2 * CB), BF16),
            pltpu.VMEM((ROWS, 8, BLK // 2), F32),
            pltpu.VMEM((G, BLK), F32),
            pltpu.VMEM((G, BLK), F32),
            pltpu.VMEM((CHIPS, 8, CB), F32),
            pltpu.VMEM((CHIPS, 2, BLK, CB), F32),
            pltpu.VMEM((BLK, BLK), BF16),
            pltpu.VMEM((BLK, BLK), BF16),
            pltpu.VMEM((BLK, BLK), BF16),
            pltpu.VMEM((BLK, BLK), BF16),
            dma, dma, dma, dma, dma,
            dma((ROWS,)),
            dma((ROWS,)),
            dma,
            dma((48,)),
            dma((CHIPS, 2)),
            dma,
        ],
        compiler_params=pltpu.CompilerParams(
            collective_id=0, has_side_effects=True, vmem_limit_bytes=56 * 1024 * 1024
        ),
    )(
        rhs,
        pivots.reshape(1, ROWS * BLK),
        factor.reshape(BLK, CB),
        diag_inv.reshape(BLK, BLK),
    )
    return out.reshape(NRHS, 1, 1, CB)


def solution(mesh):
    return jax.shard_map(
        per_device,
        mesh=mesh,
        in_specs=(P(None, ("row", "col")), P(), P("row", None, "col", None), P("row", None, None)),
        out_specs=P(None, None, "col", None),
        check_vma=False,
    )
```

```python
import functools

import jax
import jax.numpy as jnp
from jax import lax
from jax.experimental import pallas as pl
from jax.experimental.pallas import tpu as pltpu
from jax.sharding import PartitionSpec as P

MESH = pl.DeviceIdType.MESH
NX, NY = 4, 4
CHIPS = NX * NY
COLS = 2 * CHIPS
ROWS = 8
BLK = 512
CB = 128
NRHS = 64
G = NRHS // CHIPS
CHAIN, GATHER = 1, 0
BF16, F32 = jnp.bfloat16, jnp.float32
CHUNKS = 4
ROWS_C = BLK // CHUNKS


def split(v):
    hi = v.astype(BF16)
    lo = (v - hi.astype(F32)).astype(BF16)
    return hi, lo


def packed(v):
    return jnp.concatenate([v[:, : BLK // 2], v[:, BLK // 2 :]], axis=0)


def unpacked(v):
    return jnp.concatenate([v[:G], v[G:]], axis=1)


def times_t(v, hi_ref, lo_ref):
    hi, lo = split(v)
    lhs = jnp.concatenate([hi.astype(F32), lo.astype(F32)], axis=0).astype(BF16)
    dims = (((1,), (1,)), ((), ()))
    o = lax.dot_general(lhs, hi_ref[...], dims, preferred_element_type=F32)
    o = o + lax.dot_general(lhs, lo_ref[...], dims, preferred_element_type=F32)
    return o[:G] + o[G:]


def kernel(
    rhs_ref, piv_ref, l_ref, d_ref, out_ref,
    s1_send, s1_recv, s2_send, s2_recv, e2, xhi, xlo, ybuf, acc, pbuf, orecv, lall, bhi, blo, dhi, dlo,
    s1_ssem, s1_rsem, s2_ssem, s2_rsem, y_ssem, y_rsem, o_ssem, o_rsem, g_ssem, g_rsem, b_ssem,
):
    row = lax.axis_index("row")
    col = lax.axis_index("col")
    chip, core = col // 2, col % 2
    x, y = chip // NY, chip % NY
    is_chain = core == CHAIN
    is_gather = core == GATHER

    def chain_col(c):
        return 2 * c + CHAIN

    def remote(src, dst, ssem, rsem, dev):
        return pltpu.make_async_remote_copy(
            src_ref=src, dst_ref=dst, send_sem=ssem, recv_sem=rsem, device_id=dev, device_id_type=MESH
        )

    barrier = pltpu.get_barrier_semaphore()

    def greet_plane(i, _):
        pl.semaphore_signal(barrier, inc=1, device_id=(row, lax.rem(col + i, COLS)), device_id_type=MESH)
        return 0

    def greet_z(i, _):
        pl.semaphore_signal(barrier, inc=1, device_id=(lax.rem(row + i, ROWS), col), device_id_type=MESH)
        return 0

    lax.fori_loop(1, COLS, greet_plane, 0)

    @pl.when(is_chain)
    def _():
        lax.fori_loop(1, ROWS, greet_z, 0)

    for c in range(CHIPS):
        for q in range(4):
            at = 2 * G * (q % 2) + G * (q // 2)
            s1_send[c, at : at + G, :] = rhs_ref[G * c : G * c + G, CB * q : CB * q + CB]

    @pl.when(is_chain)
    def _():
        pl.semaphore_wait(barrier, COLS - 1 + ROWS - 1)

    @pl.when(is_gather)
    def _():
        pl.semaphore_wait(barrier, COLS - 1)

    def send_s1(i, _):
        c = lax.rem(chip + i, CHIPS)
        remote(s1_send.at[c], s1_recv.at[col], s1_ssem, s1_rsem, (row, chain_col(c))).start()
        return 0

    @pl.when(is_gather)
    def _():
        lax.fori_loop(0, CHIPS, send_s1, 0)

    @pl.when(is_chain)
    def _():
        s1_recv[col] = s1_send[chip]
        lax.fori_loop(1, CHIPS, send_s1, 0)

    me_chain = (row, chain_col(chip))

    def flow_cols(f, du, dv):
        dx, dy = (du, dv) if f == 0 else (dv, du)
        return lax.rem(x + dx, NX) * NY + lax.rem(y + dy, NY)

    up, un, vp, vn = (1, 0), (3, 0), (0, 1), (0, 3)
    relays = [
        ((1, 0), [(up, True), (vp, True), (vn, False)]),
        ((3, 0), [(vn, True), (vp, False)]),
        ((0, 1), [(vp, False)]),
        ((2, 0), [(vn, True), (vp, False)]),
        ((1, 1), [(vp, False)]),
        ((3, 3), [(vn, False)]),
        ((2, 3), [(vn, False)]),
    ]

    def block_of(f, e):
        (su, sv), _ = relays[e]
        c = flow_cols(f, (4 - su) % 4, (4 - sv) % 4)
        return 2 * c + f, c < 2 * row

    def push(src, block, c, ssem, dev):
        part = pl.ds(c * ROWS_C, ROWS_C)
        remote(src.at[part], lall.at[block, part], ssem, g_rsem.at[block, c], dev).start()

    def neighbour(f, send):
        (du, dv), to_gather = send
        return (row, flow_cols(f, du, dv) * 2 + (GATHER if to_gather else CHAIN))

    def chunk_wait(block, c):
        part = pl.ds(c * ROWS_C, ROWS_C)
        remote(lall.at[block, part], lall.at[block, part], b_ssem, g_rsem.at[block, c], me_chain).wait_recv()

    def chunks(body):
        def one(c, _):
            body(c)
            return 0

        lax.fori_loop(0, CHUNKS, one, 0)

    @pl.when(is_gather)
    def _():
        own_a, own_b = 2 * chip, 2 * chip + 1

        @pl.when(chip < 2 * row)
        def _():
            def first_a(c):
                push(l_ref, own_a, c, g_ssem.at[0], neighbour(0, (up, True)))
                push(l_ref, own_a, c, g_ssem.at[0], neighbour(0, (un, True)))

            def first_b(c):
                chunk_wait(own_b, c)
                push(lall.at[own_b], own_b, c, g_ssem.at[1], neighbour(1, (up, True)))
                push(lall.at[own_b], own_b, c, g_ssem.at[1], neighbour(1, (un, True)))

            def second(c):
                for f, src in ((0, l_ref), (1, lall.at[own_b])):
                    push(src, own_a + f, c, g_ssem.at[f], neighbour(f, (vp, True)))
                    push(src, own_a + f, c, g_ssem.at[f], neighbour(f, (vn, False)))
                    push(src, own_a + f, c, g_ssem.at[f], me_chain)

            chunks(first_a)
            chunks(first_b)
            chunks(second)

        for e in range(len(relays)):
            def relay(c):
                for f in (0, 1):
                    block, live = block_of(f, e)

                    @pl.when(live)
                    def _():
                        chunk_wait(block, c)
                        for send in relays[e][1]:
                            push(lall.at[block], block, c, g_ssem.at[2 + 2 * e + f], neighbour(f, send))
                        push(lall.at[block], block, c, g_ssem.at[2 + 2 * e + f], me_chain)

            chunks(relay)

        def sent(n, ssem):
            remote(lall.at[pl.ds(0, n)], lall.at[pl.ds(0, n)], ssem, o_rsem, me_chain).wait_send()

        @pl.when(chip < 2 * row)
        def _():
            sent(5, g_ssem.at[0])
            sent(5, g_ssem.at[1])

        for e in range(len(relays)):
            for f in (0, 1):
                block, live = block_of(f, e)

                @pl.when(live)
                def _():
                    sent(len(relays[e][1]) + 1, g_ssem.at[2 + 2 * e + f])

        remote(s1_send, s1_send, s1_ssem, s1_rsem, me_chain).wait_send()
        remote(orecv, orecv, b_ssem, o_rsem, me_chain).wait_recv()

    @pl.when(is_chain)
    def _():
        partner = (row, 2 * chip + GATHER)
        own_live = chip < 2 * row

        @pl.when(own_live)
        def _():
            chunks(lambda c: push(l_ref, 2 * chip + CHAIN, c, b_ssem, partner))

        d = d_ref[...]
        hi, lo = split(d)
        dhi[...] = hi
        dlo[...] = lo

        width = COLS * BLK
        piv = piv_ref[...] - row * width
        low = jnp.broadcast_to(piv & (2 * CB - 1), (2 * CB, ROWS * BLK))
        e2[...] = (lax.broadcasted_iota(jnp.int32, (2 * CB, ROWS * BLK), 0) == low).astype(F32).astype(BF16)

        remote(s1_recv.at[pl.ds(0, COLS - 1)], s1_recv.at[pl.ds(0, COLS - 1)], b_ssem, s1_rsem, partner).wait_recv()
        for h in range(2):
            v = s1_recv[:, 2 * G * h : 2 * G * h + 2 * G, :].reshape(COLS * 2 * G, CB)
            hi, lo = split(v)
            xhi[:, CB * h : CB * h + CB] = hi
            xlo[:, CB * h : CB * h + CB] = lo

        def select(j, _):
            off = pl.multiple_of(j * BLK, BLK)
            e = e2[:, pl.ds(off, BLK)]
            t = jnp.dot(xhi[...], e, preferred_element_type=F32)
            t = t + jnp.dot(xlo[...], e, preferred_element_type=F32)
            high = jnp.right_shift(piv_ref[:, pl.ds(off, BLK)] - row * width, 8)
            rows_hi = jnp.right_shift(lax.broadcasted_iota(jnp.int32, (COLS * 2 * G, BLK), 0), 2)
            t = jnp.where(rows_hi == jnp.broadcast_to(high, rows_hi.shape), t, 0.0)
            t = jnp.sum(t.reshape(COLS, 2 * G, BLK), axis=0)
            tile = packed(t[:G] + t[G:])

            @pl.when(j == row)
            def _():
                s2_recv[row] = tile

            @pl.when(j != row)
            def _():
                s2_send[j] = tile
                remote(s2_send.at[j], s2_recv.at[row], s2_ssem, s2_rsem, (j, col)).start()

            return 0

        lax.fori_loop(0, ROWS, select, 0)
        remote(s2_recv.at[pl.ds(0, ROWS - 1)], s2_recv.at[pl.ds(0, ROWS - 1)], b_ssem, s2_rsem, partner).wait_recv()
        pbuf[...] = unpacked(jnp.sum(s2_recv[...], axis=0))
        acc[...] = jnp.zeros_like(acc)

        def finish():
            fresh = times_t(pbuf[...] - acc[...], dhi, dlo)
            ybuf[row] = packed(fresh)
            for i in range(1, ROWS):
                remote(ybuf.at[row], ybuf.at[row], y_ssem, y_rsem.at[row], (lax.rem(row + i, ROWS), col)).start()

        @pl.when(row == 0)
        def _():
            finish()

        def step(m, _):
            @pl.when(m < row)
            def _():
                for t in range(4):
                    chunks(lambda c: chunk_wait(4 * m + t, c))
                for t in range(4):
                    hi, lo = split(lall[4 * m + t])
                    bhi[:, CB * t : CB * t + CB] = hi
                    blo[:, CB * t : CB * t + CB] = lo

            @pl.when(m != row)
            def _():
                remote(ybuf.at[m], ybuf.at[m], b_ssem, y_rsem.at[m], partner).wait_recv()

            @pl.when(m < row)
            def _():
                acc[...] += times_t(unpacked(ybuf[m]), bhi, blo)

            @pl.when(m + 1 == row)
            def _():
                finish()

            for t in range(4):
                lanes = pl.ds(CB * (t % 2), CB)
                dest = 4 * m + t

                @pl.when(dest == col)
                def _():
                    orecv[chip] = ybuf[m, :, lanes]

                @pl.when(dest != col)
                def _():
                    remote(ybuf.at[m, :, lanes], orecv.at[chip], o_ssem.at[m], o_rsem, (row, dest)).start()

            return 0

        lax.fori_loop(0, ROWS, step, 0)

        @pl.when(own_live)
        def _():
            remote(l_ref, l_ref, b_ssem, o_rsem, partner).wait_send()

        remote(s1_send.at[pl.ds(0, CHIPS - 1)], s1_send.at[pl.ds(0, CHIPS - 1)], s1_ssem, s1_rsem, partner).wait_send()
        remote(s2_send.at[pl.ds(0, ROWS - 1)], s2_send.at[pl.ds(0, ROWS - 1)], s2_ssem, s2_rsem, partner).wait_send()
        remote(ybuf.at[pl.ds(0, ROWS - 1)], ybuf.at[pl.ds(0, ROWS - 1)], y_ssem, y_rsem.at[row], partner).wait_send()

        def drain(m, _):
            @pl.when(m == col // 4)
            def _():
                remote(orecv.at[pl.ds(0, 3)], orecv.at[pl.ds(0, 3)], o_ssem.at[m], o_rsem, partner).wait_send()

            @pl.when(m != col // 4)
            def _():
                remote(orecv.at[pl.ds(0, 4)], orecv.at[pl.ds(0, 4)], o_ssem.at[m], o_rsem, partner).wait_send()

            return 0

        lax.fori_loop(0, ROWS, drain, 0)
        remote(
            orecv.at[pl.ds(0, CHIPS - 1)], orecv.at[pl.ds(0, CHIPS - 1)], b_ssem, o_rsem, partner
        ).wait_recv()

    upper = lax.rem(chip, 2) == 0
    for c in range(CHIPS):
        tile = orecv[c]
        out_ref[G * c : G * c + G, :] = jnp.where(upper, tile[:G], tile[G:])


def per_device(rhs, pivots, factor, diag_inv):
    vmem = pl.BlockSpec(memory_space=pltpu.VMEM)
    dma = pltpu.SemaphoreType.DMA
    out = pl.pallas_call(
        kernel,
        out_shape=jax.ShapeDtypeStruct((NRHS, CB), F32),
        in_specs=[vmem] * 4,
        out_specs=vmem,
        scratch_shapes=[
            pltpu.VMEM((CHIPS, 4 * G, CB), F32),
            pltpu.VMEM((COLS, 4 * G, CB), F32),
            pltpu.VMEM((ROWS, 8, BLK // 2), F32),
            pltpu.VMEM((ROWS, 8, BLK // 2), F32),
            pltpu.VMEM((2 * CB, ROWS * BLK), BF16),
            pltpu.VMEM((COLS * 2 * G, 2 * CB), BF16),
            pltpu.VMEM((COLS * 2 * G, 2 * CB), BF16),
            pltpu.VMEM((ROWS, 8, BLK // 2), F32),
            pltpu.VMEM((G, BLK), F32),
            pltpu.VMEM((G, BLK), F32),
            pltpu.VMEM((CHIPS, 8, CB), F32),
            pltpu.VMEM((COLS, BLK, CB), F32),
            pltpu.VMEM((BLK, BLK), BF16),
            pltpu.VMEM((BLK, BLK), BF16),
            pltpu.VMEM((BLK, BLK), BF16),
            pltpu.VMEM((BLK, BLK), BF16),
            dma, dma, dma, dma, dma,
            dma((ROWS,)),
            dma((ROWS,)),
            dma,
            dma((16,)),
            dma((COLS, CHUNKS)),
            dma,
        ],
        compiler_params=pltpu.CompilerParams(
            collective_id=0, has_side_effects=True, vmem_limit_bytes=56 * 1024 * 1024
        ),
    )(
        rhs,
        pivots.reshape(1, ROWS * BLK),
        factor.reshape(BLK, CB),
        diag_inv.reshape(BLK, BLK),
    )
    return out.reshape(NRHS, 1, 1, CB)


def solution(mesh):
    return jax.shard_map(
        per_device,
        mesh=mesh,
        in_specs=(P(None, ("row", "col")), P(), P("row", None, "col", None), P("row", None, None)),
        out_specs=P(None, None, "col", None),
        check_vma=False,
    )
```

```python
import functools

import jax
import jax.numpy as jnp
from jax import lax
from jax.experimental import pallas as pl
from jax.experimental.pallas import tpu as pltpu
from jax.sharding import PartitionSpec as P

MESH = pl.DeviceIdType.MESH
NX, NY = 4, 4
CHIPS = NX * NY
COLS = 2 * CHIPS
ROWS = 8
BLK = 512
CB = 128
NRHS = 64
G = NRHS // CHIPS
CHAIN, GATHER = 1, 0
BF16, F32 = jnp.bfloat16, jnp.float32
CHUNKS = 4
ROWS_C = BLK // CHUNKS
PART = BLK // CHIPS


def split(v):
    hi = v.astype(BF16)
    lo = (v - hi.astype(F32)).astype(BF16)
    return hi, lo


def packed(v):
    return jnp.concatenate([v[:, : BLK // 2], v[:, BLK // 2 :]], axis=0)


def unpacked(v):
    return jnp.concatenate([v[:G], v[G:]], axis=1)


def times_t(v, hi_ref, lo_ref):
    hi, lo = split(v)
    lhs = jnp.concatenate([hi.astype(F32), lo.astype(F32)], axis=0).astype(BF16)
    dims = (((1,), (1,)), ((), ()))
    o = lax.dot_general(lhs, hi_ref[...], dims, preferred_element_type=F32)
    o = o + lax.dot_general(lhs, lo_ref[...], dims, preferred_element_type=F32)
    return o[:G] + o[G:]


def kernel(
    rhs_hbm, piv_hbm, l_hbm, d_hbm, out_ref,
    rhs_ref, piv_ref, l_ref, d_ref, in_sem, s1_send, s1_recv, s2_send, s2_recv, e2, xhi, xlo, ybuf, acc, pbuf, orecv, lall, bhi, blo, dhi, dlo,
    s1_ssem, s1_rsem, s2_ssem, s2_rsem, y_ssem, y_rsem, o_ssem, o_rsem, g_ssem, g_rsem, b_ssem,
    sc_ssem, u_rsem, w_rsem, c_rsem, un_ssem,
):
    row = lax.axis_index("row")
    col = lax.axis_index("col")
    chip, core = col // 2, col % 2
    x, y = chip // NY, chip % NY
    is_chain = core == CHAIN
    is_gather = core == GATHER
    scattered = (row > 0) & (row <= 3)
    relaying = row > 3

    def chain_col(c):
        return 2 * c + CHAIN

    def remote(src, dst, ssem, rsem, dev):
        return pltpu.make_async_remote_copy(
            src_ref=src, dst_ref=dst, send_sem=ssem, recv_sem=rsem, device_id=dev, device_id_type=MESH
        )

    barrier = pltpu.get_barrier_semaphore()

    def greet_plane(i, _):
        pl.semaphore_signal(barrier, inc=1, device_id=(row, lax.rem(col + i, COLS)), device_id_type=MESH)
        return 0

    def greet_z(i, _):
        pl.semaphore_signal(barrier, inc=1, device_id=(lax.rem(row + i, ROWS), col), device_id_type=MESH)
        return 0

    lax.fori_loop(1, COLS, greet_plane, 0)

    @pl.when(is_chain)
    def _():
        lax.fori_loop(1, ROWS, greet_z, 0)

    load_rhs = pltpu.make_async_copy(rhs_hbm, rhs_ref, in_sem.at[0])
    load_l = pltpu.make_async_copy(l_hbm, l_ref, in_sem.at[1])
    load_piv = pltpu.make_async_copy(piv_hbm, piv_ref, in_sem.at[2])
    load_d = pltpu.make_async_copy(d_hbm, d_ref, in_sem.at[3])
    load_rhs.start()
    load_l.start()

    @pl.when(is_chain)
    def _():
        load_piv.start()
        load_d.start()

    load_rhs.wait()

    for c in range(CHIPS):
        for q in range(4):
            at = 2 * G * (q % 2) + G * (q // 2)
            s1_send[c, at : at + G, :] = rhs_ref[G * c : G * c + G, CB * q : CB * q + CB]

    load_l.wait()

    @pl.when(is_gather & scattered)
    def _():
        part = pl.ds(pl.multiple_of(chip * PART, PART), PART)
        lall[col, part] = l_ref[part]

    @pl.when(is_chain)
    def _():
        load_piv.wait()
        load_d.wait()
        pl.semaphore_wait(barrier, COLS - 1 + ROWS - 1)

    @pl.when(is_gather)
    def _():
        pl.semaphore_wait(barrier, COLS - 1)

    def send_s1(i, _):
        c = lax.rem(chip + i, CHIPS)
        remote(s1_send.at[c], s1_recv.at[col], s1_ssem, s1_rsem, (row, chain_col(c))).start()
        return 0

    @pl.when(is_gather)
    def _():
        lax.fori_loop(0, CHIPS, send_s1, 0)

    @pl.when(is_chain)
    def _():
        s1_recv[col] = s1_send[chip]
        lax.fori_loop(1, CHIPS, send_s1, 0)

    me_chain = (row, chain_col(chip))


    def flow_chip(f, du, dv):
        dx, dy = (du, dv) if f == 0 else (dv, du)
        return lax.rem(x + dx, NX) * NY + lax.rem(y + dy, NY)

    def place(f):
        return (x, y) if f == 0 else (y, x)

    by_second_only = row == 4

    def upward(f, du, dv=None):
        u, v = place(f)
        first = lax.rem(u - du + NX, NX)
        if dv is None:
            return lax.rem(first, 2) == 1
        second = lax.rem(v - dv + NY, NY)
        return lax.rem(second + jnp.where(by_second_only, 0, first), 2) == 1

    def block_of(f, du, dv):
        c = flow_chip(f, (4 - du) % 4, (4 - dv) % 4)
        return 2 * c + f, c < 2 * row

    def push(src, block, c, ssem, dev):
        part = pl.ds(c * ROWS_C, ROWS_C)
        remote(src.at[part], lall.at[block, part], ssem, g_rsem.at[block, c], dev).start()

    def neighbour(f, du, dv, relayed=True):
        role = jnp.where(relayed, GATHER, CHAIN) if not isinstance(relayed, bool) else (GATHER if relayed else CHAIN)
        return (row, flow_chip(f, du, dv) * 2 + role)

    def spread(f, du, src, block, c, ssem):
        plus = upward(f, du, 0)
        push(src, block, c, ssem, neighbour(f, 0, 1, plus))
        push(src, block, c, ssem, neighbour(f, 0, 3, jnp.logical_not(plus)))
        push(src, block, c, ssem, me_chain)

    def chunk_wait(block, c):
        part = pl.ds(c * ROWS_C, ROWS_C)
        remote(lall.at[block, part], lall.at[block, part], b_ssem, g_rsem.at[block, c], me_chain).wait_recv()

    def chunks(body):
        def one(c, _):
            body(c)
            return 0

        lax.fori_loop(0, CHUNKS, one, 0)

    def scatter(ssem):
        m, f = jnp.minimum(chip // 2, 2), lax.rem(chip, 2)

        def one(i, _):
            c = lax.rem(chip + i, CHIPS)
            part = pl.ds(pl.multiple_of(c * PART, PART), PART)
            remote(l_ref.at[part], lall.at[col, part], ssem, u_rsem.at[m, f], (row, 2 * c + GATHER)).start()
            return 0

        return one

    def unit(c, f, m):
        return lall.at[pl.ds(4 * m + 2 * f, 2), pl.ds(pl.multiple_of(c * PART, PART), PART)]

    def unit_of(f, du):
        return flow_chip(f, (4 - du) % 4, 0)

    def unit_send(c, f, m, rsem, dev):
        remote(unit(c, f, m), unit(c, f, m), un_ssem.at[m], rsem, dev).start()

    def unit_spread(c, f, m):
        for dv in (1, 3, 2):
            unit_send(c, f, m, c_rsem.at[m], (row, chain_col(flow_chip(f, 0, dv))))
        unit_send(c, f, m, c_rsem.at[m], me_chain)

    @pl.when(is_gather & scattered)
    def _():
        @pl.when(chip < 2 * row)
        def _():
            lax.fori_loop(1, CHIPS, scatter(sc_ssem), 0)

        def own_units(m, _):
            for f in (0, 1):
                ref = lall.at[pl.ds(4 * m + 2 * f, 2), pl.ds(0, PART)]
                one = lall.at[pl.ds(4 * m + 2 * f, 1), pl.ds(0, PART)]

                @pl.when(chip == 2 * m + f)
                def _():
                    remote(one, one, b_ssem, u_rsem.at[m, f], me_chain).wait_recv()

                @pl.when(chip != 2 * m + f)
                def _():
                    remote(ref, ref, b_ssem, u_rsem.at[m, f], me_chain).wait_recv()

                for du in (1, 3, 2):
                    unit_send(chip, f, m, w_rsem.at[du, m, f], (row, 2 * flow_chip(f, du, 0) + GATHER))
                unit_spread(chip, f, m)
            return 0

        def relay_units(m, _):
            for du in (1, 3, 2):
                for f in (0, 1):
                    c = unit_of(f, du)
                    remote(unit(c, f, m), unit(c, f, m), b_ssem, w_rsem.at[du, m, f], me_chain).wait_recv()
                    unit_spread(c, f, m)
            return 0

        def units_sent(m, _):
            ref = lall.at[pl.ds(0, 19), pl.ds(0, 4 * PART)]
            remote(ref, ref, un_ssem.at[m], o_rsem, me_chain).wait_send()
            return 0

        lax.fori_loop(0, row, own_units, 0)
        lax.fori_loop(0, row, relay_units, 0)
        lax.fori_loop(0, row, units_sent, 0)

        @pl.when(chip < 2 * row)
        def _():
            ref = l_ref.at[pl.ds(0, BLK - PART)]
            remote(ref, ref, sc_ssem, o_rsem, me_chain).wait_send()

    @pl.when(is_gather & relaying)
    def _():
        own_a, own_b = 2 * chip, 2 * chip + 1

        @pl.when(chip < 2 * row)
        def _():
            def first_a(c):
                push(l_ref, own_a, c, g_ssem.at[0], neighbour(0, 1, 0))
                push(l_ref, own_a, c, g_ssem.at[0], neighbour(0, 3, 0))

            def first_b(c):
                chunk_wait(own_b, c)
                push(lall.at[own_b], own_b, c, g_ssem.at[1], neighbour(1, 1, 0))
                push(lall.at[own_b], own_b, c, g_ssem.at[1], neighbour(1, 3, 0))

            def second(c):
                spread(0, 0, l_ref, own_a, c, g_ssem.at[0])
                spread(1, 0, lall.at[own_b], own_b, c, g_ssem.at[1])

            chunks(first_a)
            chunks(first_b)
            chunks(second)

        def on_first(du, c, f):
            block, live = block_of(f, du, 0)

            @pl.when(live)
            def _():
                chunk_wait(block, c)
                if du != 2:
                    onward = upward(f, du) if du == 1 else jnp.logical_not(upward(f, du))

                    @pl.when(onward)
                    def _():
                        push(lall.at[block], block, c, g_ssem.at[4 * du + 2 + f], neighbour(f, du, 0))

                spread(f, du, lall.at[block], block, c, g_ssem.at[4 * du + f])

        def second_state(f, du, dv):
            block, live = block_of(f, du, dv)
            onward = upward(f, du, dv) if dv == 1 else jnp.logical_not(upward(f, du, dv))
            return block, live & onward, 16 + 4 * du + (dv - 1) + f

        def on_second(du, dv, c, f):
            block, go, at = second_state(f, du, dv)

            @pl.when(go)
            def _():
                chunk_wait(block, c)
                push(lall.at[block], block, c, g_ssem.at[at], neighbour(f, 0, dv, False))
                push(lall.at[block], block, c, g_ssem.at[at], me_chain)

        def first_both(c):
            for f in (0, 1):
                on_first(1, c, f)
                on_first(3, c, f)

        def second_of(*dus):
            def body(c):
                for f in (0, 1):
                    for du in dus:
                        on_second(du, 1, c, f)
                        on_second(du, 3, c, f)

            return body

        def first_far(c):
            for f in (0, 1):
                on_first(2, c, f)

        chunks(first_both)
        chunks(second_of(0))
        chunks(first_far)
        chunks(second_of(1, 3))
        chunks(second_of(2))

        def sent(n, ssem):
            remote(lall.at[pl.ds(0, n)], lall.at[pl.ds(0, n)], ssem, o_rsem, me_chain).wait_send()

        for f in (0, 1):

            @pl.when(chip < 2 * row)
            def _():
                sent(5, g_ssem.at[f])

            for du in (1, 2, 3):
                block, live = block_of(f, du, 0)

                @pl.when(live)
                def _():
                    sent(3, g_ssem.at[4 * du + f])

                if du != 2:
                    onward = upward(f, du) if du == 1 else jnp.logical_not(upward(f, du))

                    @pl.when(live & onward)
                    def _():
                        sent(1, g_ssem.at[4 * du + 2 + f])

            for du in range(4):
                for dv in (1, 3):
                    _, go, at = second_state(f, du, dv)

                    @pl.when(go)
                    def _():
                        sent(2, g_ssem.at[at])

    @pl.when(is_gather)
    def _():
        remote(s1_send, s1_send, s1_ssem, s1_rsem, me_chain).wait_send()
        remote(orecv, orecv, b_ssem, o_rsem, me_chain).wait_recv()

    @pl.when(is_chain)
    def _():
        partner = (row, 2 * chip + GATHER)
        own_live = chip < 2 * row

        @pl.when(own_live & relaying)
        def _():
            chunks(lambda c: push(l_ref, 2 * chip + CHAIN, c, b_ssem, partner))

        @pl.when(own_live & scattered)
        def _():
            lax.fori_loop(0, CHIPS, scatter(b_ssem), 0)

        d = d_ref[...]
        hi, lo = split(d)
        dhi[...] = hi
        dlo[...] = lo

        width = COLS * BLK
        piv = piv_ref[...] - row * width
        low = jnp.broadcast_to(piv & (2 * CB - 1), (2 * CB, ROWS * BLK))
        e2[...] = (lax.broadcasted_iota(jnp.int32, (2 * CB, ROWS * BLK), 0) == low).astype(F32).astype(BF16)

        remote(s1_recv.at[pl.ds(0, COLS - 1)], s1_recv.at[pl.ds(0, COLS - 1)], b_ssem, s1_rsem, partner).wait_recv()
        for h in range(2):
            v = s1_recv[:, 2 * G * h : 2 * G * h + 2 * G, :].reshape(COLS * 2 * G, CB)
            hi, lo = split(v)
            xhi[:, CB * h : CB * h + CB] = hi
            xlo[:, CB * h : CB * h + CB] = lo

        def select(j, _):
            off = pl.multiple_of(j * BLK, BLK)
            e = e2[:, pl.ds(off, BLK)]
            t = jnp.dot(xhi[...], e, preferred_element_type=F32)
            t = t + jnp.dot(xlo[...], e, preferred_element_type=F32)
            high = jnp.right_shift(piv_ref[:, pl.ds(off, BLK)] - row * width, 8)
            rows_hi = jnp.right_shift(lax.broadcasted_iota(jnp.int32, (COLS * 2 * G, BLK), 0), 2)
            t = jnp.where(rows_hi == jnp.broadcast_to(high, rows_hi.shape), t, 0.0)
            t = jnp.sum(t.reshape(COLS, 2 * G, BLK), axis=0)
            tile = packed(t[:G] + t[G:])

            @pl.when(j == row)
            def _():
                s2_recv[row] = tile

            @pl.when(j != row)
            def _():
                s2_send[j] = tile
                remote(s2_send.at[j], s2_recv.at[row], s2_ssem, s2_rsem, (j, col)).start()

            return 0

        lax.fori_loop(0, ROWS, select, 0)
        remote(s2_recv.at[pl.ds(0, ROWS - 1)], s2_recv.at[pl.ds(0, ROWS - 1)], b_ssem, s2_rsem, partner).wait_recv()
        pbuf[...] = unpacked(jnp.sum(s2_recv[...], axis=0))
        acc[...] = jnp.zeros_like(acc)

        def finish():
            fresh = times_t(pbuf[...] - acc[...], dhi, dlo)
            ybuf[row] = packed(fresh)
            for i in range(1, ROWS):
                remote(ybuf.at[row], ybuf.at[row], y_ssem, y_rsem.at[row], (lax.rem(row + i, ROWS), col)).start()

        @pl.when(row == 0)
        def _():
            finish()

        def step(m, _):
            @pl.when(m < row)
            def _():
                @pl.when(relaying)
                def _():
                    for t in range(4):
                        chunks(lambda c: chunk_wait(4 * m + t, c))

                @pl.when(scattered)
                def _():
                    four = lall.at[pl.ds(4 * m, 4)]
                    remote(four, four, b_ssem, c_rsem.at[m], partner).wait_recv()

                for t in range(4):
                    hi, lo = split(lall[4 * m + t])
                    bhi[:, CB * t : CB * t + CB] = hi
                    blo[:, CB * t : CB * t + CB] = lo

            @pl.when(m != row)
            def _():
                remote(ybuf.at[m], ybuf.at[m], b_ssem, y_rsem.at[m], partner).wait_recv()

            @pl.when(m < row)
            def _():
                acc[...] += times_t(unpacked(ybuf[m]), bhi, blo)

            @pl.when(m + 1 == row)
            def _():
                finish()

            for t in range(4):
                lanes = pl.ds(CB * (t % 2), CB)
                dest = 4 * m + t

                @pl.when(dest == col)
                def _():
                    orecv[chip] = ybuf[m, :, lanes]

                @pl.when(dest != col)
                def _():
                    remote(ybuf.at[m, :, lanes], orecv.at[chip], o_ssem.at[m], o_rsem, (row, dest)).start()

            return 0

        lax.fori_loop(0, ROWS, step, 0)

        @pl.when(own_live)
        def _():
            remote(l_ref, l_ref, b_ssem, o_rsem, partner).wait_send()

        remote(s1_send.at[pl.ds(0, CHIPS - 1)], s1_send.at[pl.ds(0, CHIPS - 1)], s1_ssem, s1_rsem, partner).wait_send()
        remote(s2_send.at[pl.ds(0, ROWS - 1)], s2_send.at[pl.ds(0, ROWS - 1)], s2_ssem, s2_rsem, partner).wait_send()
        remote(ybuf.at[pl.ds(0, ROWS - 1)], ybuf.at[pl.ds(0, ROWS - 1)], y_ssem, y_rsem.at[row], partner).wait_send()

        def drain(m, _):
            @pl.when(m == col // 4)
            def _():
                remote(orecv.at[pl.ds(0, 3)], orecv.at[pl.ds(0, 3)], o_ssem.at[m], o_rsem, partner).wait_send()

            @pl.when(m != col // 4)
            def _():
                remote(orecv.at[pl.ds(0, 4)], orecv.at[pl.ds(0, 4)], o_ssem.at[m], o_rsem, partner).wait_send()

            return 0

        lax.fori_loop(0, ROWS, drain, 0)
        remote(
            orecv.at[pl.ds(0, CHIPS - 1)], orecv.at[pl.ds(0, CHIPS - 1)], b_ssem, o_rsem, partner
        ).wait_recv()

    upper = lax.rem(chip, 2) == 0
    for c in range(CHIPS):
        tile = orecv[c]
        out_ref[G * c : G * c + G, :] = jnp.where(upper, tile[:G], tile[G:])


def per_device(rhs, pivots, factor, diag_inv):
    hbm = pl.BlockSpec(memory_space=pltpu.HBM)
    dma = pltpu.SemaphoreType.DMA
    out = pl.pallas_call(
        kernel,
        out_shape=jax.ShapeDtypeStruct((NRHS, CB), F32),
        in_specs=[hbm] * 4,
        out_specs=pl.BlockSpec(memory_space=pltpu.VMEM),
        scratch_shapes=[
            pltpu.VMEM((NRHS, BLK), F32),
            pltpu.VMEM((1, ROWS * BLK), jnp.int32),
            pltpu.VMEM((BLK, CB), F32),
            pltpu.VMEM((BLK, BLK), F32),
            dma((4,)),
            pltpu.VMEM((CHIPS, 4 * G, CB), F32),
            pltpu.VMEM((COLS, 4 * G, CB), F32),
            pltpu.VMEM((ROWS, 8, BLK // 2), F32),
            pltpu.VMEM((ROWS, 8, BLK // 2), F32),
            pltpu.VMEM((2 * CB, ROWS * BLK), BF16),
            pltpu.VMEM((COLS * 2 * G, 2 * CB), BF16),
            pltpu.VMEM((COLS * 2 * G, 2 * CB), BF16),
            pltpu.VMEM((ROWS, 8, BLK // 2), F32),
            pltpu.VMEM((G, BLK), F32),
            pltpu.VMEM((G, BLK), F32),
            pltpu.VMEM((CHIPS, 8, CB), F32),
            pltpu.VMEM((COLS, BLK, CB), F32),
            pltpu.VMEM((BLK, BLK), BF16),
            pltpu.VMEM((BLK, BLK), BF16),
            pltpu.VMEM((BLK, BLK), BF16),
            pltpu.VMEM((BLK, BLK), BF16),
            dma, dma, dma, dma, dma,
            dma((ROWS,)),
            dma((ROWS,)),
            dma,
            dma((32,)),
            dma((COLS, CHUNKS)),
            dma,
            dma,
            dma((3, 2)),
            dma((4, 3, 2)),
            dma((3,)),
            dma((3,)),
        ],
        compiler_params=pltpu.CompilerParams(
            collective_id=0, has_side_effects=True, vmem_limit_bytes=56 * 1024 * 1024
        ),
    )(
        rhs,
        pivots.reshape(1, ROWS * BLK),
        factor.reshape(BLK, CB),
        diag_inv.reshape(BLK, BLK),
    )
    return out.reshape(NRHS, 1, 1, CB)


def solution(mesh):
    return jax.shard_map(
        per_device,
        mesh=mesh,
        in_specs=(P(None, ("row", "col")), P(), P("row", None, "col", None), P("row", None, None)),
        out_specs=P(None, None, "col", None),
        check_vma=False,
    )
```

```python
import functools

import jax
import jax.numpy as jnp
from jax import lax
from jax.experimental import pallas as pl
from jax.experimental.pallas import tpu as pltpu
from jax.sharding import PartitionSpec as P

MESH = pl.DeviceIdType.MESH
NX, NY = 4, 4
CHIPS = NX * NY
COLS = 2 * CHIPS
ROWS = 8
BLK = 512
CB = 128
NRHS = 64
G = NRHS // CHIPS
CHAIN, GATHER = 1, 0
BF16, F32 = jnp.bfloat16, jnp.float32
CHUNKS = 4
ROWS_C = BLK // CHUNKS
PART = BLK // CHIPS


def split(v):
    hi = v.astype(BF16)
    lo = (v - hi.astype(F32)).astype(BF16)
    return hi, lo


def packed(v):
    return jnp.concatenate([v[:, : BLK // 2], v[:, BLK // 2 :]], axis=0)


def unpacked(v):
    return jnp.concatenate([v[:G], v[G:]], axis=1)


def times_t(v, hi_ref, lo_ref):
    hi, lo = split(v)
    lhs = jnp.concatenate([hi.astype(F32), lo.astype(F32)], axis=0).astype(BF16)
    dims = (((1,), (1,)), ((), ()))
    o = lax.dot_general(lhs, hi_ref[...], dims, preferred_element_type=F32)
    o = o + lax.dot_general(lhs, lo_ref[...], dims, preferred_element_type=F32)
    return o[:G] + o[G:]


def kernel(
    rhs_hbm, piv_hbm, l_hbm, d_hbm, out_ref,
    rhs_ref, piv_ref, l_ref, d_ref, in_sem, s1_send, s1_recv, s2_send, s2_recv, e2, xhi, xlo, ybuf, acc, pbuf, orecv, lall, bhi, blo, dhi, dlo,
    s1_ssem, s1_rsem, s2_ssem, s2_rsem, y_ssem, y_rsem, o_ssem, o_rsem, g_ssem, g_rsem, b_ssem,
    sc_ssem, u_rsem, w_rsem, c_rsem, un_ssem,
):
    row = lax.axis_index("row")
    col = lax.axis_index("col")
    chip, core = col // 2, col % 2
    x, y = chip // NY, chip % NY
    is_chain = core == CHAIN
    is_gather = core == GATHER
    scattered = (row > 0) & (row <= 3)
    relaying = row > 3

    def chain_col(c):
        return 2 * c + CHAIN

    def remote(src, dst, ssem, rsem, dev):
        return pltpu.make_async_remote_copy(
            src_ref=src, dst_ref=dst, send_sem=ssem, recv_sem=rsem, device_id=dev, device_id_type=MESH
        )

    barrier = pltpu.get_barrier_semaphore()

    def greet_plane(i, _):
        pl.semaphore_signal(barrier, inc=1, device_id=(row, lax.rem(col + i, COLS)), device_id_type=MESH)
        return 0

    def greet_z(i, _):
        pl.semaphore_signal(barrier, inc=1, device_id=(lax.rem(row + i, ROWS), col), device_id_type=MESH)
        return 0

    lax.fori_loop(1, COLS, greet_plane, 0)

    @pl.when(is_chain)
    def _():
        lax.fori_loop(1, ROWS, greet_z, 0)

    load_rhs = pltpu.make_async_copy(rhs_hbm, rhs_ref, in_sem.at[0])
    load_l = pltpu.make_async_copy(l_hbm, l_ref, in_sem.at[1])
    load_piv = pltpu.make_async_copy(piv_hbm, piv_ref, in_sem.at[2])
    load_d = pltpu.make_async_copy(d_hbm, d_ref, in_sem.at[3])
    load_rhs.start()
    load_l.start()

    @pl.when(is_chain)
    def _():
        load_piv.start()
        load_d.start()

    load_rhs.wait()

    for c in range(CHIPS):
        for q in range(4):
            at = 2 * G * (q % 2) + G * (q // 2)
            s1_send[c, at : at + G, :] = rhs_ref[G * c : G * c + G, CB * q : CB * q + CB]

    load_l.wait()

    @pl.when(is_gather & scattered)
    def _():
        part = pl.ds(pl.multiple_of(chip * PART, PART), PART)
        lall[col, part] = l_ref[part]

    @pl.when(is_chain)
    def _():
        load_piv.wait()
        load_d.wait()
        pl.semaphore_wait(barrier, COLS - 1 + ROWS - 1)

    @pl.when(is_gather)
    def _():
        pl.semaphore_wait(barrier, COLS - 1)

    def scatter(ssem):
        m, f = jnp.minimum(chip // 2, 2), lax.rem(chip, 2)

        def one(i, _):
            c = lax.rem(chip + i, CHIPS)
            part = pl.ds(pl.multiple_of(c * PART, PART), PART)
            remote(l_ref.at[part], lall.at[col, part], ssem, u_rsem.at[m, f], (row, 2 * c + GATHER)).start()
            return 0

        return one

    own_live = chip < 2 * row

    @pl.when(own_live & scattered & is_gather)
    def _():
        lax.fori_loop(1, CHIPS, scatter(sc_ssem), 0)

    @pl.when(own_live & scattered & is_chain)
    def _():
        lax.fori_loop(0, CHIPS, scatter(b_ssem), 0)

    def send_s1(i, _):
        c = lax.rem(chip + i, CHIPS)
        remote(s1_send.at[c], s1_recv.at[col], s1_ssem, s1_rsem, (row, chain_col(c))).start()
        return 0

    @pl.when(is_gather)
    def _():
        lax.fori_loop(0, CHIPS, send_s1, 0)

    @pl.when(is_chain)
    def _():
        s1_recv[col] = s1_send[chip]
        lax.fori_loop(1, CHIPS, send_s1, 0)

    me_chain = (row, chain_col(chip))


    def flow_chip(f, du, dv):
        dx, dy = (du, dv) if f == 0 else (dv, du)
        return lax.rem(x + dx, NX) * NY + lax.rem(y + dy, NY)

    def place(f):
        return (x, y) if f == 0 else (y, x)

    by_chunk = row > 4

    def upward(f, c, du, dv=None):
        u, v = place(f)
        first = lax.rem(u - du + NX, NX)
        if dv is None:
            return lax.rem(first + jnp.where(by_chunk, c, 0), 2) == 1
        second = lax.rem(v - dv + NY, NY)
        return lax.rem(second + jnp.where(by_chunk, c + first, 0), 2) == 1

    def block_of(f, du, dv):
        c = flow_chip(f, (4 - du) % 4, (4 - dv) % 4)
        return 2 * c + f, c < 2 * row

    def push(src, block, c, ssem, dev):
        part = pl.ds(c * ROWS_C, ROWS_C)
        remote(src.at[part], lall.at[block, part], ssem, g_rsem.at[block, c], dev).start()

    def neighbour(f, du, dv, relayed=True):
        role = jnp.where(relayed, GATHER, CHAIN) if not isinstance(relayed, bool) else (GATHER if relayed else CHAIN)
        return (row, flow_chip(f, du, dv) * 2 + role)

    def spread(f, du, src, block, c, ssem):
        plus = upward(f, c, du, 0)
        push(src, block, c, ssem, neighbour(f, 0, 1, plus))
        push(src, block, c, ssem, neighbour(f, 0, 3, jnp.logical_not(plus)))
        push(src, block, c, ssem, me_chain)

    def chunk_wait(block, c):
        part = pl.ds(c * ROWS_C, ROWS_C)
        remote(lall.at[block, part], lall.at[block, part], b_ssem, g_rsem.at[block, c], me_chain).wait_recv()

    def chunks(body):
        def one(c, _):
            body(c)
            return 0

        lax.fori_loop(0, CHUNKS, one, 0)

    def unit(c, f, m):
        return lall.at[pl.ds(4 * m + 2 * f, 2), pl.ds(pl.multiple_of(c * PART, PART), PART)]

    def unit_of(f, du):
        return flow_chip(f, (4 - du) % 4, 0)

    def unit_send(c, f, m, rsem, dev):
        remote(unit(c, f, m), unit(c, f, m), un_ssem.at[m], rsem, dev).start()

    def unit_spread(c, f, m):
        for dv in (1, 3, 2):
            unit_send(c, f, m, c_rsem.at[m], (row, chain_col(flow_chip(f, 0, dv))))
        unit_send(c, f, m, c_rsem.at[m], me_chain)

    @pl.when(is_gather & scattered)
    def _():
        def own_units(m, _):
            for f in (0, 1):
                ref = lall.at[pl.ds(4 * m + 2 * f, 2), pl.ds(0, PART)]
                one = lall.at[pl.ds(4 * m + 2 * f, 1), pl.ds(0, PART)]

                @pl.when(chip == 2 * m + f)
                def _():
                    remote(one, one, b_ssem, u_rsem.at[m, f], me_chain).wait_recv()

                @pl.when(chip != 2 * m + f)
                def _():
                    remote(ref, ref, b_ssem, u_rsem.at[m, f], me_chain).wait_recv()

                for du in (1, 3, 2):
                    unit_send(chip, f, m, w_rsem.at[du, m, f], (row, 2 * flow_chip(f, du, 0) + GATHER))
                unit_spread(chip, f, m)
            return 0

        def relay_units(m, _):
            for du in (1, 3, 2):
                for f in (0, 1):
                    c = unit_of(f, du)
                    remote(unit(c, f, m), unit(c, f, m), b_ssem, w_rsem.at[du, m, f], me_chain).wait_recv()
                    unit_spread(c, f, m)
            return 0

        def units_sent(m, _):
            ref = lall.at[pl.ds(0, 19), pl.ds(0, 4 * PART)]
            remote(ref, ref, un_ssem.at[m], o_rsem, me_chain).wait_send()
            return 0

        lax.fori_loop(0, row, own_units, 0)
        lax.fori_loop(0, row, relay_units, 0)
        lax.fori_loop(0, row, units_sent, 0)

        @pl.when(chip < 2 * row)
        def _():
            ref = l_ref.at[pl.ds(0, BLK - PART)]
            remote(ref, ref, sc_ssem, o_rsem, me_chain).wait_send()

    @pl.when(is_gather & relaying)
    def _():
        own_a, own_b = 2 * chip, 2 * chip + 1

        @pl.when(chip < 2 * row)
        def _():
            def first_a(c):
                push(l_ref, own_a, c, g_ssem.at[0], neighbour(0, 1, 0))
                push(l_ref, own_a, c, g_ssem.at[0], neighbour(0, 3, 0))

            def first_b(c):
                chunk_wait(own_b, c)
                push(lall.at[own_b], own_b, c, g_ssem.at[1], neighbour(1, 1, 0))
                push(lall.at[own_b], own_b, c, g_ssem.at[1], neighbour(1, 3, 0))

            def second(c):
                spread(0, 0, l_ref, own_a, c, g_ssem.at[0])
                spread(1, 0, lall.at[own_b], own_b, c, g_ssem.at[1])

            chunks(first_a)
            chunks(first_b)
            chunks(second)

        def on_first(du, c, f):
            block, live = block_of(f, du, 0)

            @pl.when(live)
            def _():
                chunk_wait(block, c)
                if du != 2:
                    onward = upward(f, c, du) if du == 1 else jnp.logical_not(upward(f, c, du))

                    @pl.when(onward)
                    def _():
                        push(lall.at[block], block, c, g_ssem.at[4 * du + 2 + f], neighbour(f, du, 0))

                spread(f, du, lall.at[block], block, c, g_ssem.at[4 * du + f])

        def second_state(f, c, du, dv):
            block, live = block_of(f, du, dv)
            onward = upward(f, c, du, dv) if dv == 1 else jnp.logical_not(upward(f, c, du, dv))
            return block, live & onward, 16 + 4 * du + (dv - 1) + f

        def on_second(du, dv, c, f):
            block, go, at = second_state(f, c, du, dv)

            @pl.when(go)
            def _():
                chunk_wait(block, c)
                push(lall.at[block], block, c, g_ssem.at[at], neighbour(f, 0, dv, False))
                push(lall.at[block], block, c, g_ssem.at[at], me_chain)

        def first_both(c):
            for f in (0, 1):
                on_first(1, c, f)
                on_first(3, c, f)

        def second_of(*dus):
            def body(c):
                for f in (0, 1):
                    for du in dus:
                        on_second(du, 1, c, f)
                        on_second(du, 3, c, f)

            return body

        def first_far(c):
            for f in (0, 1):
                on_first(2, c, f)

        chunks(first_both)
        chunks(second_of(0))
        chunks(first_far)
        chunks(second_of(1, 3))
        chunks(second_of(2))

        def sent(n, ssem):
            remote(lall.at[pl.ds(0, n)], lall.at[pl.ds(0, n)], ssem, o_rsem, me_chain).wait_send()

        def some_sent(live, go, n, ssem):
            @pl.when(live & by_chunk)
            def _():
                ref = lall.at[pl.ds(0, n), pl.ds(0, BLK // 2)]
                remote(ref, ref, ssem, o_rsem, me_chain).wait_send()

            @pl.when(live & go & jnp.logical_not(by_chunk))
            def _():
                sent(n, ssem)

        for f in (0, 1):

            @pl.when(chip < 2 * row)
            def _():
                sent(5, g_ssem.at[f])

            for du in (1, 2, 3):
                block, live = block_of(f, du, 0)

                @pl.when(live)
                def _():
                    sent(3, g_ssem.at[4 * du + f])

                if du != 2:
                    onward = upward(f, 0, du) if du == 1 else jnp.logical_not(upward(f, 0, du))
                    some_sent(live, onward, 1, g_ssem.at[4 * du + 2 + f])

            for du in range(4):
                for dv in (1, 3):
                    live = block_of(f, du, dv)[1]
                    _, go, at = second_state(f, 0, du, dv)
                    some_sent(live, go, 2, g_ssem.at[at])

    @pl.when(is_gather)
    def _():
        remote(s1_send, s1_send, s1_ssem, s1_rsem, me_chain).wait_send()
        remote(orecv, orecv, b_ssem, o_rsem, me_chain).wait_recv()

    @pl.when(is_chain)
    def _():
        partner = (row, 2 * chip + GATHER)
        @pl.when(own_live & relaying)
        def _():
            chunks(lambda c: push(l_ref, 2 * chip + CHAIN, c, b_ssem, partner))

        d = d_ref[...]
        hi, lo = split(d)
        dhi[...] = hi
        dlo[...] = lo

        width = COLS * BLK
        piv = piv_ref[...] - row * width
        low = jnp.broadcast_to(piv & (2 * CB - 1), (2 * CB, ROWS * BLK))
        e2[...] = (lax.broadcasted_iota(jnp.int32, (2 * CB, ROWS * BLK), 0) == low).astype(F32).astype(BF16)

        remote(s1_recv.at[pl.ds(0, COLS - 1)], s1_recv.at[pl.ds(0, COLS - 1)], b_ssem, s1_rsem, partner).wait_recv()
        for h in range(2):
            v = s1_recv[:, 2 * G * h : 2 * G * h + 2 * G, :].reshape(COLS * 2 * G, CB)
            hi, lo = split(v)
            xhi[:, CB * h : CB * h + CB] = hi
            xlo[:, CB * h : CB * h + CB] = lo

        def select(j, _):
            off = pl.multiple_of(j * BLK, BLK)
            e = e2[:, pl.ds(off, BLK)]
            t = jnp.dot(xhi[...], e, preferred_element_type=F32)
            t = t + jnp.dot(xlo[...], e, preferred_element_type=F32)
            high = jnp.right_shift(piv_ref[:, pl.ds(off, BLK)] - row * width, 8)
            rows_hi = jnp.right_shift(lax.broadcasted_iota(jnp.int32, (COLS * 2 * G, BLK), 0), 2)
            t = jnp.where(rows_hi == jnp.broadcast_to(high, rows_hi.shape), t, 0.0)
            t = jnp.sum(t.reshape(COLS, 2 * G, BLK), axis=0)
            tile = packed(t[:G] + t[G:])

            @pl.when(j == row)
            def _():
                s2_recv[row] = tile

            @pl.when(j != row)
            def _():
                s2_send[j] = tile
                remote(s2_send.at[j], s2_recv.at[row], s2_ssem, s2_rsem, (j, col)).start()

            return 0

        lax.fori_loop(0, ROWS, select, 0)
        remote(s2_recv.at[pl.ds(0, ROWS - 1)], s2_recv.at[pl.ds(0, ROWS - 1)], b_ssem, s2_rsem, partner).wait_recv()
        pbuf[...] = unpacked(jnp.sum(s2_recv[...], axis=0))
        acc[...] = jnp.zeros_like(acc)

        def finish():
            fresh = times_t(pbuf[...] - acc[...], dhi, dlo)
            ybuf[row] = packed(fresh)
            for i in range(1, ROWS):
                remote(ybuf.at[row], ybuf.at[row], y_ssem, y_rsem.at[row], (lax.rem(row + i, ROWS), col)).start()

        @pl.when(row == 0)
        def _():
            finish()

        def step(m, _):
            @pl.when(m < row)
            def _():
                @pl.when(relaying)
                def _():
                    for t in range(4):
                        chunks(lambda c: chunk_wait(4 * m + t, c))

                @pl.when(scattered)
                def _():
                    four = lall.at[pl.ds(4 * m, 4)]
                    remote(four, four, b_ssem, c_rsem.at[m], partner).wait_recv()

                for t in range(4):
                    hi, lo = split(lall[4 * m + t])
                    bhi[:, CB * t : CB * t + CB] = hi
                    blo[:, CB * t : CB * t + CB] = lo

            @pl.when(m != row)
            def _():
                remote(ybuf.at[m], ybuf.at[m], b_ssem, y_rsem.at[m], partner).wait_recv()

            @pl.when(m < row)
            def _():
                acc[...] += times_t(unpacked(ybuf[m]), bhi, blo)

            @pl.when(m + 1 == row)
            def _():
                finish()

            for t in range(4):
                lanes = pl.ds(CB * (t % 2), CB)
                dest = 4 * m + t

                @pl.when(dest == col)
                def _():
                    orecv[chip] = ybuf[m, :, lanes]

                @pl.when(dest != col)
                def _():
                    remote(ybuf.at[m, :, lanes], orecv.at[chip], o_ssem.at[m], o_rsem, (row, dest)).start()

            return 0

        lax.fori_loop(0, ROWS, step, 0)

        @pl.when(own_live)
        def _():
            remote(l_ref, l_ref, b_ssem, o_rsem, partner).wait_send()

        remote(s1_send.at[pl.ds(0, CHIPS - 1)], s1_send.at[pl.ds(0, CHIPS - 1)], s1_ssem, s1_rsem, partner).wait_send()
        remote(s2_send.at[pl.ds(0, ROWS - 1)], s2_send.at[pl.ds(0, ROWS - 1)], s2_ssem, s2_rsem, partner).wait_send()
        remote(ybuf.at[pl.ds(0, ROWS - 1)], ybuf.at[pl.ds(0, ROWS - 1)], y_ssem, y_rsem.at[row], partner).wait_send()

        def drain(m, _):
            @pl.when(m == col // 4)
            def _():
                remote(orecv.at[pl.ds(0, 3)], orecv.at[pl.ds(0, 3)], o_ssem.at[m], o_rsem, partner).wait_send()

            @pl.when(m != col // 4)
            def _():
                remote(orecv.at[pl.ds(0, 4)], orecv.at[pl.ds(0, 4)], o_ssem.at[m], o_rsem, partner).wait_send()

            return 0

        lax.fori_loop(0, ROWS, drain, 0)
        remote(
            orecv.at[pl.ds(0, CHIPS - 1)], orecv.at[pl.ds(0, CHIPS - 1)], b_ssem, o_rsem, partner
        ).wait_recv()

    upper = lax.rem(chip, 2) == 0
    for c in range(CHIPS):
        tile = orecv[c]
        out_ref[G * c : G * c + G, :] = jnp.where(upper, tile[:G], tile[G:])


def per_device(rhs, pivots, factor, diag_inv):
    hbm = pl.BlockSpec(memory_space=pltpu.HBM)
    dma = pltpu.SemaphoreType.DMA
    out = pl.pallas_call(
        kernel,
        out_shape=pltpu.VMEM((NRHS, CB), F32),
        in_specs=[hbm] * 4,
        out_specs=pl.BlockSpec(memory_space=pltpu.VMEM),
        scratch_shapes=[
            pltpu.VMEM((NRHS, BLK), F32),
            pltpu.VMEM((1, ROWS * BLK), jnp.int32),
            pltpu.VMEM((BLK, CB), F32),
            pltpu.VMEM((BLK, BLK), F32),
            dma((4,)),
            pltpu.VMEM((CHIPS, 4 * G, CB), F32),
            pltpu.VMEM((COLS, 4 * G, CB), F32),
            pltpu.VMEM((ROWS, 8, BLK // 2), F32),
            pltpu.VMEM((ROWS, 8, BLK // 2), F32),
            pltpu.VMEM((2 * CB, ROWS * BLK), BF16),
            pltpu.VMEM((COLS * 2 * G, 2 * CB), BF16),
            pltpu.VMEM((COLS * 2 * G, 2 * CB), BF16),
            pltpu.VMEM((ROWS, 8, BLK // 2), F32),
            pltpu.VMEM((G, BLK), F32),
            pltpu.VMEM((G, BLK), F32),
            pltpu.VMEM((CHIPS, 8, CB), F32),
            pltpu.VMEM((COLS, BLK, CB), F32),
            pltpu.VMEM((BLK, BLK), BF16),
            pltpu.VMEM((BLK, BLK), BF16),
            pltpu.VMEM((BLK, BLK), BF16),
            pltpu.VMEM((BLK, BLK), BF16),
            dma, dma, dma, dma, dma,
            dma((ROWS,)),
            dma((ROWS,)),
            dma,
            dma((32,)),
            dma((COLS, CHUNKS)),
            dma,
            dma,
            dma((3, 2)),
            dma((4, 3, 2)),
            dma((3,)),
            dma((3,)),
        ],
        compiler_params=pltpu.CompilerParams(
            collective_id=0, has_side_effects=True, vmem_limit_bytes=55200 * 1024
        ),
    )(
        rhs,
        pivots.reshape(1, ROWS * BLK),
        factor.reshape(BLK, CB),
        diag_inv.reshape(BLK, BLK),
    )
    return out.reshape(NRHS, 1, 1, CB)


def solution(mesh):
    return jax.shard_map(
        per_device,
        mesh=mesh,
        in_specs=(P(None, ("row", "col")), P(), P("row", None, "col", None), P("row", None, None)),
        out_specs=P(None, None, "col", None),
        check_vma=False,
    )
```

```python
import functools

import jax
import jax.numpy as jnp
from jax import lax
from jax.experimental import pallas as pl
from jax.experimental.pallas import tpu as pltpu
from jax.sharding import PartitionSpec as P

MESH = pl.DeviceIdType.MESH
NX, NY = 4, 4
CHIPS = NX * NY
COLS = 2 * CHIPS
ROWS = 8
BLK = 512
CB = 128
NRHS = 64
G = NRHS // CHIPS
CHAIN, GATHER = 1, 0
BF16, F32 = jnp.bfloat16, jnp.float32
CHUNKS = 4
ROWS_C = CB // CHUNKS
PART = CB // CHIPS


def split(v):
    hi = v.astype(BF16)
    lo = (v - hi.astype(F32)).astype(BF16)
    return hi, lo


def packed(v):
    return jnp.concatenate([v[:, : BLK // 2], v[:, BLK // 2 :]], axis=0)


def unpacked(v):
    return jnp.concatenate([v[:G], v[G:]], axis=1)


def times(v, hi_ref, lo_ref):
    hi, lo = split(v)
    lhs = jnp.concatenate([hi.astype(F32), lo.astype(F32)], axis=0).astype(BF16)
    o = jnp.dot(lhs, hi_ref[...], preferred_element_type=F32)
    o = o + jnp.dot(lhs, lo_ref[...], preferred_element_type=F32)
    return o[:G] + o[G:]


def kernel(
    rhs_hbm, piv_hbm, l_hbm, d_hbm, out_ref,
    rhs_ref, piv_ref, l_in, l_ref, d_ref, in_sem, s1_send, s1_recv, s2_send, s2_recv, e2, xhi, xlo, ybuf, acc, pbuf, orecv, lall, bhi, blo, dhi, dlo,
    s1_ssem, s1_rsem, s2_ssem, s2_rsem, y_ssem, y_rsem, o_ssem, o_rsem, g_ssem, g_rsem, b_ssem,
    sc_ssem, u_rsem, w_rsem, c_rsem, un_ssem,
):
    row = lax.axis_index("row")
    col = lax.axis_index("col")
    chip, core = col // 2, col % 2
    x, y = chip // NY, chip % NY
    is_chain = core == CHAIN
    is_gather = core == GATHER
    scattered = (row > 0) & (row <= 3)
    relaying = row > 3

    def chain_col(c):
        return 2 * c + CHAIN

    def remote(src, dst, ssem, rsem, dev):
        return pltpu.make_async_remote_copy(
            src_ref=src, dst_ref=dst, send_sem=ssem, recv_sem=rsem, device_id=dev, device_id_type=MESH
        )

    barrier = pltpu.get_barrier_semaphore()

    def greet_plane(i, _):
        pl.semaphore_signal(barrier, inc=1, device_id=(row, lax.rem(col + i, COLS)), device_id_type=MESH)
        return 0

    def greet_z(i, _):
        pl.semaphore_signal(barrier, inc=1, device_id=(lax.rem(row + i, ROWS), col), device_id_type=MESH)
        return 0

    lax.fori_loop(1, COLS, greet_plane, 0)

    @pl.when(is_chain)
    def _():
        lax.fori_loop(1, ROWS, greet_z, 0)

    load_rhs = pltpu.make_async_copy(rhs_hbm, rhs_ref, in_sem.at[0])
    load_l = pltpu.make_async_copy(l_hbm, l_in, in_sem.at[1])
    load_piv = pltpu.make_async_copy(piv_hbm, piv_ref, in_sem.at[2])
    load_d = pltpu.make_async_copy(d_hbm, d_ref, in_sem.at[3])
    load_rhs.start()
    load_l.start()

    @pl.when(is_chain)
    def _():
        load_piv.start()
        load_d.start()

    load_rhs.wait()

    for c in range(CHIPS):
        for q in range(4):
            at = 2 * G * (q % 2) + G * (q // 2)
            s1_send[c, at : at + G, :] = rhs_ref[G * c : G * c + G, CB * q : CB * q + CB]

    load_l.wait()
    l_ref[...] = l_in[...].T

    @pl.when(is_gather & scattered)
    def _():
        part = pl.ds(pl.multiple_of(chip * PART, PART), PART)
        lall[col, part] = l_ref[part]

    @pl.when(is_chain)
    def _():
        load_piv.wait()
        load_d.wait()
        pl.semaphore_wait(barrier, COLS - 1 + ROWS - 1)

    @pl.when(is_gather)
    def _():
        pl.semaphore_wait(barrier, COLS - 1)

    def scatter(ssem):
        m, f = jnp.minimum(chip // 2, 2), lax.rem(chip, 2)

        def one(i, _):
            c = lax.rem(chip + i, CHIPS)
            part = pl.ds(pl.multiple_of(c * PART, PART), PART)
            remote(l_ref.at[part], lall.at[col, part], ssem, u_rsem.at[m, f], (row, 2 * c + GATHER)).start()
            return 0

        return one

    own_live = chip < 2 * row

    @pl.when(own_live & scattered & is_gather)
    def _():
        lax.fori_loop(1, CHIPS, scatter(sc_ssem), 0)

    @pl.when(own_live & scattered & is_chain)
    def _():
        lax.fori_loop(0, CHIPS, scatter(b_ssem), 0)

    def send_s1(i, _):
        c = lax.rem(chip + i, CHIPS)
        remote(s1_send.at[c], s1_recv.at[col], s1_ssem, s1_rsem, (row, chain_col(c))).start()
        return 0

    @pl.when(is_gather)
    def _():
        lax.fori_loop(0, CHIPS, send_s1, 0)

    @pl.when(is_chain)
    def _():
        s1_recv[col] = s1_send[chip]
        lax.fori_loop(1, CHIPS, send_s1, 0)

    me_chain = (row, chain_col(chip))


    def flow_chip(f, du, dv):
        dx, dy = (du, dv) if f == 0 else (dv, du)
        return lax.rem(x + dx, NX) * NY + lax.rem(y + dy, NY)

    def place(f):
        return (x, y) if f == 0 else (y, x)

    by_chunk = row > 4

    def upward(f, c, du, dv=None):
        u, v = place(f)
        first = lax.rem(u - du + NX, NX)
        if dv is None:
            return lax.rem(first + jnp.where(by_chunk, c, 0), 2) == 1
        second = lax.rem(v - dv + NY, NY)
        return lax.rem(second + jnp.where(by_chunk, c + first, 0), 2) == 1

    def block_of(f, du, dv):
        c = flow_chip(f, (4 - du) % 4, (4 - dv) % 4)
        return 2 * c + f, c < 2 * row

    def push(src, block, c, ssem, dev):
        part = pl.ds(c * ROWS_C, ROWS_C)
        remote(src.at[part], lall.at[block, part], ssem, g_rsem.at[block, c], dev).start()

    def neighbour(f, du, dv, relayed=True):
        role = jnp.where(relayed, GATHER, CHAIN) if not isinstance(relayed, bool) else (GATHER if relayed else CHAIN)
        return (row, flow_chip(f, du, dv) * 2 + role)

    def spread(f, du, src, block, c, ssem):
        plus = upward(f, c, du, 0)
        push(src, block, c, ssem, neighbour(f, 0, 1, plus))
        push(src, block, c, ssem, neighbour(f, 0, 3, jnp.logical_not(plus)))
        push(src, block, c, ssem, me_chain)

    def chunk_wait(block, c):
        part = pl.ds(c * ROWS_C, ROWS_C)
        remote(lall.at[block, part], lall.at[block, part], b_ssem, g_rsem.at[block, c], me_chain).wait_recv()

    def chunks(body):
        def one(c, _):
            body(c)
            return 0

        lax.fori_loop(0, CHUNKS, one, 0)

    def unit(c, f, m):
        return lall.at[pl.ds(4 * m + 2 * f, 2), pl.ds(pl.multiple_of(c * PART, PART), PART)]

    def unit_of(f, du):
        return flow_chip(f, (4 - du) % 4, 0)

    def unit_send(c, f, m, rsem, dev):
        remote(unit(c, f, m), unit(c, f, m), un_ssem.at[m], rsem, dev).start()

    def unit_spread(c, f, m):
        for dv in (1, 3, 2):
            unit_send(c, f, m, c_rsem.at[m], (row, chain_col(flow_chip(f, 0, dv))))
        unit_send(c, f, m, c_rsem.at[m], me_chain)

    @pl.when(is_gather & scattered)
    def _():
        def own_units(m, _):
            for f in (0, 1):
                ref = lall.at[pl.ds(4 * m + 2 * f, 2), pl.ds(0, PART)]
                one = lall.at[pl.ds(4 * m + 2 * f, 1), pl.ds(0, PART)]

                @pl.when(chip == 2 * m + f)
                def _():
                    remote(one, one, b_ssem, u_rsem.at[m, f], me_chain).wait_recv()

                @pl.when(chip != 2 * m + f)
                def _():
                    remote(ref, ref, b_ssem, u_rsem.at[m, f], me_chain).wait_recv()

                for du in (1, 3, 2):
                    unit_send(chip, f, m, w_rsem.at[du, m, f], (row, 2 * flow_chip(f, du, 0) + GATHER))
                unit_spread(chip, f, m)
            return 0

        def relay_units(m, _):
            for du in (1, 3, 2):
                for f in (0, 1):
                    c = unit_of(f, du)
                    remote(unit(c, f, m), unit(c, f, m), b_ssem, w_rsem.at[du, m, f], me_chain).wait_recv()
                    unit_spread(c, f, m)
            return 0

        def units_sent(m, _):
            ref = lall.at[pl.ds(0, 19), pl.ds(0, 4 * PART)]
            remote(ref, ref, un_ssem.at[m], o_rsem, me_chain).wait_send()
            return 0

        lax.fori_loop(0, row, own_units, 0)
        lax.fori_loop(0, row, relay_units, 0)
        lax.fori_loop(0, row, units_sent, 0)

        @pl.when(chip < 2 * row)
        def _():
            ref = l_ref.at[pl.ds(0, CB - PART)]
            remote(ref, ref, sc_ssem, o_rsem, me_chain).wait_send()

    @pl.when(is_gather & relaying)
    def _():
        own_a, own_b = 2 * chip, 2 * chip + 1

        @pl.when(chip < 2 * row)
        def _():
            def first_a(c):
                push(l_ref, own_a, c, g_ssem.at[0], neighbour(0, 1, 0))
                push(l_ref, own_a, c, g_ssem.at[0], neighbour(0, 3, 0))

            def first_b(c):
                chunk_wait(own_b, c)
                push(lall.at[own_b], own_b, c, g_ssem.at[1], neighbour(1, 1, 0))
                push(lall.at[own_b], own_b, c, g_ssem.at[1], neighbour(1, 3, 0))

            def second(c):
                spread(0, 0, l_ref, own_a, c, g_ssem.at[0])
                spread(1, 0, lall.at[own_b], own_b, c, g_ssem.at[1])

            chunks(first_a)
            chunks(first_b)
            chunks(second)

        def on_first(du, c, f):
            block, live = block_of(f, du, 0)

            @pl.when(live)
            def _():
                chunk_wait(block, c)
                if du != 2:
                    onward = upward(f, c, du) if du == 1 else jnp.logical_not(upward(f, c, du))

                    @pl.when(onward)
                    def _():
                        push(lall.at[block], block, c, g_ssem.at[4 * du + 2 + f], neighbour(f, du, 0))

                spread(f, du, lall.at[block], block, c, g_ssem.at[4 * du + f])

        def second_state(f, c, du, dv):
            block, live = block_of(f, du, dv)
            onward = upward(f, c, du, dv) if dv == 1 else jnp.logical_not(upward(f, c, du, dv))
            return block, live & onward, 16 + 4 * du + (dv - 1) + f

        def on_second(du, dv, c, f):
            block, go, at = second_state(f, c, du, dv)

            @pl.when(go)
            def _():
                chunk_wait(block, c)
                push(lall.at[block], block, c, g_ssem.at[at], neighbour(f, 0, dv, False))
                push(lall.at[block], block, c, g_ssem.at[at], me_chain)

        def first_both(c):
            for f in (0, 1):
                on_first(1, c, f)
                on_first(3, c, f)

        def second_of(*dus):
            def body(c):
                for f in (0, 1):
                    for du in dus:
                        on_second(du, 1, c, f)
                        on_second(du, 3, c, f)

            return body

        def first_far(c):
            for f in (0, 1):
                on_first(2, c, f)

        chunks(first_both)
        chunks(second_of(0))
        chunks(first_far)
        chunks(second_of(1, 3))
        chunks(second_of(2))

        def sent(n, ssem):
            remote(lall.at[pl.ds(0, n)], lall.at[pl.ds(0, n)], ssem, o_rsem, me_chain).wait_send()

        def some_sent(live, go, n, ssem):
            @pl.when(live & by_chunk)
            def _():
                ref = lall.at[pl.ds(0, n), pl.ds(0, CB // 2)]
                remote(ref, ref, ssem, o_rsem, me_chain).wait_send()

            @pl.when(live & go & jnp.logical_not(by_chunk))
            def _():
                sent(n, ssem)

        for f in (0, 1):

            @pl.when(chip < 2 * row)
            def _():
                sent(5, g_ssem.at[f])

            for du in (1, 2, 3):
                block, live = block_of(f, du, 0)

                @pl.when(live)
                def _():
                    sent(3, g_ssem.at[4 * du + f])

                if du != 2:
                    onward = upward(f, 0, du) if du == 1 else jnp.logical_not(upward(f, 0, du))
                    some_sent(live, onward, 1, g_ssem.at[4 * du + 2 + f])

            for du in range(4):
                for dv in (1, 3):
                    live = block_of(f, du, dv)[1]
                    _, go, at = second_state(f, 0, du, dv)
                    some_sent(live, go, 2, g_ssem.at[at])

    @pl.when(is_gather)
    def _():
        remote(s1_send, s1_send, s1_ssem, s1_rsem, me_chain).wait_send()
        remote(orecv, orecv, b_ssem, o_rsem, me_chain).wait_recv()

    @pl.when(is_chain)
    def _():
        partner = (row, 2 * chip + GATHER)
        @pl.when(own_live & relaying)
        def _():
            chunks(lambda c: push(l_ref, 2 * chip + CHAIN, c, b_ssem, partner))

        d = d_ref[...].T
        hi, lo = split(d)
        dhi[...] = hi
        dlo[...] = lo

        width = COLS * BLK
        piv = piv_ref[...] - row * width
        low = jnp.broadcast_to(piv & (2 * CB - 1), (2 * CB, ROWS * BLK))
        e2[...] = (lax.broadcasted_iota(jnp.int32, (2 * CB, ROWS * BLK), 0) == low).astype(F32).astype(BF16)

        remote(s1_recv.at[pl.ds(0, COLS - 1)], s1_recv.at[pl.ds(0, COLS - 1)], b_ssem, s1_rsem, partner).wait_recv()
        for h in range(2):
            v = s1_recv[:, 2 * G * h : 2 * G * h + 2 * G, :].reshape(COLS * 2 * G, CB)
            hi, lo = split(v)
            xhi[:, CB * h : CB * h + CB] = hi
            xlo[:, CB * h : CB * h + CB] = lo

        def select(j, _):
            off = pl.multiple_of(j * BLK, BLK)
            e = e2[:, pl.ds(off, BLK)]
            t = jnp.dot(xhi[...], e, preferred_element_type=F32)
            t = t + jnp.dot(xlo[...], e, preferred_element_type=F32)
            high = jnp.right_shift(piv_ref[:, pl.ds(off, BLK)] - row * width, 8)
            rows_hi = jnp.right_shift(lax.broadcasted_iota(jnp.int32, (COLS * 2 * G, BLK), 0), 2)
            t = jnp.where(rows_hi == jnp.broadcast_to(high, rows_hi.shape), t, 0.0)
            t = jnp.sum(t.reshape(COLS, 2 * G, BLK), axis=0)
            tile = packed(t[:G] + t[G:])

            @pl.when(j == row)
            def _():
                s2_recv[row] = tile

            @pl.when(j != row)
            def _():
                s2_send[j] = tile
                remote(s2_send.at[j], s2_recv.at[row], s2_ssem, s2_rsem, (j, col)).start()

            return 0

        lax.fori_loop(0, ROWS, select, 0)
        remote(s2_recv.at[pl.ds(0, ROWS - 1)], s2_recv.at[pl.ds(0, ROWS - 1)], b_ssem, s2_rsem, partner).wait_recv()
        pbuf[...] = unpacked(jnp.sum(s2_recv[...], axis=0))
        acc[...] = jnp.zeros_like(acc)

        def finish():
            fresh = times(pbuf[...] - acc[...], dhi, dlo)
            ybuf[row] = packed(fresh)
            for i in range(1, ROWS):
                remote(ybuf.at[row], ybuf.at[row], y_ssem, y_rsem.at[row], (lax.rem(row + i, ROWS), col)).start()

        @pl.when(row == 0)
        def _():
            finish()

        def step(m, _):
            @pl.when(m < row)
            def _():
                @pl.when(relaying)
                def _():
                    for t in range(4):
                        chunks(lambda c: chunk_wait(4 * m + t, c))

                @pl.when(scattered)
                def _():
                    four = lall.at[pl.ds(4 * m, 4)]
                    remote(four, four, b_ssem, c_rsem.at[m], partner).wait_recv()

                for t in range(4):
                    hi, lo = split(lall[4 * m + t])
                    bhi[CB * t : CB * t + CB, :] = hi
                    blo[CB * t : CB * t + CB, :] = lo

            @pl.when(m != row)
            def _():
                remote(ybuf.at[m], ybuf.at[m], b_ssem, y_rsem.at[m], partner).wait_recv()

            @pl.when(m < row)
            def _():
                acc[...] += times(unpacked(ybuf[m]), bhi, blo)

            @pl.when(m + 1 == row)
            def _():
                finish()

            for t in range(4):
                lanes = pl.ds(CB * (t % 2), CB)
                dest = 4 * m + t

                @pl.when(dest == col)
                def _():
                    orecv[chip] = ybuf[m, :, lanes]

                @pl.when(dest != col)
                def _():
                    remote(ybuf.at[m, :, lanes], orecv.at[chip], o_ssem.at[m], o_rsem, (row, dest)).start()

            return 0

        lax.fori_loop(0, ROWS, step, 0)

        @pl.when(own_live)
        def _():
            remote(l_ref, l_ref, b_ssem, o_rsem, partner).wait_send()

        remote(s1_send.at[pl.ds(0, CHIPS - 1)], s1_send.at[pl.ds(0, CHIPS - 1)], s1_ssem, s1_rsem, partner).wait_send()
        remote(s2_send.at[pl.ds(0, ROWS - 1)], s2_send.at[pl.ds(0, ROWS - 1)], s2_ssem, s2_rsem, partner).wait_send()
        remote(ybuf.at[pl.ds(0, ROWS - 1)], ybuf.at[pl.ds(0, ROWS - 1)], y_ssem, y_rsem.at[row], partner).wait_send()

        def drain(m, _):
            @pl.when(m == col // 4)
            def _():
                remote(orecv.at[pl.ds(0, 3)], orecv.at[pl.ds(0, 3)], o_ssem.at[m], o_rsem, partner).wait_send()

            @pl.when(m != col // 4)
            def _():
                remote(orecv.at[pl.ds(0, 4)], orecv.at[pl.ds(0, 4)], o_ssem.at[m], o_rsem, partner).wait_send()

            return 0

        lax.fori_loop(0, ROWS, drain, 0)
        remote(
            orecv.at[pl.ds(0, CHIPS - 1)], orecv.at[pl.ds(0, CHIPS - 1)], b_ssem, o_rsem, partner
        ).wait_recv()

    upper = lax.rem(chip, 2) == 0
    for c in range(CHIPS):
        tile = orecv[c]
        out_ref[G * c : G * c + G, :] = jnp.where(upper, tile[:G], tile[G:])


def per_device(rhs, pivots, factor, diag_inv):
    hbm = pl.BlockSpec(memory_space=pltpu.HBM)
    dma = pltpu.SemaphoreType.DMA
    out = pl.pallas_call(
        kernel,
        out_shape=pltpu.VMEM((NRHS, CB), F32),
        in_specs=[hbm] * 4,
        out_specs=pl.BlockSpec(memory_space=pltpu.VMEM),
        scratch_shapes=[
            pltpu.VMEM((NRHS, BLK), F32),
            pltpu.VMEM((1, ROWS * BLK), jnp.int32),
            pltpu.VMEM((BLK, CB), F32),
            pltpu.VMEM((CB, BLK), F32),
            pltpu.VMEM((BLK, BLK), F32),
            dma((4,)),
            pltpu.VMEM((CHIPS, 4 * G, CB), F32),
            pltpu.VMEM((COLS, 4 * G, CB), F32),
            pltpu.VMEM((ROWS, 8, BLK // 2), F32),
            pltpu.VMEM((ROWS, 8, BLK // 2), F32),
            pltpu.VMEM((2 * CB, ROWS * BLK), BF16),
            pltpu.VMEM((COLS * 2 * G, 2 * CB), BF16),
            pltpu.VMEM((COLS * 2 * G, 2 * CB), BF16),
            pltpu.VMEM((ROWS, 8, BLK // 2), F32),
            pltpu.VMEM((G, BLK), F32),
            pltpu.VMEM((G, BLK), F32),
            pltpu.VMEM((CHIPS, 8, CB), F32),
            pltpu.VMEM((COLS, CB, BLK), F32),
            pltpu.VMEM((BLK, BLK), BF16),
            pltpu.VMEM((BLK, BLK), BF16),
            pltpu.VMEM((BLK, BLK), BF16),
            pltpu.VMEM((BLK, BLK), BF16),
            dma, dma, dma, dma, dma,
            dma((ROWS,)),
            dma((ROWS,)),
            dma,
            dma((32,)),
            dma((COLS, CHUNKS)),
            dma,
            dma,
            dma((3, 2)),
            dma((4, 3, 2)),
            dma((3,)),
            dma((3,)),
        ],
        compiler_params=pltpu.CompilerParams(
            collective_id=0, has_side_effects=True, vmem_limit_bytes=55200 * 1024
        ),
    )(
        rhs,
        pivots.reshape(1, ROWS * BLK),
        factor.reshape(BLK, CB),
        diag_inv.reshape(BLK, BLK),
    )
    return out.reshape(NRHS, 1, 1, CB)


def solution(mesh):
    return jax.shard_map(
        per_device,
        mesh=mesh,
        in_specs=(P(None, ("row", "col")), P(), P("row", None, "col", None), P("row", None, None)),
        out_specs=P(None, None, "col", None),
        check_vma=False,
    )
```

```python
import functools

import jax
import jax.numpy as jnp
from jax import lax
from jax.experimental import pallas as pl
from jax.experimental.pallas import tpu as pltpu
from jax.sharding import PartitionSpec as P

MESH = pl.DeviceIdType.MESH
NX, NY = 4, 4
CHIPS = NX * NY
COLS = 2 * CHIPS
ROWS = 8
BLK = 512
CB = 128
NRHS = 64
G = NRHS // CHIPS
CHAIN, GATHER = 1, 0
BF16, F32 = jnp.bfloat16, jnp.float32
CHUNKS = 4
ROWS_C = CB // CHUNKS
PART = CB // CHIPS


def split(v):
    hi = v.astype(BF16)
    lo = (v - hi.astype(F32)).astype(BF16)
    return hi, lo


def packed(v):
    return jnp.concatenate([v[:, : BLK // 2], v[:, BLK // 2 :]], axis=0)


def unpacked(v):
    return jnp.concatenate([v[:G], v[G:]], axis=1)


def times(v, hi_ref, lo_ref):
    hi, lo = split(v)
    lhs = jnp.concatenate([hi.astype(F32), lo.astype(F32)], axis=0).astype(BF16)
    o = jnp.dot(lhs, hi_ref[...], preferred_element_type=F32)
    o = o + jnp.dot(lhs, lo_ref[...], preferred_element_type=F32)
    return o[:G] + o[G:]


def kernel(
    rhs_hbm, piv_hbm, l_hbm, d_hbm, out_ref,
    rhs_ref, piv_ref, l_in, l_ref, d_ref, in_sem, s1_send, s1_recv, s2_send, s2_recv, e2, xhi, xlo, ybuf, acc, pbuf, orecv, lall, bhi, blo, dhi, dlo,
    s1_ssem, s1_rsem, s2_ssem, s2_rsem, y_ssem, y_rsem, o_ssem, o_rsem, g_ssem, g_rsem, b_ssem,
    sc_ssem, u_rsem, w_rsem, c_rsem, un_ssem,
):
    row = lax.axis_index("row")
    col = lax.axis_index("col")
    chip, core = col // 2, col % 2
    x, y = chip // NY, chip % NY
    is_chain = core == CHAIN
    is_gather = core == GATHER
    scattered = (row > 0) & (row <= 3)
    relaying = row > 3

    def chain_col(c):
        return 2 * c + CHAIN

    def remote(src, dst, ssem, rsem, dev):
        return pltpu.make_async_remote_copy(
            src_ref=src, dst_ref=dst, send_sem=ssem, recv_sem=rsem, device_id=dev, device_id_type=MESH
        )

    barrier = pltpu.get_barrier_semaphore()

    def greet_plane(i, _):
        pl.semaphore_signal(barrier, inc=1, device_id=(row, lax.rem(col + i, COLS)), device_id_type=MESH)
        return 0

    def greet_z(i, _):
        pl.semaphore_signal(barrier, inc=1, device_id=(lax.rem(row + i, ROWS), col), device_id_type=MESH)
        return 0

    lax.fori_loop(1, COLS, greet_plane, 0)

    @pl.when(is_chain)
    def _():
        lax.fori_loop(1, ROWS, greet_z, 0)

    load_rhs = pltpu.make_async_copy(rhs_hbm, rhs_ref, in_sem.at[0])
    load_l = pltpu.make_async_copy(l_hbm, l_in, in_sem.at[1])
    load_piv = pltpu.make_async_copy(piv_hbm, piv_ref, in_sem.at[2])
    load_d = pltpu.make_async_copy(d_hbm, d_ref, in_sem.at[3])
    load_rhs.start()
    load_l.start()

    @pl.when(is_chain)
    def _():
        load_piv.start()
        load_d.start()

    load_rhs.wait()

    for c in range(CHIPS):
        for q in range(4):
            at = 2 * G * (q % 2) + G * (q // 2)
            s1_send[c, at : at + G, :] = rhs_ref[G * c : G * c + G, CB * q : CB * q + CB]

    load_l.wait()
    l_ref[...] = l_in[...].T

    @pl.when(is_gather & scattered)
    def _():
        part = pl.ds(pl.multiple_of(chip * PART, PART), PART)
        lall[col, part] = l_ref[part]

    @pl.when(is_chain)
    def _():
        load_piv.wait()
        load_d.wait()
        pl.semaphore_wait(barrier, COLS - 1 + ROWS - 1)

    @pl.when(is_gather)
    def _():
        pl.semaphore_wait(barrier, COLS - 1)

    def scatter(ssem):
        m, f = jnp.minimum(chip // 2, 2), lax.rem(chip, 2)

        def one(i, _):
            c = lax.rem(chip + i, CHIPS)
            part = pl.ds(pl.multiple_of(c * PART, PART), PART)
            remote(l_ref.at[part], lall.at[col, part], ssem, u_rsem.at[m, f], (row, 2 * c + GATHER)).start()
            return 0

        return one

    own_live = chip < 2 * row

    @pl.when(own_live & scattered & is_gather)
    def _():
        lax.fori_loop(1, CHIPS, scatter(sc_ssem), 0)

    @pl.when(own_live & scattered & is_chain)
    def _():
        lax.fori_loop(0, CHIPS, scatter(b_ssem), 0)

    def send_s1(i, _):
        c = lax.rem(chip + i, CHIPS)
        remote(s1_send.at[c], s1_recv.at[col], s1_ssem, s1_rsem, (row, chain_col(c))).start()
        return 0

    @pl.when(is_gather)
    def _():
        lax.fori_loop(0, CHIPS, send_s1, 0)

    @pl.when(is_chain)
    def _():
        s1_recv[col] = s1_send[chip]
        lax.fori_loop(1, CHIPS, send_s1, 0)

    me_chain = (row, chain_col(chip))


    def flow_chip(f, du, dv):
        dx, dy = (du, dv) if f == 0 else (dv, du)
        return lax.rem(x + dx, NX) * NY + lax.rem(y + dy, NY)

    def place(f):
        return (x, y) if f == 0 else (y, x)

    def upward(f, c, du, dv=None):
        u, v = place(f)
        first = lax.rem(u - du + NX, NX)
        if dv is None:
            odd = lax.rem(first + c, 2) == 1
            along_x, at_x = f == 0, first
        else:
            second = lax.rem(v - dv + NY, NY)
            odd = lax.rem(first + second + c, 2) == 1
            along_x, at_x = f == 1, second
        if not along_x:
            return odd
        uneven = (at_x == 2) | ((at_x == 1) & ((row == 4) | (c != 0)))
        return ((row >= 6) & odd) | ((row < 6) & uneven)

    def block_of(f, du, dv):
        c = flow_chip(f, (4 - du) % 4, (4 - dv) % 4)
        return 2 * c + f, c < 2 * row

    def push(src, block, c, ssem, dev):
        part = pl.ds(c * ROWS_C, ROWS_C)
        remote(src.at[part], lall.at[block, part], ssem, g_rsem.at[block, c], dev).start()

    def neighbour(f, du, dv, relayed=True):
        role = jnp.where(relayed, GATHER, CHAIN) if not isinstance(relayed, bool) else (GATHER if relayed else CHAIN)
        return (row, flow_chip(f, du, dv) * 2 + role)

    def spread(f, du, src, block, c, ssem):
        plus = upward(f, c, du, 0)
        push(src, block, c, ssem, neighbour(f, 0, 1, plus))
        push(src, block, c, ssem, neighbour(f, 0, 3, jnp.logical_not(plus)))
        push(src, block, c, ssem, me_chain)

    def chunk_wait(block, c):
        part = pl.ds(c * ROWS_C, ROWS_C)
        remote(lall.at[block, part], lall.at[block, part], b_ssem, g_rsem.at[block, c], me_chain).wait_recv()

    def chunks(body):
        def one(c, _):
            body(c)
            return 0

        lax.fori_loop(0, CHUNKS, one, 0)

    def unit(c, f, m):
        return lall.at[pl.ds(4 * m + 2 * f, 2), pl.ds(pl.multiple_of(c * PART, PART), PART)]

    def unit_of(f, du):
        return flow_chip(f, (4 - du) % 4, 0)

    def unit_send(c, f, m, rsem, dev):
        remote(unit(c, f, m), unit(c, f, m), un_ssem.at[m], rsem, dev).start()

    def unit_spread(c, f, m):
        unit_send(c, f, m, c_rsem.at[m], me_chain)
        for dv in (2, 3, 1):
            unit_send(c, f, m, c_rsem.at[m], (row, chain_col(flow_chip(f, 0, dv))))

    @pl.when(is_gather & scattered)
    def _():
        def own_units(m, _):
            for f in (0, 1):
                ref = lall.at[pl.ds(4 * m + 2 * f, 2), pl.ds(0, PART)]
                one = lall.at[pl.ds(4 * m + 2 * f, 1), pl.ds(0, PART)]

                @pl.when(chip == 2 * m + f)
                def _():
                    remote(one, one, b_ssem, u_rsem.at[m, f], me_chain).wait_recv()

                @pl.when(chip != 2 * m + f)
                def _():
                    remote(ref, ref, b_ssem, u_rsem.at[m, f], me_chain).wait_recv()

                for du in (2, 1, 3):
                    unit_send(chip, f, m, w_rsem.at[du, m, f], (row, 2 * flow_chip(f, du, 0) + GATHER))
            return 0

        def own_spread(m, _):
            for f in (0, 1):
                unit_spread(chip, f, m)
            return 0

        def relay_units(m, _):
            for du in (1, 3, 2):
                for f in (0, 1):
                    c = unit_of(f, du)
                    remote(unit(c, f, m), unit(c, f, m), b_ssem, w_rsem.at[du, m, f], me_chain).wait_recv()
                    unit_spread(c, f, m)
            return 0

        def units_sent(m, _):
            ref = lall.at[pl.ds(0, 19), pl.ds(0, 4 * PART)]
            remote(ref, ref, un_ssem.at[m], o_rsem, me_chain).wait_send()
            return 0

        lax.fori_loop(0, row, own_units, 0)
        lax.fori_loop(0, row, own_spread, 0)
        lax.fori_loop(0, row, relay_units, 0)
        lax.fori_loop(0, row, units_sent, 0)

        @pl.when(chip < 2 * row)
        def _():
            ref = l_ref.at[pl.ds(0, CB - PART)]
            remote(ref, ref, sc_ssem, o_rsem, me_chain).wait_send()

    @pl.when(is_gather & relaying)
    def _():
        own_a, own_b = 2 * chip, 2 * chip + 1

        @pl.when(chip < 2 * row)
        def _():
            def first_a(c):
                push(l_ref, own_a, c, g_ssem.at[0], neighbour(0, 1, 0))
                push(l_ref, own_a, c, g_ssem.at[0], neighbour(0, 3, 0))

            def first_b(c):
                chunk_wait(own_b, c)
                push(lall.at[own_b], own_b, c, g_ssem.at[1], neighbour(1, 1, 0))
                push(lall.at[own_b], own_b, c, g_ssem.at[1], neighbour(1, 3, 0))

            chunks(first_a)
            chunks(first_b)

        def first_onward(f, c, du):
            return upward(f, c, du) if du == 1 else jnp.logical_not(upward(f, c, du))

        def second_onward(f, c, du, dv):
            return upward(f, c, du, dv) if dv == 1 else jnp.logical_not(upward(f, c, du, dv))

        def second_sem(f, du, dv):
            return 16 + 4 * du + (dv - 1) + f

        def own_second(c):
            @pl.when(chip < 2 * row)
            def _():
                spread(0, 0, l_ref, own_a, c, g_ssem.at[0])
                spread(1, 0, lall.at[own_b], own_b, c, g_ssem.at[1])

        chunks(own_second)

        def first_arrival(du, c, f):
            block, live = block_of(f, du, 0)

            @pl.when(live)
            def _():
                chunk_wait(block, c)
                if du != 2:

                    @pl.when(first_onward(f, c, du))
                    def _():
                        push(lall.at[block], block, c, g_ssem.at[4 * du + 2 + f], neighbour(f, du, 0))

        def first_spread(du, c, f):
            block, live = block_of(f, du, 0)

            @pl.when(live)
            def _():
                spread(f, du, lall.at[block], block, c, g_ssem.at[4 * du + f])

        def on_second(du, dv, c, f):
            block, live = block_of(f, du, dv)
            at = second_sem(f, du, dv)

            @pl.when(live & second_onward(f, c, du, dv))
            def _():
                chunk_wait(block, c)
                push(lall.at[block], block, c, g_ssem.at[at], neighbour(f, 0, dv, False))
                push(lall.at[block], block, c, g_ssem.at[at], me_chain)

        def first_both(c):
            for f in (0, 1):
                first_arrival(1, c, f)
                first_arrival(3, c, f)
            for f in (0, 1):
                first_spread(1, c, f)
                first_spread(3, c, f)

        def second_of(*dus):
            def body(c):
                for f in (0, 1):
                    for du in dus:
                        on_second(du, 1, c, f)
                        on_second(du, 3, c, f)

            return body

        def first_far(c):
            for f in (0, 1):
                first_arrival(2, c, f)
                first_spread(2, c, f)

        chunks(first_both)
        chunks(second_of(0))
        chunks(first_far)
        chunks(second_of(1, 3))
        chunks(second_of(2))

        def sent(n, ssem):
            remote(lall.at[pl.ds(0, n)], lall.at[pl.ds(0, n)], ssem, o_rsem, me_chain).wait_send()

        def some_sent(live, onward, n, ssem):
            count = sum(onward(c).astype(jnp.int32) for c in range(CHUNKS))
            for k in range(1, CHUNKS + 1):

                @pl.when(live & (count == k))
                def _():
                    ref = lall.at[pl.ds(0, n), pl.ds(0, k * ROWS_C)]
                    remote(ref, ref, ssem, o_rsem, me_chain).wait_send()

        for f in (0, 1):

            @pl.when(chip < 2 * row)
            def _():
                sent(5, g_ssem.at[f])

            for du in (1, 2, 3):
                block, live = block_of(f, du, 0)

                @pl.when(live)
                def _():
                    sent(3, g_ssem.at[4 * du + f])

                if du != 2:
                    some_sent(live, lambda c: first_onward(f, c, du), 1, g_ssem.at[4 * du + 2 + f])

            for du in range(4):
                for dv in (1, 3):
                    live = block_of(f, du, dv)[1]
                    some_sent(live, lambda c: second_onward(f, c, du, dv), 2, g_ssem.at[second_sem(f, du, dv)])

    @pl.when(is_gather)
    def _():
        remote(s1_send, s1_send, s1_ssem, s1_rsem, me_chain).wait_send()
        remote(orecv, orecv, b_ssem, o_rsem, me_chain).wait_recv()

    @pl.when(is_chain)
    def _():
        partner = (row, 2 * chip + GATHER)
        @pl.when(own_live & relaying)
        def _():
            chunks(lambda c: push(l_ref, 2 * chip + CHAIN, c, b_ssem, partner))

        d = d_ref[...].T
        hi, lo = split(d)
        dhi[...] = hi
        dlo[...] = lo

        width = COLS * BLK
        piv = piv_ref[...] - row * width
        low = jnp.broadcast_to(piv & (2 * CB - 1), (2 * CB, ROWS * BLK))
        e2[...] = (lax.broadcasted_iota(jnp.int32, (2 * CB, ROWS * BLK), 0) == low).astype(F32).astype(BF16)

        remote(s1_recv.at[pl.ds(0, COLS - 1)], s1_recv.at[pl.ds(0, COLS - 1)], b_ssem, s1_rsem, partner).wait_recv()
        for h in range(2):
            v = s1_recv[:, 2 * G * h : 2 * G * h + 2 * G, :].reshape(COLS * 2 * G, CB)
            hi, lo = split(v)
            xhi[:, CB * h : CB * h + CB] = hi
            xlo[:, CB * h : CB * h + CB] = lo

        def select(j, _):
            off = pl.multiple_of(j * BLK, BLK)
            e = e2[:, pl.ds(off, BLK)]
            t = jnp.dot(xhi[...], e, preferred_element_type=F32)
            t = t + jnp.dot(xlo[...], e, preferred_element_type=F32)
            high = jnp.right_shift(piv_ref[:, pl.ds(off, BLK)] - row * width, 8)
            rows_hi = jnp.right_shift(lax.broadcasted_iota(jnp.int32, (COLS * 2 * G, BLK), 0), 2)
            t = jnp.where(rows_hi == jnp.broadcast_to(high, rows_hi.shape), t, 0.0)
            t = jnp.sum(t.reshape(COLS, 2 * G, BLK), axis=0)
            tile = packed(t[:G] + t[G:])

            @pl.when(j == row)
            def _():
                s2_recv[row] = tile

            @pl.when(j != row)
            def _():
                s2_send[j] = tile
                remote(s2_send.at[j], s2_recv.at[row], s2_ssem, s2_rsem, (j, col)).start()

            return 0

        lax.fori_loop(0, ROWS, select, 0)
        remote(s2_recv.at[pl.ds(0, ROWS - 1)], s2_recv.at[pl.ds(0, ROWS - 1)], b_ssem, s2_rsem, partner).wait_recv()
        pbuf[...] = unpacked(jnp.sum(s2_recv[...], axis=0))
        acc[...] = jnp.zeros_like(acc)

        def finish():
            fresh = times(pbuf[...] - acc[...], dhi, dlo)
            ybuf[row] = packed(fresh)
            for i in range(1, ROWS):
                remote(ybuf.at[row], ybuf.at[row], y_ssem, y_rsem.at[row], (lax.rem(row + i, ROWS), col)).start()

        @pl.when(row == 0)
        def _():
            finish()

        def step(m, _):
            @pl.when(m < row)
            def _():
                @pl.when(relaying)
                def _():
                    for t in range(4):
                        chunks(lambda c: chunk_wait(4 * m + t, c))

                @pl.when(scattered)
                def _():
                    four = lall.at[pl.ds(4 * m, 4)]
                    remote(four, four, b_ssem, c_rsem.at[m], partner).wait_recv()

                for t in range(4):
                    hi, lo = split(lall[4 * m + t])
                    bhi[CB * t : CB * t + CB, :] = hi
                    blo[CB * t : CB * t + CB, :] = lo

            @pl.when(m != row)
            def _():
                remote(ybuf.at[m], ybuf.at[m], b_ssem, y_rsem.at[m], partner).wait_recv()

            @pl.when(m < row)
            def _():
                acc[...] += times(unpacked(ybuf[m]), bhi, blo)

            @pl.when(m + 1 == row)
            def _():
                finish()

            for t in range(4):
                lanes = pl.ds(CB * (t % 2), CB)
                dest = 4 * m + t

                @pl.when(dest == col)
                def _():
                    orecv[chip] = ybuf[m, :, lanes]

                @pl.when(dest != col)
                def _():
                    remote(ybuf.at[m, :, lanes], orecv.at[chip], o_ssem.at[m], o_rsem, (row, dest)).start()

            return 0

        lax.fori_loop(0, ROWS, step, 0)

        @pl.when(own_live)
        def _():
            remote(l_ref, l_ref, b_ssem, o_rsem, partner).wait_send()

        remote(s1_send.at[pl.ds(0, CHIPS - 1)], s1_send.at[pl.ds(0, CHIPS - 1)], s1_ssem, s1_rsem, partner).wait_send()
        remote(s2_send.at[pl.ds(0, ROWS - 1)], s2_send.at[pl.ds(0, ROWS - 1)], s2_ssem, s2_rsem, partner).wait_send()
        remote(ybuf.at[pl.ds(0, ROWS - 1)], ybuf.at[pl.ds(0, ROWS - 1)], y_ssem, y_rsem.at[row], partner).wait_send()

        def drain(m, _):
            @pl.when(m == col // 4)
            def _():
                remote(orecv.at[pl.ds(0, 3)], orecv.at[pl.ds(0, 3)], o_ssem.at[m], o_rsem, partner).wait_send()

            @pl.when(m != col // 4)
            def _():
                remote(orecv.at[pl.ds(0, 4)], orecv.at[pl.ds(0, 4)], o_ssem.at[m], o_rsem, partner).wait_send()

            return 0

        lax.fori_loop(0, ROWS, drain, 0)
        remote(
            orecv.at[pl.ds(0, CHIPS - 1)], orecv.at[pl.ds(0, CHIPS - 1)], b_ssem, o_rsem, partner
        ).wait_recv()

    upper = lax.rem(chip, 2) == 0
    for c in range(CHIPS):
        tile = orecv[c]
        out_ref[G * c : G * c + G, :] = jnp.where(upper, tile[:G], tile[G:])


def per_device(rhs, pivots, factor, diag_inv):
    hbm = pl.BlockSpec(memory_space=pltpu.HBM)
    dma = pltpu.SemaphoreType.DMA
    out = pl.pallas_call(
        kernel,
        out_shape=pltpu.VMEM((NRHS, CB), F32),
        in_specs=[hbm] * 4,
        out_specs=pl.BlockSpec(memory_space=pltpu.VMEM),
        scratch_shapes=[
            pltpu.VMEM((NRHS, BLK), F32),
            pltpu.VMEM((1, ROWS * BLK), jnp.int32),
            pltpu.VMEM((BLK, CB), F32),
            pltpu.VMEM((CB, BLK), F32),
            pltpu.VMEM((BLK, BLK), F32),
            dma((4,)),
            pltpu.VMEM((CHIPS, 4 * G, CB), F32),
            pltpu.VMEM((COLS, 4 * G, CB), F32),
            pltpu.VMEM((ROWS, 8, BLK // 2), F32),
            pltpu.VMEM((ROWS, 8, BLK // 2), F32),
            pltpu.VMEM((2 * CB, ROWS * BLK), BF16),
            pltpu.VMEM((COLS * 2 * G, 2 * CB), BF16),
            pltpu.VMEM((COLS * 2 * G, 2 * CB), BF16),
            pltpu.VMEM((ROWS, 8, BLK // 2), F32),
            pltpu.VMEM((G, BLK), F32),
            pltpu.VMEM((G, BLK), F32),
            pltpu.VMEM((CHIPS, 8, CB), F32),
            pltpu.VMEM((COLS, CB, BLK), F32),
            pltpu.VMEM((BLK, BLK), BF16),
            pltpu.VMEM((BLK, BLK), BF16),
            pltpu.VMEM((BLK, BLK), BF16),
            pltpu.VMEM((BLK, BLK), BF16),
            dma, dma, dma, dma, dma,
            dma((ROWS,)),
            dma((ROWS,)),
            dma,
            dma((32,)),
            dma((COLS, CHUNKS)),
            dma,
            dma,
            dma((3, 2)),
            dma((4, 3, 2)),
            dma((3,)),
            dma((3,)),
        ],
        compiler_params=pltpu.CompilerParams(
            collective_id=0, has_side_effects=True, vmem_limit_bytes=55200 * 1024
        ),
    )(
        rhs,
        pivots.reshape(1, ROWS * BLK),
        factor.reshape(BLK, CB),
        diag_inv.reshape(BLK, BLK),
    )
    return out.reshape(NRHS, 1, 1, CB)


def solution(mesh):
    return jax.shard_map(
        per_device,
        mesh=mesh,
        in_specs=(P(None, ("row", "col")), P(), P("row", None, "col", None), P("row", None, None)),
        out_specs=P(None, None, "col", None),
        check_vma=False,
    )
```

```python
import functools

import jax
import jax.numpy as jnp
from jax import lax
from jax.experimental import pallas as pl
from jax.experimental.pallas import tpu as pltpu
from jax.sharding import PartitionSpec as P

MESH = pl.DeviceIdType.MESH
NX, NY = 4, 4
CHIPS = NX * NY
COLS = 2 * CHIPS
ROWS = 8
BLK = 512
CB = 128
NRHS = 64
G = NRHS // CHIPS
CHAIN, GATHER = 1, 0
BF16, F32 = jnp.bfloat16, jnp.float32
CHUNKS = 4
ROWS_C = CB // CHUNKS


def split(v):
    hi = v.astype(BF16)
    lo = (v - hi.astype(F32)).astype(BF16)
    return hi, lo


def packed(v):
    return jnp.concatenate([v[:, : BLK // 2], v[:, BLK // 2 :]], axis=0)


def unpacked(v):
    return jnp.concatenate([v[:G], v[G:]], axis=1)


def times(v, hi_ref, lo_ref):
    hi, lo = split(v)
    lhs = jnp.concatenate([hi.astype(F32), lo.astype(F32)], axis=0).astype(BF16)
    o = jnp.dot(lhs, hi_ref[...], preferred_element_type=F32)
    o = o + jnp.dot(lhs, lo_ref[...], preferred_element_type=F32)
    return o[:G] + o[G:]


def kernel(
    rhs_hbm, piv_hbm, l_hbm, d_hbm, out_ref,
    rhs_ref, piv_ref, l_in, l_ref, d_ref, in_sem, s1_part, s1_send, s1_recv, s2_send, s2_recv, e2, xhi, xlo, ybuf, acc, pbuf, orecv, lall, bhi, blo, dhi, dlo,
    s1_ssem, s1_rsem, s2_ssem, s2_rsem, y_ssem, y_rsem, o_ssem, o_rsem, g_ssem, g_rsem, b_ssem,
    part_sem, meet_sem,
):
    row = lax.axis_index("row")
    col = lax.axis_index("col")
    chip, core = col // 2, col % 2
    x, y = chip // NY, chip % NY
    is_chain = core == CHAIN
    is_gather = core == GATHER

    def chain_col(c):
        return 2 * c + CHAIN

    def remote(src, dst, ssem, rsem, dev):
        return pltpu.make_async_remote_copy(
            src_ref=src, dst_ref=dst, send_sem=ssem, recv_sem=rsem, device_id=dev, device_id_type=MESH
        )

    def at_xy(dx, dy):
        return lax.rem(x + dx, NX) * NY + lax.rem(y + dy, NY)

    around = [at_xy(1, 0), at_xy(3, 0), at_xy(0, 1), at_xy(0, 3)]
    above, below = lax.rem(row + 1, ROWS), lax.rem(row + ROWS - 1, ROWS)

    barrier = pltpu.get_barrier_semaphore()

    def greet(r, c):
        pl.semaphore_signal(barrier, inc=1, device_id=(r, c), device_id_type=MESH)

    greet(row, 2 * chip + 1 - core)
    for c in around:
        greet(row, 2 * c + GATHER)

    @pl.when(is_chain)
    def _():
        for c in around:
            greet(row, 2 * c + CHAIN)
        greet(above, col)
        greet(below, col)

    load_rhs = pltpu.make_async_copy(rhs_hbm, rhs_ref, in_sem.at[0])
    load_l = pltpu.make_async_copy(l_hbm, l_in, in_sem.at[1])
    load_piv = pltpu.make_async_copy(piv_hbm, piv_ref, in_sem.at[2])
    load_d = pltpu.make_async_copy(d_hbm, d_ref, in_sem.at[3])
    load_rhs.start()
    load_l.start()

    @pl.when(is_chain)
    def _():
        load_piv.start()
        load_d.start()

    load_rhs.wait()

    for c in range(CHIPS):
        for q in range(4):
            at = 2 * G * (q % 2) + G * (q // 2)
            s1_send[c, at : at + G, :] = rhs_ref[G * c : G * c + G, CB * q : CB * q + CB]

    load_l.wait()
    l_ref[...] = l_in[...].T

    @pl.when(is_chain)
    def _():
        pl.semaphore_wait(barrier, 1 + 4 + 2)

    @pl.when(is_gather)
    def _():
        pl.semaphore_wait(barrier, 1 + 8)

    own_live = chip < 2 * row
    partner = (row, 2 * chip + 1 - core)
    me_chain = (row, chain_col(chip))


    def flow_chip(f, du, dv):
        dx, dy = (du, dv) if f == 0 else (dv, du)
        return lax.rem(x + dx, NX) * NY + lax.rem(y + dy, NY)

    def place(f):
        return (x, y) if f == 0 else (y, x)

    def upward(f, c, du, dv=None):
        u, v = place(f)
        first = lax.rem(u - du + NX, NX)
        if dv is None:
            odd = lax.rem(first + jnp.where(row == 1, 0, c), 2) == 1
            along_x, at_x = f == 0, first
        else:
            second = lax.rem(v - dv + NY, NY)
            odd = lax.rem(second + jnp.where(row == 1, 0, first + c), 2) == 1
            along_x, at_x = f == 1, second
        if not along_x:
            return odd
        uneven = (at_x == 2) | ((at_x == 1) & ((row <= 4) | (c != 0)))
        return ((row >= 6) & odd) | ((row < 6) & uneven)

    def block_of(f, du, dv):
        c = flow_chip(f, (4 - du) % 4, (4 - dv) % 4)
        return 2 * c + f, c < 2 * row

    def push(src, block, c, ssem, dev):
        part = pl.ds(c * ROWS_C, ROWS_C)
        remote(src.at[part], lall.at[block, part], ssem, g_rsem.at[block, c], dev).start()

    def neighbour(f, du, dv, relayed=True):
        role = jnp.where(relayed, GATHER, CHAIN) if not isinstance(relayed, bool) else (GATHER if relayed else CHAIN)
        return (row, flow_chip(f, du, dv) * 2 + role)

    def spread(f, du, src, block, c, ssem):
        plus = upward(f, c, du, 0)
        push(src, block, c, ssem, neighbour(f, 0, 1, plus))
        push(src, block, c, ssem, neighbour(f, 0, 3, jnp.logical_not(plus)))
        push(src, block, c, ssem, me_chain)

    def chunk_wait(block, c):
        part = pl.ds(c * ROWS_C, ROWS_C)
        remote(lall.at[block, part], lall.at[block, part], b_ssem, g_rsem.at[block, c], me_chain).wait_recv()

    def chunks(body):
        def one(c, _):
            body(c)
            return 0

        lax.fori_loop(0, CHUNKS, one, 0)

    @pl.when(is_gather)
    def _():
        remote(s1_send, s1_part, s1_ssem, part_sem, me_chain).start()

        own_a, own_b = 2 * chip, 2 * chip + 1

        @pl.when(chip < 2 * row)
        def _():
            def first_a(c):
                push(l_ref, own_a, c, g_ssem.at[0], neighbour(0, 1, 0))
                push(l_ref, own_a, c, g_ssem.at[0], neighbour(0, 3, 0))

            def first_b(c):
                chunk_wait(own_b, c)
                push(lall.at[own_b], own_b, c, g_ssem.at[1], neighbour(1, 1, 0))
                push(lall.at[own_b], own_b, c, g_ssem.at[1], neighbour(1, 3, 0))

            chunks(first_a)
            chunks(first_b)

        def first_onward(f, c, du):
            return upward(f, c, du) if du == 1 else jnp.logical_not(upward(f, c, du))

        def second_onward(f, c, du, dv):
            return upward(f, c, du, dv) if dv == 1 else jnp.logical_not(upward(f, c, du, dv))

        def second_sem(f, du, dv):
            return 16 + 4 * du + (dv - 1) + f

        def own_second(c):
            @pl.when(chip < 2 * row)
            def _():
                spread(0, 0, l_ref, own_a, c, g_ssem.at[0])
                spread(1, 0, lall.at[own_b], own_b, c, g_ssem.at[1])

        chunks(own_second)

        def first_arrival(du, c, f):
            block, live = block_of(f, du, 0)

            @pl.when(live)
            def _():
                chunk_wait(block, c)
                if du != 2:

                    @pl.when(first_onward(f, c, du))
                    def _():
                        push(lall.at[block], block, c, g_ssem.at[4 * du + 2 + f], neighbour(f, du, 0))

        def first_spread(du, c, f):
            block, live = block_of(f, du, 0)

            @pl.when(live)
            def _():
                spread(f, du, lall.at[block], block, c, g_ssem.at[4 * du + f])

        def on_second(du, dv, c, f):
            block, live = block_of(f, du, dv)
            at = second_sem(f, du, dv)

            @pl.when(live & second_onward(f, c, du, dv))
            def _():
                chunk_wait(block, c)
                push(lall.at[block], block, c, g_ssem.at[at], neighbour(f, 0, dv, False))
                push(lall.at[block], block, c, g_ssem.at[at], me_chain)

        def first_both(c):
            for f in (0, 1):
                first_arrival(1, c, f)
                first_arrival(3, c, f)
            for f in (0, 1):
                first_spread(1, c, f)
                first_spread(3, c, f)

        def second_of(*dus):
            def body(c):
                for f in (0, 1):
                    for du in dus:
                        on_second(du, 1, c, f)
                        on_second(du, 3, c, f)

            return body

        def first_far(c):
            for f in (0, 1):
                first_arrival(2, c, f)
                first_spread(2, c, f)

        chunks(first_both)
        chunks(second_of(0))
        chunks(first_far)
        chunks(second_of(1, 3))
        chunks(second_of(2))

        def sent(n, ssem):
            remote(lall.at[pl.ds(0, n)], lall.at[pl.ds(0, n)], ssem, o_rsem, me_chain).wait_send()

        def some_sent(live, onward, n, ssem):
            count = sum(onward(c).astype(jnp.int32) for c in range(CHUNKS))
            for k in range(1, CHUNKS + 1):

                @pl.when(live & (count == k))
                def _():
                    ref = lall.at[pl.ds(0, n), pl.ds(0, k * ROWS_C)]
                    remote(ref, ref, ssem, o_rsem, me_chain).wait_send()

        for f in (0, 1):

            @pl.when(chip < 2 * row)
            def _():
                sent(5, g_ssem.at[f])

            for du in (1, 2, 3):
                block, live = block_of(f, du, 0)

                @pl.when(live)
                def _():
                    sent(3, g_ssem.at[4 * du + f])

                if du != 2:
                    some_sent(live, lambda c: first_onward(f, c, du), 1, g_ssem.at[4 * du + 2 + f])

            for du in range(4):
                for dv in (1, 3):
                    live = block_of(f, du, dv)[1]
                    some_sent(live, lambda c: second_onward(f, c, du, dv), 2, g_ssem.at[second_sem(f, du, dv)])

    @pl.when(is_gather)
    def _():
        remote(s1_send, s1_send, s1_ssem, s1_rsem, me_chain).wait_send()
        remote(orecv, orecv, b_ssem, o_rsem, me_chain).wait_recv()

    @pl.when(is_chain)
    def _():
        def tell(k, a, b):
            for dev in (a, b):
                pl.semaphore_signal(meet_sem.at[k], inc=1, device_id=dev, device_id_type=MESH)

        def hear(k):
            pl.semaphore_wait(meet_sem.at[k], 2)

        x_sides = [(row, chain_col(c)) for c in around[:2]]
        y_sides = [(row, chain_col(c)) for c in around[2:]]
        z_sides = [(above, col), (below, col)]

        tell(0, *x_sides)
        tell(3, *z_sides)

        @pl.when(own_live)
        def _():
            chunks(lambda c: push(l_ref, 2 * chip + CHAIN, c, b_ssem, partner))

        hear(0)
        tell(1, *y_sides)
        hear(1)
        tell(2, *y_sides)
        hear(2)

        remote(s1_part, s1_part, b_ssem, part_sem, partner).wait_recv()

        def send_s1(i, _):
            c = lax.rem(chip + i, CHIPS)
            remote(s1_send.at[c], s1_recv.at[col], s1_ssem, s1_rsem, (row, chain_col(c))).start()
            remote(s1_part.at[c], s1_recv.at[2 * chip + GATHER], s1_ssem, s1_rsem, (row, chain_col(c))).start()
            return 0

        lax.fori_loop(1, CHIPS, send_s1, 0)
        s1_recv[col] = s1_send[chip]
        s1_recv[2 * chip + GATHER] = s1_part[chip]
        hear(3)
        tell(4, *z_sides)
        load_d.wait()
        load_piv.wait()

        d = d_ref[...].T
        hi, lo = split(d)
        dhi[...] = hi
        dlo[...] = lo

        hear(4)
        tell(5, *z_sides)

        width = COLS * BLK
        piv = piv_ref[...] - row * width
        low = jnp.broadcast_to(piv & (2 * CB - 1), (2 * CB, ROWS * BLK))
        e2[...] = (lax.broadcasted_iota(jnp.int32, (2 * CB, ROWS * BLK), 0) == low).astype(F32).astype(BF16)

        hear(5)
        others = s1_recv.at[pl.ds(0, COLS - 2)]
        remote(others, others, b_ssem, s1_rsem, partner).wait_recv()
        for h in range(2):
            v = s1_recv[:, 2 * G * h : 2 * G * h + 2 * G, :].reshape(COLS * 2 * G, CB)
            hi, lo = split(v)
            xhi[:, CB * h : CB * h + CB] = hi
            xlo[:, CB * h : CB * h + CB] = lo

        def select(j, _):
            off = pl.multiple_of(j * BLK, BLK)
            e = e2[:, pl.ds(off, BLK)]
            t = jnp.dot(xhi[...], e, preferred_element_type=F32)
            t = t + jnp.dot(xlo[...], e, preferred_element_type=F32)
            high = jnp.right_shift(piv_ref[:, pl.ds(off, BLK)] - row * width, 8)
            rows_hi = jnp.right_shift(lax.broadcasted_iota(jnp.int32, (COLS * 2 * G, BLK), 0), 2)
            t = jnp.where(rows_hi == jnp.broadcast_to(high, rows_hi.shape), t, 0.0)
            t = jnp.sum(t.reshape(COLS, 2 * G, BLK), axis=0)
            tile = packed(t[:G] + t[G:])

            @pl.when(j == row)
            def _():
                s2_recv[row] = tile

            @pl.when(j != row)
            def _():
                s2_send[j] = tile
                remote(s2_send.at[j], s2_recv.at[row], s2_ssem, s2_rsem, (j, col)).start()

            return 0

        lax.fori_loop(0, ROWS, select, 0)
        remote(s2_recv.at[pl.ds(0, ROWS - 1)], s2_recv.at[pl.ds(0, ROWS - 1)], b_ssem, s2_rsem, partner).wait_recv()
        pbuf[...] = unpacked(jnp.sum(s2_recv[...], axis=0))
        acc[...] = jnp.zeros_like(acc)

        def finish():
            fresh = times(pbuf[...] - acc[...], dhi, dlo)
            ybuf[row] = packed(fresh)
            for i in range(1, ROWS):
                remote(ybuf.at[row], ybuf.at[row], y_ssem, y_rsem.at[row], (lax.rem(row + i, ROWS), col)).start()

        @pl.when(row == 0)
        def _():
            finish()

        def step(m, _):
            @pl.when(m < row)
            def _():
                for t in range(4):
                    chunks(lambda c: chunk_wait(4 * m + t, c))

                for t in range(4):
                    hi, lo = split(lall[4 * m + t])
                    bhi[CB * t : CB * t + CB, :] = hi
                    blo[CB * t : CB * t + CB, :] = lo

            @pl.when(m != row)
            def _():
                remote(ybuf.at[m], ybuf.at[m], b_ssem, y_rsem.at[m], partner).wait_recv()

            @pl.when(m < row)
            def _():
                acc[...] += times(unpacked(ybuf[m]), bhi, blo)

            @pl.when(m + 1 == row)
            def _():
                finish()

            for t in range(4):
                lanes = pl.ds(CB * (t % 2), CB)
                dest = 4 * m + t

                @pl.when(dest == col)
                def _():
                    orecv[chip] = ybuf[m, :, lanes]

                @pl.when(dest != col)
                def _():
                    remote(ybuf.at[m, :, lanes], orecv.at[chip], o_ssem.at[m], o_rsem, (row, dest)).start()

            return 0

        lax.fori_loop(0, ROWS, step, 0)

        @pl.when(own_live)
        def _():
            remote(l_ref, l_ref, b_ssem, o_rsem, partner).wait_send()

        remote(others, others, s1_ssem, s1_rsem, partner).wait_send()
        remote(s2_send.at[pl.ds(0, ROWS - 1)], s2_send.at[pl.ds(0, ROWS - 1)], s2_ssem, s2_rsem, partner).wait_send()
        remote(ybuf.at[pl.ds(0, ROWS - 1)], ybuf.at[pl.ds(0, ROWS - 1)], y_ssem, y_rsem.at[row], partner).wait_send()

        def drain(m, _):
            @pl.when(m == col // 4)
            def _():
                remote(orecv.at[pl.ds(0, 3)], orecv.at[pl.ds(0, 3)], o_ssem.at[m], o_rsem, partner).wait_send()

            @pl.when(m != col // 4)
            def _():
                remote(orecv.at[pl.ds(0, 4)], orecv.at[pl.ds(0, 4)], o_ssem.at[m], o_rsem, partner).wait_send()

            return 0

        lax.fori_loop(0, ROWS, drain, 0)
        remote(
            orecv.at[pl.ds(0, CHIPS - 1)], orecv.at[pl.ds(0, CHIPS - 1)], b_ssem, o_rsem, partner
        ).wait_recv()

    upper = lax.rem(chip, 2) == 0
    for c in range(CHIPS):
        tile = orecv[c]
        out_ref[G * c : G * c + G, :] = jnp.where(upper, tile[:G], tile[G:])


def per_device(rhs, pivots, factor, diag_inv):
    hbm = pl.BlockSpec(memory_space=pltpu.HBM)
    dma = pltpu.SemaphoreType.DMA
    out = pl.pallas_call(
        kernel,
        out_shape=pltpu.VMEM((NRHS, CB), F32),
        in_specs=[hbm] * 4,
        out_specs=pl.BlockSpec(memory_space=pltpu.VMEM),
        scratch_shapes=[
            pltpu.VMEM((NRHS, BLK), F32),
            pltpu.VMEM((1, ROWS * BLK), jnp.int32),
            pltpu.VMEM((BLK, CB), F32),
            pltpu.VMEM((CB, BLK), F32),
            pltpu.VMEM((BLK, BLK), F32),
            dma((4,)),
            pltpu.VMEM((CHIPS, 4 * G, CB), F32),
            pltpu.VMEM((CHIPS, 4 * G, CB), F32),
            pltpu.VMEM((COLS, 4 * G, CB), F32),
            pltpu.VMEM((ROWS, 8, BLK // 2), F32),
            pltpu.VMEM((ROWS, 8, BLK // 2), F32),
            pltpu.VMEM((2 * CB, ROWS * BLK), BF16),
            pltpu.VMEM((COLS * 2 * G, 2 * CB), BF16),
            pltpu.VMEM((COLS * 2 * G, 2 * CB), BF16),
            pltpu.VMEM((ROWS, 8, BLK // 2), F32),
            pltpu.VMEM((G, BLK), F32),
            pltpu.VMEM((G, BLK), F32),
            pltpu.VMEM((CHIPS, 8, CB), F32),
            pltpu.VMEM((COLS, CB, BLK), F32),
            pltpu.VMEM((BLK, BLK), BF16),
            pltpu.VMEM((BLK, BLK), BF16),
            pltpu.VMEM((BLK, BLK), BF16),
            pltpu.VMEM((BLK, BLK), BF16),
            dma, dma, dma, dma, dma,
            dma((ROWS,)),
            dma((ROWS,)),
            dma,
            dma((32,)),
            dma((COLS, CHUNKS)),
            dma,
            dma,
            pltpu.SemaphoreType.REGULAR((6,)),
        ],
        compiler_params=pltpu.CompilerParams(
            collective_id=0, has_side_effects=True, vmem_limit_bytes=55200 * 1024
        ),
    )(
        rhs,
        pivots.reshape(1, ROWS * BLK),
        factor.reshape(BLK, CB),
        diag_inv.reshape(BLK, BLK),
    )
    return out.reshape(NRHS, 1, 1, CB)


def solution(mesh):
    return jax.shard_map(
        per_device,
        mesh=mesh,
        in_specs=(P(None, ("row", "col")), P(), P("row", None, "col", None), P("row", None, None)),
        out_specs=P(None, None, "col", None),
        check_vma=False,
    )
```

```python
import functools

import jax
import jax.numpy as jnp
from jax import lax
from jax.experimental import pallas as pl
from jax.experimental.pallas import tpu as pltpu
from jax.sharding import PartitionSpec as P

MESH = pl.DeviceIdType.MESH
NX, NY = 4, 4
CHIPS = NX * NY
COLS = 2 * CHIPS
ROWS = 8
BLK = 512
CB = 128
NRHS = 64
G = NRHS // CHIPS
CHAIN, GATHER = 1, 0
BF16, F32 = jnp.bfloat16, jnp.float32
CHUNKS = 4
ROWS_C = CB // CHUNKS


def split(v):
    hi = v.astype(BF16)
    lo = (v - hi.astype(F32)).astype(BF16)
    return hi, lo


def packed(v):
    return jnp.concatenate([v[:, : BLK // 2], v[:, BLK // 2 :]], axis=0)


def unpacked(v):
    return jnp.concatenate([v[:G], v[G:]], axis=1)


def times(v, hi_ref, lo_ref):
    hi, lo = split(v)
    lhs = jnp.concatenate([hi.astype(F32), lo.astype(F32)], axis=0).astype(BF16)
    o = jnp.dot(lhs, hi_ref[...], preferred_element_type=F32)
    o = o + jnp.dot(lhs, lo_ref[...], preferred_element_type=F32)
    return o[:G] + o[G:]


def kernel(
    rhs_hbm, piv_hbm, l_hbm, d_hbm, out_ref,
    rhs_ref, piv_ref, l_in, l_ref, d_ref, in_sem, s1_part, s1_send, s1_recv, s2_send, s2_recv, e2, xhi, xlo, ybuf, acc, pbuf, orecv, lall, bhi, blo, dhi, dlo,
    s1_ssem, s1_rsem, s2_ssem, s2_rsem, y_ssem, y_rsem, o_ssem, o_rsem, g_ssem, g_rsem, b_ssem,
    part_sem, meet_sem,
):
    row = lax.axis_index("row")
    col = lax.axis_index("col")
    chip, core = col // 2, col % 2
    x, y = chip // NY, chip % NY
    is_chain = core == CHAIN
    is_gather = core == GATHER

    def chain_col(c):
        return 2 * c + CHAIN

    def remote(src, dst, ssem, rsem, dev):
        return pltpu.make_async_remote_copy(
            src_ref=src, dst_ref=dst, send_sem=ssem, recv_sem=rsem, device_id=dev, device_id_type=MESH
        )

    def at_xy(dx, dy):
        return lax.rem(x + dx, NX) * NY + lax.rem(y + dy, NY)

    around = [at_xy(1, 0), at_xy(3, 0), at_xy(0, 1), at_xy(0, 3)]
    x_ring = [at_xy(i, 0) for i in (1, 3, 2)]
    y_ring = [at_xy(0, i) for i in (1, 3, 2)]
    above, below = lax.rem(row + 1, ROWS), lax.rem(row + ROWS - 1, ROWS)

    barrier = pltpu.get_barrier_semaphore()

    def greet(r, c):
        pl.semaphore_signal(barrier, inc=1, device_id=(r, c), device_id_type=MESH)

    greet(row, 2 * chip + 1 - core)
    for c in around:
        greet(row, 2 * c + GATHER)

    @pl.when(is_gather)
    def _():
        for c in around:
            greet(row, chain_col(c))

    @pl.when(is_chain)
    def _():
        for c in x_ring + y_ring:
            greet(row, chain_col(c))
        greet(above, col)
        greet(below, col)

    load_rhs = pltpu.make_async_copy(rhs_hbm, rhs_ref, in_sem.at[0])
    load_l = pltpu.make_async_copy(l_hbm, l_in, in_sem.at[1])
    load_piv = pltpu.make_async_copy(piv_hbm, piv_ref, in_sem.at[2])
    load_d = pltpu.make_async_copy(d_hbm, d_ref, in_sem.at[3])
    load_rhs.start()
    load_l.start()

    @pl.when(is_chain)
    def _():
        load_piv.start()
        load_d.start()

    load_rhs.wait()

    for c in range(CHIPS):
        for q in range(4):
            at = 2 * G * (q % 2) + G * (q // 2)
            s1_send[c, at : at + G, :] = rhs_ref[G * c : G * c + G, CB * q : CB * q + CB]

    load_l.wait()
    l_ref[...] = l_in[...].T

    @pl.when(is_chain)
    def _():
        pl.semaphore_wait(barrier, 1 + 4 + 6 + 2)

    @pl.when(is_gather)
    def _():
        pl.semaphore_wait(barrier, 1 + 8)

    own_live = chip < 2 * row
    partner = (row, 2 * chip + 1 - core)
    me_chain = (row, chain_col(chip))


    def x_first(f, c):
        return True if f == 0 else (row == 2) & (c < 2)

    def either(f, c, a, b):
        return a if f == 0 else jnp.where(x_first(f, c), a, b)

    def flow_chip(f, c, du, dv):
        return at_xy(either(f, c, du, dv), either(f, c, dv, du))

    def upward(f, c, du, dv=None):
        first = lax.rem(either(f, c, x, y) - du + NX, NX)
        if dv is None:
            at = first
            odd = lax.rem(first + jnp.where(row == 1, 0, c), 2) == 1
        else:
            at = lax.rem(either(f, c, y, x) - dv + NY, NY)
            odd = lax.rem(at + jnp.where(row == 1, 0, first + c), 2) == 1
        uneven = (at == 2) | ((at == 1) & ((row <= 4) | (c != 0)))
        by_x = ((row >= 6) & odd) | ((row < 6) & uneven)
        if f == 0:
            return by_x if dv is None else odd
        along_x = x_first(f, c) if dv is None else jnp.logical_not(x_first(f, c))
        return (along_x & by_x) | (jnp.logical_not(along_x) & odd)

    def block_of(f, c, du, dv):
        a = flow_chip(f, c, (4 - du) % 4, (4 - dv) % 4)
        return 2 * a + f, a < 2 * row

    def push(src, block, c, ssem, dev):
        part = pl.ds(c * ROWS_C, ROWS_C)
        remote(src.at[part], lall.at[block, part], ssem, g_rsem.at[block, c], dev).start()

    def neighbour(f, c, du, dv, relayed=True):
        role = jnp.where(relayed, GATHER, CHAIN) if not isinstance(relayed, bool) else (GATHER if relayed else CHAIN)
        return (row, flow_chip(f, c, du, dv) * 2 + role)

    def spread(f, du, src, block, c, ssem, home=True):
        plus = upward(f, c, du, 0)
        if home:
            push(src, block, c, ssem, me_chain)
        push(src, block, c, ssem, neighbour(f, c, 0, 1, plus))
        push(src, block, c, ssem, neighbour(f, c, 0, 3, jnp.logical_not(plus)))

    def chunk_wait(block, c):
        part = pl.ds(c * ROWS_C, ROWS_C)
        remote(lall.at[block, part], lall.at[block, part], b_ssem, g_rsem.at[block, c], me_chain).wait_recv()

    def chunks(body):
        def one(c, _):
            body(c)
            return 0

        lax.fori_loop(0, CHUNKS, one, 0)

    @pl.when(is_gather)
    def _():
        remote(s1_send, s1_part, s1_ssem, part_sem, me_chain).start()

        own = 2 * chip + GATHER

        @pl.when(chip < 2 * row)
        def _():
            def first(c):
                push(l_ref, own, c, g_ssem.at[0], neighbour(0, c, 1, 0))
                push(l_ref, own, c, g_ssem.at[0], neighbour(0, c, 3, 0))

            def second(c):
                spread(0, 0, l_ref, own, c, g_ssem.at[0])
                chunk_wait(own + 1, c)
                spread(1, 0, lall.at[own + 1], own + 1, c, g_ssem.at[1], False)

            chunks(first)
            chunks(second)

        def first_onward(f, c, du):
            return upward(f, c, du) if du == 1 else jnp.logical_not(upward(f, c, du))

        def second_onward(f, c, du, dv):
            return upward(f, c, du, dv) if dv == 1 else jnp.logical_not(upward(f, c, du, dv))

        def second_sem(f, du, dv):
            return 16 + 4 * du + (dv - 1) + f

        def first_arrival(du, c, f):
            block, live = block_of(f, c, du, 0)

            @pl.when(live)
            def _():
                chunk_wait(block, c)
                if du != 2:

                    @pl.when(first_onward(f, c, du))
                    def _():
                        push(lall.at[block], block, c, g_ssem.at[4 * du + 2 + f], neighbour(f, c, du, 0))

        def first_spread(du, c, f):
            block, live = block_of(f, c, du, 0)

            @pl.when(live)
            def _():
                spread(f, du, lall.at[block], block, c, g_ssem.at[4 * du + f])

        def on_second(du, dv, c, f):
            block, live = block_of(f, c, du, dv)
            at = second_sem(f, du, dv)

            @pl.when(live & second_onward(f, c, du, dv))
            def _():
                chunk_wait(block, c)
                push(lall.at[block], block, c, g_ssem.at[at], neighbour(f, c, 0, dv, False))
                push(lall.at[block], block, c, g_ssem.at[at], me_chain)

        def first_both(c):
            for f in (0, 1):
                first_arrival(1, c, f)
                first_arrival(3, c, f)
            for f in (0, 1):
                first_spread(1, c, f)
                first_spread(3, c, f)

        def second_of(*dus):
            def body(c):
                for f in (0, 1):
                    for du in dus:
                        on_second(du, 1, c, f)
                        on_second(du, 3, c, f)

            return body

        def first_far(c):
            for f in (0, 1):
                first_arrival(2, c, f)
                first_spread(2, c, f)

        chunks(first_both)
        chunks(second_of(0))
        chunks(first_far)
        chunks(second_of(1, 3))
        chunks(second_of(2))

        def some_sent(went, n, ssem):
            count = sum(went(c).astype(jnp.int32) for c in range(CHUNKS))
            for k in range(1, CHUNKS + 1):

                @pl.when(count == k)
                def _():
                    ref = lall.at[pl.ds(0, n), pl.ds(0, k * ROWS_C)]
                    remote(ref, ref, ssem, o_rsem, me_chain).wait_send()

        def live_chunk(f, du, dv):
            return lambda c: block_of(f, c, du, dv)[1]

        for f in (0, 1):
            some_sent(lambda c: chip < 2 * row, 2 if f == CHAIN else 5, g_ssem.at[f])

            for du in (1, 2, 3):
                live = live_chunk(f, du, 0)
                some_sent(live, 3, g_ssem.at[4 * du + f])
                if du != 2:
                    some_sent(lambda c: live(c) & first_onward(f, c, du), 1, g_ssem.at[4 * du + 2 + f])

            for du in range(4):
                for dv in (1, 3):
                    live = live_chunk(f, du, dv)
                    some_sent(lambda c: live(c) & second_onward(f, c, du, dv), 2, g_ssem.at[second_sem(f, du, dv)])

    @pl.when(is_gather)
    def _():
        remote(s1_send, s1_send, s1_ssem, s1_rsem, me_chain).wait_send()
        remote(orecv, orecv, b_ssem, o_rsem, me_chain).wait_recv()

    @pl.when(is_chain)
    def _():
        def tell(k, devs):
            for dev in devs:
                pl.semaphore_signal(meet_sem.at[k], inc=1, device_id=dev, device_id_type=MESH)

        def hear(k, n):
            pl.semaphore_wait(meet_sem.at[k], n)

        z_sides = [(above, col), (below, col)]

        tell(0, [(row, chain_col(c)) for c in y_ring])
        tell(1, z_sides)

        @pl.when(own_live)
        def _():
            def first(c):
                push(l_ref, col, c, b_ssem, neighbour(1, c, 1, 0))
                push(l_ref, col, c, b_ssem, neighbour(1, c, 3, 0))
                push(l_ref, col, c, b_ssem, partner)

            chunks(first)
            lall[col] = l_ref[...]

        hear(0, 3)

        remote(s1_part, s1_part, b_ssem, part_sem, partner).wait_recv()

        def send_s1(i, _):
            c = lax.rem(chip + i, CHIPS)
            remote(s1_send.at[c], s1_recv.at[col], s1_ssem, s1_rsem, (row, chain_col(c))).start()
            remote(s1_part.at[c], s1_recv.at[2 * chip + GATHER], s1_ssem, s1_rsem, (row, chain_col(c))).start()
            return 0

        lax.fori_loop(1, CHIPS, send_s1, 0)
        s1_recv[col] = s1_send[chip]
        s1_recv[2 * chip + GATHER] = s1_part[chip]
        hear(1, 2)
        tell(2, z_sides)
        load_d.wait()
        load_piv.wait()

        d = d_ref[...].T
        hi, lo = split(d)
        dhi[...] = hi
        dlo[...] = lo

        hear(2, 2)
        tell(3, z_sides)

        width = COLS * BLK
        piv = piv_ref[...] - row * width
        low = jnp.broadcast_to(piv & (2 * CB - 1), (2 * CB, ROWS * BLK))
        e2[...] = (lax.broadcasted_iota(jnp.int32, (2 * CB, ROWS * BLK), 0) == low).astype(F32).astype(BF16)

        hear(3, 2)
        others = s1_recv.at[pl.ds(0, COLS - 2)]
        remote(others, others, b_ssem, s1_rsem, partner).wait_recv()
        for h in range(2):
            v = s1_recv[:, 2 * G * h : 2 * G * h + 2 * G, :].reshape(COLS * 2 * G, CB)
            hi, lo = split(v)
            xhi[:, CB * h : CB * h + CB] = hi
            xlo[:, CB * h : CB * h + CB] = lo

        def select(j, _):
            off = pl.multiple_of(j * BLK, BLK)
            e = e2[:, pl.ds(off, BLK)]
            t = jnp.dot(xhi[...], e, preferred_element_type=F32)
            t = t + jnp.dot(xlo[...], e, preferred_element_type=F32)
            high = jnp.right_shift(piv_ref[:, pl.ds(off, BLK)] - row * width, 8)
            rows_hi = jnp.right_shift(lax.broadcasted_iota(jnp.int32, (COLS * 2 * G, BLK), 0), 2)
            t = jnp.where(rows_hi == jnp.broadcast_to(high, rows_hi.shape), t, 0.0)
            t = jnp.sum(t.reshape(COLS, 2 * G, BLK), axis=0)
            tile = packed(t[:G] + t[G:])

            @pl.when(j == row)
            def _():
                s2_recv[row] = tile

            @pl.when(j != row)
            def _():
                s2_send[j] = tile
                remote(s2_send.at[j], s2_recv.at[row], s2_ssem, s2_rsem, (j, col)).start()

            return 0

        lax.fori_loop(0, ROWS, select, 0)
        remote(s2_recv.at[pl.ds(0, ROWS - 1)], s2_recv.at[pl.ds(0, ROWS - 1)], b_ssem, s2_rsem, partner).wait_recv()
        pbuf[...] = unpacked(jnp.sum(s2_recv[...], axis=0))
        acc[...] = jnp.zeros_like(acc)

        def finish(summed):
            fresh = times(pbuf[...] - summed, dhi, dlo)
            ybuf[row] = packed(fresh)
            for i in range(1, ROWS):
                remote(ybuf.at[row], ybuf.at[row], y_ssem, y_rsem.at[row], (lax.rem(row + i, ROWS), col)).start()

        @pl.when(row == 0)
        def _():
            finish(acc[...])

        def step(m, _):
            @pl.when(m < row)
            def _():
                for t in range(4):

                    @pl.when(4 * m + t != col)
                    def _():
                        chunks(lambda c: chunk_wait(4 * m + t, c))

                    hi, lo = split(lall[4 * m + t])
                    bhi[CB * t : CB * t + CB, :] = hi
                    blo[CB * t : CB * t + CB, :] = lo

            @pl.when(m != row)
            def _():
                remote(ybuf.at[m], ybuf.at[m], b_ssem, y_rsem.at[m], partner).wait_recv()

            @pl.when(m + 1 < row)
            def _():
                acc[...] += times(unpacked(ybuf[m]), bhi, blo)

            @pl.when(m + 1 == row)
            def _():
                finish(acc[...] + times(unpacked(ybuf[m]), bhi, blo))

            for t in range(4):
                lanes = pl.ds(CB * (t % 2), CB)
                dest = 4 * m + t

                @pl.when(dest == col)
                def _():
                    orecv[chip] = ybuf[m, :, lanes]

                @pl.when(dest != col)
                def _():
                    remote(ybuf.at[m, :, lanes], orecv.at[chip], o_ssem.at[m], o_rsem, (row, dest)).start()

            return 0

        lax.fori_loop(0, ROWS, step, 0)

        @pl.when(own_live)
        def _():
            three = lall.at[pl.ds(0, 3)]
            remote(three, three, b_ssem, o_rsem, partner).wait_send()

        remote(others, others, s1_ssem, s1_rsem, partner).wait_send()
        remote(s2_send.at[pl.ds(0, ROWS - 1)], s2_send.at[pl.ds(0, ROWS - 1)], s2_ssem, s2_rsem, partner).wait_send()
        remote(ybuf.at[pl.ds(0, ROWS - 1)], ybuf.at[pl.ds(0, ROWS - 1)], y_ssem, y_rsem.at[row], partner).wait_send()

        def drain(m, _):
            @pl.when(m == col // 4)
            def _():
                remote(orecv.at[pl.ds(0, 3)], orecv.at[pl.ds(0, 3)], o_ssem.at[m], o_rsem, partner).wait_send()

            @pl.when(m != col // 4)
            def _():
                remote(orecv.at[pl.ds(0, 4)], orecv.at[pl.ds(0, 4)], o_ssem.at[m], o_rsem, partner).wait_send()

            return 0

        lax.fori_loop(0, ROWS, drain, 0)
        remote(
            orecv.at[pl.ds(0, CHIPS - 1)], orecv.at[pl.ds(0, CHIPS - 1)], b_ssem, o_rsem, partner
        ).wait_recv()

    upper = lax.rem(chip, 2) == 0
    for c in range(CHIPS):
        tile = orecv[c]
        out_ref[G * c : G * c + G, :] = jnp.where(upper, tile[:G], tile[G:])


def per_device(rhs, pivots, factor, diag_inv):
    hbm = pl.BlockSpec(memory_space=pltpu.HBM)
    dma = pltpu.SemaphoreType.DMA
    out = pl.pallas_call(
        kernel,
        out_shape=pltpu.VMEM((NRHS, CB), F32),
        in_specs=[hbm] * 4,
        out_specs=pl.BlockSpec(memory_space=pltpu.VMEM),
        scratch_shapes=[
            pltpu.VMEM((NRHS, BLK), F32),
            pltpu.VMEM((1, ROWS * BLK), jnp.int32),
            pltpu.VMEM((BLK, CB), F32),
            pltpu.VMEM((CB, BLK), F32),
            pltpu.VMEM((BLK, BLK), F32),
            dma((4,)),
            pltpu.VMEM((CHIPS, 4 * G, CB), F32),
            pltpu.VMEM((CHIPS, 4 * G, CB), F32),
            pltpu.VMEM((COLS, 4 * G, CB), F32),
            pltpu.VMEM((ROWS, 8, BLK // 2), F32),
            pltpu.VMEM((ROWS, 8, BLK // 2), F32),
            pltpu.VMEM((2 * CB, ROWS * BLK), BF16),
            pltpu.VMEM((COLS * 2 * G, 2 * CB), BF16),
            pltpu.VMEM((COLS * 2 * G, 2 * CB), BF16),
            pltpu.VMEM((ROWS, 8, BLK // 2), F32),
            pltpu.VMEM((G, BLK), F32),
            pltpu.VMEM((G, BLK), F32),
            pltpu.VMEM((CHIPS, 8, CB), F32),
            pltpu.VMEM((COLS, CB, BLK), F32),
            pltpu.VMEM((BLK, BLK), BF16),
            pltpu.VMEM((BLK, BLK), BF16),
            pltpu.VMEM((BLK, BLK), BF16),
            pltpu.VMEM((BLK, BLK), BF16),
            dma, dma, dma, dma, dma,
            dma((ROWS,)),
            dma((ROWS,)),
            dma,
            dma((32,)),
            dma((COLS, CHUNKS)),
            dma,
            dma,
            pltpu.SemaphoreType.REGULAR((4,)),
        ],
        compiler_params=pltpu.CompilerParams(
            collective_id=0, has_side_effects=True, vmem_limit_bytes=55200 * 1024
        ),
    )(
        rhs,
        pivots.reshape(1, ROWS * BLK),
        factor.reshape(BLK, CB),
        diag_inv.reshape(BLK, BLK),
    )
    return out.reshape(NRHS, 1, 1, CB)


def solution(mesh):
    return jax.shard_map(
        per_device,
        mesh=mesh,
        in_specs=(P(None, ("row", "col")), P(), P("row", None, "col", None), P("row", None, None)),
        out_specs=P(None, None, "col", None),
        check_vma=False,
    )
```

```python
import functools

import jax
import jax.numpy as jnp
from jax import lax
from jax.experimental import pallas as pl
from jax.experimental.pallas import tpu as pltpu
from jax.sharding import PartitionSpec as P

MESH = pl.DeviceIdType.MESH
NX, NY = 4, 4
CHIPS = NX * NY
COLS = 2 * CHIPS
ROWS = 8
BLK = 512
CB = 128
NRHS = 64
G = NRHS // CHIPS
CHAIN, GATHER = 1, 0
BF16, F32 = jnp.bfloat16, jnp.float32
CHUNKS = 2
ROWS_C = CB // CHUNKS


def split(v):
    hi = v.astype(BF16)
    lo = (v - hi.astype(F32)).astype(BF16)
    return hi, lo


def packed(v):
    return jnp.concatenate([v[:, : BLK // 2], v[:, BLK // 2 :]], axis=0)


def unpacked(v):
    return jnp.concatenate([v[:G], v[G:]], axis=1)


def times(v, hi_ref, lo_ref):
    hi, lo = split(v)
    lhs = jnp.concatenate([hi.astype(F32), lo.astype(F32)], axis=0).astype(BF16)
    o = jnp.dot(lhs, hi_ref[...], preferred_element_type=F32)
    o = o + jnp.dot(lhs, lo_ref[...], preferred_element_type=F32)
    return o[:G] + o[G:]


def kernel(
    rhs_hbm, piv_hbm, l_hbm, d_hbm, out_ref,
    rhs_ref, piv_ref, l_in, l_ref, d_ref, in_sem, s1_part, s1_send, s1_recv, s2_send, s2_recv, e2, xhi, xlo, ybuf, acc, pbuf, orecv, lall, bhi, blo, dhi, dlo,
    s1_ssem, s1_rsem, s2_ssem, s2_rsem, y_ssem, y_rsem, o_ssem, o_rsem, g_ssem, g_rsem, b_ssem,
    part_sem, meet_sem,
):
    row = lax.axis_index("row")
    col = lax.axis_index("col")
    chip, core = col // 2, col % 2
    x, y = chip // NY, chip % NY
    is_chain = core == CHAIN
    is_gather = core == GATHER

    def chain_col(c):
        return 2 * c + CHAIN

    def remote(src, dst, ssem, rsem, dev):
        return pltpu.make_async_remote_copy(
            src_ref=src, dst_ref=dst, send_sem=ssem, recv_sem=rsem, device_id=dev, device_id_type=MESH
        )

    def at_xy(dx, dy):
        return lax.rem(x + dx, NX) * NY + lax.rem(y + dy, NY)

    around = [at_xy(1, 0), at_xy(3, 0), at_xy(0, 1), at_xy(0, 3)]
    x_ring = [at_xy(i, 0) for i in (1, 3, 2)]
    y_ring = [at_xy(0, i) for i in (1, 3, 2)]
    above, below = lax.rem(row + 1, ROWS), lax.rem(row + ROWS - 1, ROWS)

    barrier = pltpu.get_barrier_semaphore()

    def greet(r, c):
        pl.semaphore_signal(barrier, inc=1, device_id=(r, c), device_id_type=MESH)

    greet(row, 2 * chip + 1 - core)
    for c in around:
        greet(row, 2 * c + GATHER)

    @pl.when(is_gather)
    def _():
        for c in around:
            greet(row, chain_col(c))

    @pl.when(is_chain)
    def _():
        for c in x_ring + y_ring:
            greet(row, chain_col(c))
        greet(above, col)
        greet(below, col)

    load_rhs = pltpu.make_async_copy(rhs_hbm, rhs_ref, in_sem.at[0])
    load_l = pltpu.make_async_copy(l_hbm, l_in, in_sem.at[1])
    load_piv = pltpu.make_async_copy(piv_hbm, piv_ref, in_sem.at[2])
    load_d = pltpu.make_async_copy(d_hbm, d_ref, in_sem.at[3])
    load_rhs.start()
    load_l.start()

    @pl.when(is_chain)
    def _():
        load_piv.start()
        load_d.start()

    load_rhs.wait()

    for c in range(CHIPS):
        for q in range(4):
            at = 2 * G * (q % 2) + G * (q // 2)
            s1_send[c, at : at + G, :] = rhs_ref[G * c : G * c + G, CB * q : CB * q + CB]

    load_l.wait()
    l_ref[...] = l_in[...].T

    @pl.when(is_chain)
    def _():
        pl.semaphore_wait(barrier, 1 + 4 + 6 + 2)

    @pl.when(is_gather)
    def _():
        pl.semaphore_wait(barrier, 1 + 8)

    own_live = chip < 2 * row
    partner = (row, 2 * chip + 1 - core)
    me_chain = (row, chain_col(chip))


    def x_first(f, c):
        return True if f == 0 else (row == 2) & (c < 1)

    def either(f, c, a, b):
        return a if f == 0 else jnp.where(x_first(f, c), a, b)

    def flow_chip(f, c, du, dv):
        return at_xy(either(f, c, du, dv), either(f, c, dv, du))

    def upward(f, c, du, dv=None):
        first = lax.rem(either(f, c, x, y) - du + NX, NX)
        if dv is None:
            at = first
            odd = lax.rem(first + jnp.where(row == 1, 0, c), 2) == 1
        else:
            at = lax.rem(either(f, c, y, x) - dv + NY, NY)
            odd = lax.rem(at + jnp.where(row == 1, 0, first + c), 2) == 1
        uneven = (at == 2) | ((at == 1) & ((row <= 4) | (c != 0)))
        by_x = ((row >= 6) & odd) | ((row < 6) & uneven)
        if f == 0:
            return by_x if dv is None else odd
        along_x = x_first(f, c) if dv is None else jnp.logical_not(x_first(f, c))
        return (along_x & by_x) | (jnp.logical_not(along_x) & odd)

    def block_of(f, c, du, dv):
        a = flow_chip(f, c, (4 - du) % 4, (4 - dv) % 4)
        return 2 * a + f, a < 2 * row

    def push(src, block, c, ssem, dev):
        part = pl.ds(c * ROWS_C, ROWS_C)
        remote(src.at[part], lall.at[block, part], ssem, g_rsem.at[block, c], dev).start()

    def neighbour(f, c, du, dv, relayed=True):
        role = jnp.where(relayed, GATHER, CHAIN) if not isinstance(relayed, bool) else (GATHER if relayed else CHAIN)
        return (row, flow_chip(f, c, du, dv) * 2 + role)

    def spread(f, du, src, block, c, ssem, home=True):
        plus = upward(f, c, du, 0)
        if home:
            push(src, block, c, ssem, me_chain)
        push(src, block, c, ssem, neighbour(f, c, 0, 1, plus))
        push(src, block, c, ssem, neighbour(f, c, 0, 3, jnp.logical_not(plus)))

    def chunk_wait(block, c):
        part = pl.ds(c * ROWS_C, ROWS_C)
        remote(lall.at[block, part], lall.at[block, part], b_ssem, g_rsem.at[block, c], me_chain).wait_recv()

    def chunks(body):
        def one(c, _):
            body(c)
            return 0

        lax.fori_loop(0, CHUNKS, one, 0)

    @pl.when(is_gather)
    def _():
        remote(s1_send, s1_part, s1_ssem, part_sem, me_chain).start()

        own = 2 * chip + GATHER

        @pl.when(chip < 2 * row)
        def _():
            def first(c):
                push(l_ref, own, c, g_ssem.at[0], neighbour(0, c, 1, 0))
                push(l_ref, own, c, g_ssem.at[0], neighbour(0, c, 3, 0))

            def second(c):
                spread(0, 0, l_ref, own, c, g_ssem.at[0])
                chunk_wait(own + 1, c)
                spread(1, 0, lall.at[own + 1], own + 1, c, g_ssem.at[1], False)

            chunks(first)
            chunks(second)

        def first_onward(f, c, du):
            return upward(f, c, du) if du == 1 else jnp.logical_not(upward(f, c, du))

        def second_onward(f, c, du, dv):
            return upward(f, c, du, dv) if dv == 1 else jnp.logical_not(upward(f, c, du, dv))

        def second_sem(f, du, dv):
            return 16 + 4 * du + (dv - 1) + f

        def first_arrival(du, c, f):
            block, live = block_of(f, c, du, 0)

            @pl.when(live)
            def _():
                chunk_wait(block, c)
                if du != 2:

                    @pl.when(first_onward(f, c, du))
                    def _():
                        push(lall.at[block], block, c, g_ssem.at[4 * du + 2 + f], neighbour(f, c, du, 0))

        def first_spread(du, c, f):
            block, live = block_of(f, c, du, 0)

            @pl.when(live)
            def _():
                spread(f, du, lall.at[block], block, c, g_ssem.at[4 * du + f])

        def on_second(du, dv, c, f):
            block, live = block_of(f, c, du, dv)
            at = second_sem(f, du, dv)

            @pl.when(live & second_onward(f, c, du, dv))
            def _():
                chunk_wait(block, c)
                push(lall.at[block], block, c, g_ssem.at[at], neighbour(f, c, 0, dv, False))
                push(lall.at[block], block, c, g_ssem.at[at], me_chain)

        def first_both(c):
            for f in (0, 1):
                first_arrival(1, c, f)
                first_arrival(3, c, f)
            for f in (0, 1):
                first_spread(1, c, f)
                first_spread(3, c, f)

        def second_of(*dus):
            def body(c):
                for f in (0, 1):
                    for du in dus:
                        on_second(du, 1, c, f)
                        on_second(du, 3, c, f)

            return body

        def first_far(c):
            for f in (0, 1):
                first_arrival(2, c, f)
                first_spread(2, c, f)

        chunks(first_both)
        chunks(second_of(0))
        chunks(first_far)
        chunks(second_of(1, 3))
        chunks(second_of(2))

        def some_sent(went, n, ssem):
            count = sum(went(c).astype(jnp.int32) for c in range(CHUNKS))
            for k in range(1, CHUNKS + 1):

                @pl.when(count == k)
                def _():
                    ref = lall.at[pl.ds(0, n), pl.ds(0, k * ROWS_C)]
                    remote(ref, ref, ssem, o_rsem, me_chain).wait_send()

        def live_chunk(f, du, dv):
            return lambda c: block_of(f, c, du, dv)[1]

        for f in (0, 1):
            some_sent(lambda c: chip < 2 * row, 2 if f == CHAIN else 5, g_ssem.at[f])

            for du in (1, 2, 3):
                live = live_chunk(f, du, 0)
                some_sent(live, 3, g_ssem.at[4 * du + f])
                if du != 2:
                    some_sent(lambda c: live(c) & first_onward(f, c, du), 1, g_ssem.at[4 * du + 2 + f])

            for du in range(4):
                for dv in (1, 3):
                    live = live_chunk(f, du, dv)
                    some_sent(lambda c: live(c) & second_onward(f, c, du, dv), 2, g_ssem.at[second_sem(f, du, dv)])

    @pl.when(is_gather)
    def _():
        remote(s1_send, s1_send, s1_ssem, s1_rsem, me_chain).wait_send()
        remote(orecv, orecv, b_ssem, o_rsem, me_chain).wait_recv()

    @pl.when(is_chain)
    def _():
        def tell(k, devs):
            for dev in devs:
                pl.semaphore_signal(meet_sem.at[k], inc=1, device_id=dev, device_id_type=MESH)

        def hear(k, n):
            pl.semaphore_wait(meet_sem.at[k], n)

        z_sides = [(above, col), (below, col)]

        tell(0, [(row, chain_col(c)) for c in y_ring])
        tell(1, z_sides)

        @pl.when(own_live)
        def _():
            def first(c):
                push(l_ref, col, c, b_ssem, neighbour(1, c, 1, 0))
                push(l_ref, col, c, b_ssem, neighbour(1, c, 3, 0))
                push(l_ref, col, c, b_ssem, partner)

            chunks(first)
            lall[col] = l_ref[...]

        hear(0, 3)

        remote(s1_part, s1_part, b_ssem, part_sem, partner).wait_recv()

        def send_s1(i, _):
            c = lax.rem(chip + i, CHIPS)
            remote(s1_send.at[c], s1_recv.at[col], s1_ssem, s1_rsem, (row, chain_col(c))).start()
            remote(s1_part.at[c], s1_recv.at[2 * chip + GATHER], s1_ssem, s1_rsem, (row, chain_col(c))).start()
            return 0

        lax.fori_loop(1, CHIPS, send_s1, 0)
        s1_recv[col] = s1_send[chip]
        s1_recv[2 * chip + GATHER] = s1_part[chip]
        hear(1, 2)
        tell(2, z_sides)
        load_d.wait()
        load_piv.wait()

        d = d_ref[...].T
        hi, lo = split(d)
        dhi[...] = hi
        dlo[...] = lo

        hear(2, 2)
        tell(3, z_sides)

        width = COLS * BLK
        piv = piv_ref[...] - row * width
        low = jnp.broadcast_to(piv & (2 * CB - 1), (2 * CB, ROWS * BLK))
        e2[...] = (lax.broadcasted_iota(jnp.int32, (2 * CB, ROWS * BLK), 0) == low).astype(F32).astype(BF16)

        hear(3, 2)
        others = s1_recv.at[pl.ds(0, COLS - 2)]
        remote(others, others, b_ssem, s1_rsem, partner).wait_recv()
        for h in range(2):
            v = s1_recv[:, 2 * G * h : 2 * G * h + 2 * G, :].reshape(COLS * 2 * G, CB)
            hi, lo = split(v)
            xhi[:, CB * h : CB * h + CB] = hi
            xlo[:, CB * h : CB * h + CB] = lo

        def select(j, _):
            off = pl.multiple_of(j * BLK, BLK)
            e = e2[:, pl.ds(off, BLK)]
            t = jnp.dot(xhi[...], e, preferred_element_type=F32)
            t = t + jnp.dot(xlo[...], e, preferred_element_type=F32)
            high = jnp.right_shift(piv_ref[:, pl.ds(off, BLK)] - row * width, 8)
            rows_hi = jnp.right_shift(lax.broadcasted_iota(jnp.int32, (COLS * 2 * G, BLK), 0), 2)
            t = jnp.where(rows_hi == jnp.broadcast_to(high, rows_hi.shape), t, 0.0)
            t = jnp.sum(t.reshape(COLS, 2 * G, BLK), axis=0)
            tile = packed(t[:G] + t[G:])

            @pl.when(j == row)
            def _():
                s2_recv[row] = tile

            @pl.when(j != row)
            def _():
                s2_send[j] = tile
                remote(s2_send.at[j], s2_recv.at[row], s2_ssem, s2_rsem, (j, col)).start()

            return 0

        lax.fori_loop(0, ROWS, select, 0)
        remote(s2_recv.at[pl.ds(0, ROWS - 1)], s2_recv.at[pl.ds(0, ROWS - 1)], b_ssem, s2_rsem, partner).wait_recv()
        pbuf[...] = unpacked(jnp.sum(s2_recv[...], axis=0))
        acc[...] = jnp.zeros_like(acc)

        def finish(summed):
            fresh = times(pbuf[...] - summed, dhi, dlo)
            ybuf[row] = packed(fresh)
            for i in range(1, ROWS):
                remote(ybuf.at[row], ybuf.at[row], y_ssem, y_rsem.at[row], (lax.rem(row + i, ROWS), col)).start()

        @pl.when(row == 0)
        def _():
            finish(acc[...])

        def step(m, _):
            @pl.when(m < row)
            def _():
                for t in range(4):

                    @pl.when(4 * m + t != col)
                    def _():
                        chunks(lambda c: chunk_wait(4 * m + t, c))

                    hi, lo = split(lall[4 * m + t])
                    bhi[CB * t : CB * t + CB, :] = hi
                    blo[CB * t : CB * t + CB, :] = lo

            @pl.when(m != row)
            def _():
                remote(ybuf.at[m], ybuf.at[m], b_ssem, y_rsem.at[m], partner).wait_recv()

            @pl.when(m + 1 < row)
            def _():
                acc[...] += times(unpacked(ybuf[m]), bhi, blo)

            @pl.when(m + 1 == row)
            def _():
                finish(acc[...] + times(unpacked(ybuf[m]), bhi, blo))

            for t in range(4):
                lanes = pl.ds(CB * (t % 2), CB)
                dest = 4 * m + t

                @pl.when(dest == col)
                def _():
                    orecv[chip] = ybuf[m, :, lanes]

                @pl.when(dest != col)
                def _():
                    remote(ybuf.at[m, :, lanes], orecv.at[chip], o_ssem.at[m], o_rsem, (row, dest)).start()

            return 0

        lax.fori_loop(0, ROWS, step, 0)

        @pl.when(own_live)
        def _():
            three = lall.at[pl.ds(0, 3)]
            remote(three, three, b_ssem, o_rsem, partner).wait_send()

        remote(others, others, s1_ssem, s1_rsem, partner).wait_send()
        remote(s2_send.at[pl.ds(0, ROWS - 1)], s2_send.at[pl.ds(0, ROWS - 1)], s2_ssem, s2_rsem, partner).wait_send()
        remote(ybuf.at[pl.ds(0, ROWS - 1)], ybuf.at[pl.ds(0, ROWS - 1)], y_ssem, y_rsem.at[row], partner).wait_send()

        def drain(m, _):
            @pl.when(m == col // 4)
            def _():
                remote(orecv.at[pl.ds(0, 3)], orecv.at[pl.ds(0, 3)], o_ssem.at[m], o_rsem, partner).wait_send()

            @pl.when(m != col // 4)
            def _():
                remote(orecv.at[pl.ds(0, 4)], orecv.at[pl.ds(0, 4)], o_ssem.at[m], o_rsem, partner).wait_send()

            return 0

        lax.fori_loop(0, ROWS, drain, 0)
        remote(
            orecv.at[pl.ds(0, CHIPS - 1)], orecv.at[pl.ds(0, CHIPS - 1)], b_ssem, o_rsem, partner
        ).wait_recv()

    upper = lax.rem(chip, 2) == 0
    for c in range(CHIPS):
        tile = orecv[c]
        out_ref[G * c : G * c + G, :] = jnp.where(upper, tile[:G], tile[G:])


def per_device(rhs, pivots, factor, diag_inv):
    hbm = pl.BlockSpec(memory_space=pltpu.HBM)
    dma = pltpu.SemaphoreType.DMA
    out = pl.pallas_call(
        kernel,
        out_shape=pltpu.VMEM((NRHS, CB), F32),
        in_specs=[hbm] * 4,
        out_specs=pl.BlockSpec(memory_space=pltpu.VMEM),
        scratch_shapes=[
            pltpu.VMEM((NRHS, BLK), F32),
            pltpu.VMEM((1, ROWS * BLK), jnp.int32),
            pltpu.VMEM((BLK, CB), F32),
            pltpu.VMEM((CB, BLK), F32),
            pltpu.VMEM((BLK, BLK), F32),
            dma((4,)),
            pltpu.VMEM((CHIPS, 4 * G, CB), F32),
            pltpu.VMEM((CHIPS, 4 * G, CB), F32),
            pltpu.VMEM((COLS, 4 * G, CB), F32),
            pltpu.VMEM((ROWS, 8, BLK // 2), F32),
            pltpu.VMEM((ROWS, 8, BLK // 2), F32),
            pltpu.VMEM((2 * CB, ROWS * BLK), BF16),
            pltpu.VMEM((COLS * 2 * G, 2 * CB), BF16),
            pltpu.VMEM((COLS * 2 * G, 2 * CB), BF16),
            pltpu.VMEM((ROWS, 8, BLK // 2), F32),
            pltpu.VMEM((G, BLK), F32),
            pltpu.VMEM((G, BLK), F32),
            pltpu.VMEM((CHIPS, 8, CB), F32),
            pltpu.VMEM((COLS, CB, BLK), F32),
            pltpu.VMEM((BLK, BLK), BF16),
            pltpu.VMEM((BLK, BLK), BF16),
            pltpu.VMEM((BLK, BLK), BF16),
            pltpu.VMEM((BLK, BLK), BF16),
            dma, dma, dma, dma, dma,
            dma((ROWS,)),
            dma((ROWS,)),
            dma,
            dma((32,)),
            dma((COLS, CHUNKS)),
            dma,
            dma,
            pltpu.SemaphoreType.REGULAR((4,)),
        ],
        compiler_params=pltpu.CompilerParams(
            collective_id=0, has_side_effects=True, vmem_limit_bytes=55200 * 1024
        ),
    )(
        rhs,
        pivots.reshape(1, ROWS * BLK),
        factor.reshape(BLK, CB),
        diag_inv.reshape(BLK, BLK),
    )
    return out.reshape(NRHS, 1, 1, CB)


def solution(mesh):
    return jax.shard_map(
        per_device,
        mesh=mesh,
        in_specs=(P(None, ("row", "col")), P(), P("row", None, "col", None), P("row", None, None)),
        out_specs=P(None, None, "col", None),
        check_vma=False,
    )
```

```python
import functools

import jax
import jax.numpy as jnp
from jax import lax
from jax.experimental import pallas as pl
from jax.experimental.pallas import tpu as pltpu
from jax.sharding import PartitionSpec as P

MESH = pl.DeviceIdType.MESH
NX, NY = 4, 4
CHIPS = NX * NY
COLS = 2 * CHIPS
ROWS = 8
BLK = 512
CB = 128
NRHS = 64
G = NRHS // CHIPS
CHAIN, GATHER = 1, 0
BF16, F32 = jnp.bfloat16, jnp.float32
CHUNKS = 2
ROWS_C = CB // CHUNKS


def split(v):
    hi = v.astype(BF16)
    lo = (v - hi.astype(F32)).astype(BF16)
    return hi, lo


def packed(v):
    return jnp.concatenate([v[:, : BLK // 2], v[:, BLK // 2 :]], axis=0)


def unpacked(v):
    return jnp.concatenate([v[:G], v[G:]], axis=1)


def times(v, hi_ref, lo_ref):
    hi, lo = split(v)
    lhs = jnp.concatenate([hi.astype(F32), lo.astype(F32)], axis=0).astype(BF16)
    o = jnp.dot(lhs, hi_ref[...], preferred_element_type=F32)
    o = o + jnp.dot(lhs, lo_ref[...], preferred_element_type=F32)
    return o[:G] + o[G:]


def kernel(
    rhs_hbm, piv_hbm, l_hbm, d_hbm, out_ref,
    rhs_ref, piv_ref, l_in, l_ref, d_ref, in_sem, s1_part, s1_send, s1_recv, s2_send, s2_recv, e2, xhi, xlo, ybuf, acc, pbuf, orecv, lall, bhi, blo, dhi, dlo,
    s1_ssem, s1_rsem, s2_ssem, s2_rsem, y_ssem, y_rsem, o_ssem, o_rsem, g_ssem, g_rsem, b_ssem,
    part_sem, meet_sem,
):
    row = lax.axis_index("row")
    col = lax.axis_index("col")
    chip, core = col // 2, col % 2
    x, y = chip // NY, chip % NY
    is_chain = core == CHAIN
    is_gather = core == GATHER

    def chain_col(c):
        return 2 * c + CHAIN

    def remote(src, dst, ssem, rsem, dev):
        return pltpu.make_async_remote_copy(
            src_ref=src, dst_ref=dst, send_sem=ssem, recv_sem=rsem, device_id=dev, device_id_type=MESH
        )

    def at_xy(dx, dy):
        return lax.rem(x + dx, NX) * NY + lax.rem(y + dy, NY)

    around = [at_xy(1, 0), at_xy(3, 0), at_xy(0, 1), at_xy(0, 3)]
    x_ring = [at_xy(i, 0) for i in (1, 3, 2)]
    y_ring = [at_xy(0, i) for i in (1, 3, 2)]
    above, below = lax.rem(row + 1, ROWS), lax.rem(row + ROWS - 1, ROWS)

    barrier = pltpu.get_barrier_semaphore()

    def greet(r, c):
        pl.semaphore_signal(barrier, inc=1, device_id=(r, c), device_id_type=MESH)

    greet(row, 2 * chip + 1 - core)
    for c in around:
        greet(row, 2 * c + GATHER)

    @pl.when(is_gather)
    def _():
        for c in around:
            greet(row, chain_col(c))

    @pl.when(is_chain)
    def _():
        for c in x_ring + y_ring:
            greet(row, chain_col(c))
        greet(above, col)
        greet(below, col)

    load_rhs = pltpu.make_async_copy(rhs_hbm, rhs_ref, in_sem.at[0])
    load_l = pltpu.make_async_copy(l_hbm, l_in, in_sem.at[1])
    load_piv = pltpu.make_async_copy(piv_hbm, piv_ref, in_sem.at[2])
    load_d = pltpu.make_async_copy(d_hbm, d_ref, in_sem.at[3])
    load_rhs.start()
    load_l.start()

    @pl.when(is_chain)
    def _():
        load_piv.start()
        load_d.start()

    load_rhs.wait()

    for c in range(CHIPS):
        for q in range(4):
            at = 2 * G * (q % 2) + G * (q // 2)
            s1_send[c, at : at + G, :] = rhs_ref[G * c : G * c + G, CB * q : CB * q + CB]

    load_l.wait()
    l_ref[...] = l_in[...].T

    @pl.when(is_chain)
    def _():
        pl.semaphore_wait(barrier, 1 + 4 + 6 + 2)

    @pl.when(is_gather)
    def _():
        pl.semaphore_wait(barrier, 1 + 8)

    own_live = chip < 2 * row
    partner = (row, 2 * chip + 1 - core)
    me_chain = (row, chain_col(chip))


    def x_first(f, c):
        return True if f == 0 else ((row == 2) | (row == 3)) & (c < 1)

    def either(f, c, a, b):
        return a if f == 0 else jnp.where(x_first(f, c), a, b)

    def flow_chip(f, c, du, dv):
        return at_xy(either(f, c, du, dv), either(f, c, dv, du))

    def upward(f, c, du, dv=None):
        first = lax.rem(either(f, c, x, y) - du + NX, NX)
        if dv is None:
            at = first
            odd = lax.rem(first + jnp.where(row == 1, 0, c), 2) == 1
        else:
            at = lax.rem(either(f, c, y, x) - dv + NY, NY)
            odd = lax.rem(at + jnp.where(row == 1, 0, first + c), 2) == 1
        uneven = (at == 2) | ((at == 1) & ((row <= 4) | (c != 0)))
        by_x = ((row >= 6) & odd) | ((row < 6) & uneven)
        if f == 0:
            return by_x if dv is None else odd
        along_x = x_first(f, c) if dv is None else jnp.logical_not(x_first(f, c))
        return (along_x & by_x) | (jnp.logical_not(along_x) & odd)

    def block_of(f, c, du, dv):
        a = flow_chip(f, c, (4 - du) % 4, (4 - dv) % 4)
        return 2 * a + f, a < 2 * row

    def push(src, block, c, ssem, dev):
        part = pl.ds(c * ROWS_C, ROWS_C)
        remote(src.at[part], lall.at[block, part], ssem, g_rsem.at[block, c], dev).start()

    def neighbour(f, c, du, dv, relayed=True):
        role = jnp.where(relayed, GATHER, CHAIN) if not isinstance(relayed, bool) else (GATHER if relayed else CHAIN)
        return (row, flow_chip(f, c, du, dv) * 2 + role)

    def spread(f, du, src, block, c, ssem, home=True):
        plus = upward(f, c, du, 0)
        if home:
            push(src, block, c, ssem, me_chain)
        push(src, block, c, ssem, neighbour(f, c, 0, 1, plus))
        push(src, block, c, ssem, neighbour(f, c, 0, 3, jnp.logical_not(plus)))

    def chunk_wait(block, c):
        part = pl.ds(c * ROWS_C, ROWS_C)
        remote(lall.at[block, part], lall.at[block, part], b_ssem, g_rsem.at[block, c], me_chain).wait_recv()

    def chunks(body):
        def one(c, _):
            body(c)
            return 0

        lax.fori_loop(0, CHUNKS, one, 0)

    @pl.when(is_gather)
    def _():
        remote(s1_send, s1_part, s1_ssem, part_sem, me_chain).start()

        own = 2 * chip + GATHER

        @pl.when(chip < 2 * row)
        def _():
            def first(c):
                push(l_ref, own, c, g_ssem.at[0], neighbour(0, c, 1, 0))
                push(l_ref, own, c, g_ssem.at[0], neighbour(0, c, 3, 0))

            def second(c):
                spread(0, 0, l_ref, own, c, g_ssem.at[0])
                chunk_wait(own + 1, c)
                spread(1, 0, lall.at[own + 1], own + 1, c, g_ssem.at[1], False)

            chunks(first)
            chunks(second)

        def first_onward(f, c, du):
            return upward(f, c, du) if du == 1 else jnp.logical_not(upward(f, c, du))

        def second_onward(f, c, du, dv):
            return upward(f, c, du, dv) if dv == 1 else jnp.logical_not(upward(f, c, du, dv))

        def second_sem(f, du, dv):
            return 16 + 4 * du + (dv - 1) + f

        def first_arrival(du, c, f):
            block, live = block_of(f, c, du, 0)

            @pl.when(live)
            def _():
                chunk_wait(block, c)
                if du != 2:

                    @pl.when(first_onward(f, c, du))
                    def _():
                        push(lall.at[block], block, c, g_ssem.at[4 * du + 2 + f], neighbour(f, c, du, 0))

        def first_spread(du, c, f):
            block, live = block_of(f, c, du, 0)

            @pl.when(live)
            def _():
                spread(f, du, lall.at[block], block, c, g_ssem.at[4 * du + f])

        def on_second(du, dv, c, f):
            block, live = block_of(f, c, du, dv)
            at = second_sem(f, du, dv)

            @pl.when(live & second_onward(f, c, du, dv))
            def _():
                chunk_wait(block, c)
                push(lall.at[block], block, c, g_ssem.at[at], neighbour(f, c, 0, dv, False))
                push(lall.at[block], block, c, g_ssem.at[at], me_chain)

        def first_both(c):
            for f in (0, 1):
                first_arrival(1, c, f)
                first_arrival(3, c, f)
            for f in (0, 1):
                first_spread(1, c, f)
                first_spread(3, c, f)

        def second_of(*dus):
            def body(c):
                for f in (0, 1):
                    for du in dus:
                        on_second(du, 1, c, f)
                        on_second(du, 3, c, f)

            return body

        def first_far(c):
            for f in (0, 1):
                first_arrival(2, c, f)
                first_spread(2, c, f)

        chunks(first_both)
        chunks(second_of(0))
        chunks(first_far)
        chunks(second_of(1, 3))
        chunks(second_of(2))

        def some_sent(went, n, ssem):
            count = sum(went(c).astype(jnp.int32) for c in range(CHUNKS))
            for k in range(1, CHUNKS + 1):

                @pl.when(count == k)
                def _():
                    ref = lall.at[pl.ds(0, n), pl.ds(0, k * ROWS_C)]
                    remote(ref, ref, ssem, o_rsem, me_chain).wait_send()

        def live_chunk(f, du, dv):
            return lambda c: block_of(f, c, du, dv)[1]

        for f in (0, 1):
            some_sent(lambda c: chip < 2 * row, 2 if f == CHAIN else 5, g_ssem.at[f])

            for du in (1, 2, 3):
                live = live_chunk(f, du, 0)
                some_sent(live, 3, g_ssem.at[4 * du + f])
                if du != 2:
                    some_sent(lambda c: live(c) & first_onward(f, c, du), 1, g_ssem.at[4 * du + 2 + f])

            for du in range(4):
                for dv in (1, 3):
                    live = live_chunk(f, du, dv)
                    some_sent(lambda c: live(c) & second_onward(f, c, du, dv), 2, g_ssem.at[second_sem(f, du, dv)])

    @pl.when(is_gather)
    def _():
        remote(s1_send, s1_send, s1_ssem, s1_rsem, me_chain).wait_send()
        remote(orecv, orecv, b_ssem, o_rsem, me_chain).wait_recv()

    @pl.when(is_chain)
    def _():
        def tell(k, devs):
            for dev in devs:
                pl.semaphore_signal(meet_sem.at[k], inc=1, device_id=dev, device_id_type=MESH)

        def hear(k, n):
            pl.semaphore_wait(meet_sem.at[k], n)

        z_sides = [(above, col), (below, col)]

        tell(0, [(row, chain_col(c)) for c in y_ring])
        tell(1, z_sides)

        @pl.when(own_live)
        def _():
            def first(c):
                push(l_ref, col, c, b_ssem, neighbour(1, c, 1, 0))
                push(l_ref, col, c, b_ssem, neighbour(1, c, 3, 0))
                push(l_ref, col, c, b_ssem, partner)

            chunks(first)
            lall[col] = l_ref[...]

        hear(0, 3)

        remote(s1_part, s1_part, b_ssem, part_sem, partner).wait_recv()

        def send_s1(i, _):
            c = lax.rem(chip + i, CHIPS)
            remote(s1_send.at[c], s1_recv.at[col], s1_ssem, s1_rsem, (row, chain_col(c))).start()
            remote(s1_part.at[c], s1_recv.at[2 * chip + GATHER], s1_ssem, s1_rsem, (row, chain_col(c))).start()
            return 0

        lax.fori_loop(1, CHIPS, send_s1, 0)
        s1_recv[col] = s1_send[chip]
        s1_recv[2 * chip + GATHER] = s1_part[chip]
        hear(1, 2)
        tell(2, z_sides)
        load_d.wait()
        load_piv.wait()

        d = d_ref[...].T
        hi, lo = split(d)
        dhi[...] = hi
        dlo[...] = lo

        hear(2, 2)
        tell(3, z_sides)

        width = COLS * BLK
        piv = piv_ref[...] - row * width
        low = jnp.broadcast_to(piv & (2 * CB - 1), (2 * CB, ROWS * BLK))
        e2[...] = (lax.broadcasted_iota(jnp.int32, (2 * CB, ROWS * BLK), 0) == low).astype(F32).astype(BF16)

        hear(3, 2)
        others = s1_recv.at[pl.ds(0, COLS - 2)]
        remote(others, others, b_ssem, s1_rsem, partner).wait_recv()
        for h in range(2):
            v = s1_recv[:, 2 * G * h : 2 * G * h + 2 * G, :].reshape(COLS * 2 * G, CB)
            hi, lo = split(v)
            xhi[:, CB * h : CB * h + CB] = hi
            xlo[:, CB * h : CB * h + CB] = lo

        def select(j, _):
            off = pl.multiple_of(j * BLK, BLK)
            e = e2[:, pl.ds(off, BLK)]
            t = jnp.dot(xhi[...], e, preferred_element_type=F32)
            t = t + jnp.dot(xlo[...], e, preferred_element_type=F32)
            high = jnp.right_shift(piv_ref[:, pl.ds(off, BLK)] - row * width, 8)
            rows_hi = jnp.right_shift(lax.broadcasted_iota(jnp.int32, (COLS * 2 * G, BLK), 0), 2)
            t = jnp.where(rows_hi == jnp.broadcast_to(high, rows_hi.shape), t, 0.0)
            t = jnp.sum(t.reshape(COLS, 2 * G, BLK), axis=0)
            tile = packed(t[:G] + t[G:])

            @pl.when(j == row)
            def _():
                s2_recv[row] = tile

            @pl.when(j != row)
            def _():
                s2_send[j] = tile
                remote(s2_send.at[j], s2_recv.at[row], s2_ssem, s2_rsem, (j, col)).start()

            return 0

        lax.fori_loop(0, ROWS, select, 0)
        remote(s2_recv.at[pl.ds(0, ROWS - 1)], s2_recv.at[pl.ds(0, ROWS - 1)], b_ssem, s2_rsem, partner).wait_recv()
        pbuf[...] = unpacked(jnp.sum(s2_recv[...], axis=0))
        acc[...] = jnp.zeros_like(acc)

        def finish(summed):
            fresh = times(pbuf[...] - summed, dhi, dlo)
            ybuf[row] = packed(fresh)
            for i in range(1, ROWS):
                remote(ybuf.at[row], ybuf.at[row], y_ssem, y_rsem.at[row], (lax.rem(row + i, ROWS), col)).start()

        @pl.when(row == 0)
        def _():
            finish(acc[...])

        def step(m, _):
            @pl.when(m < row)
            def _():
                for t in range(4):

                    @pl.when(4 * m + t != col)
                    def _():
                        chunks(lambda c: chunk_wait(4 * m + t, c))

                    hi, lo = split(lall[4 * m + t])
                    bhi[CB * t : CB * t + CB, :] = hi
                    blo[CB * t : CB * t + CB, :] = lo

            @pl.when(m != row)
            def _():
                remote(ybuf.at[m], ybuf.at[m], b_ssem, y_rsem.at[m], partner).wait_recv()

            @pl.when(m + 1 < row)
            def _():
                acc[...] += times(unpacked(ybuf[m]), bhi, blo)

            @pl.when(m + 1 == row)
            def _():
                finish(acc[...] + times(unpacked(ybuf[m]), bhi, blo))

            for t in range(4):
                lanes = pl.ds(CB * (t % 2), CB)
                dest = 4 * m + t

                @pl.when(dest == col)
                def _():
                    orecv[chip] = ybuf[m, :, lanes]

                @pl.when(dest != col)
                def _():
                    remote(ybuf.at[m, :, lanes], orecv.at[chip], o_ssem.at[m], o_rsem, (row, dest)).start()

            return 0

        lax.fori_loop(0, ROWS, step, 0)

        @pl.when(own_live)
        def _():
            three = lall.at[pl.ds(0, 3)]
            remote(three, three, b_ssem, o_rsem, partner).wait_send()

        remote(others, others, s1_ssem, s1_rsem, partner).wait_send()
        remote(s2_send.at[pl.ds(0, ROWS - 1)], s2_send.at[pl.ds(0, ROWS - 1)], s2_ssem, s2_rsem, partner).wait_send()
        remote(ybuf.at[pl.ds(0, ROWS - 1)], ybuf.at[pl.ds(0, ROWS - 1)], y_ssem, y_rsem.at[row], partner).wait_send()

        def drain(m, _):
            @pl.when(m == col // 4)
            def _():
                remote(orecv.at[pl.ds(0, 3)], orecv.at[pl.ds(0, 3)], o_ssem.at[m], o_rsem, partner).wait_send()

            @pl.when(m != col // 4)
            def _():
                remote(orecv.at[pl.ds(0, 4)], orecv.at[pl.ds(0, 4)], o_ssem.at[m], o_rsem, partner).wait_send()

            return 0

        lax.fori_loop(0, ROWS, drain, 0)
        remote(
            orecv.at[pl.ds(0, CHIPS - 1)], orecv.at[pl.ds(0, CHIPS - 1)], b_ssem, o_rsem, partner
        ).wait_recv()

    upper = lax.rem(chip, 2) == 0
    for c in range(CHIPS):
        tile = orecv[c]
        out_ref[G * c : G * c + G, :] = jnp.where(upper, tile[:G], tile[G:])


def per_device(rhs, pivots, factor, diag_inv):
    hbm = pl.BlockSpec(memory_space=pltpu.HBM)
    dma = pltpu.SemaphoreType.DMA
    out = pl.pallas_call(
        kernel,
        out_shape=pltpu.VMEM((NRHS, CB), F32),
        in_specs=[hbm] * 4,
        out_specs=pl.BlockSpec(memory_space=pltpu.VMEM),
        scratch_shapes=[
            pltpu.VMEM((NRHS, BLK), F32),
            pltpu.VMEM((1, ROWS * BLK), jnp.int32),
            pltpu.VMEM((BLK, CB), F32),
            pltpu.VMEM((CB, BLK), F32),
            pltpu.VMEM((BLK, BLK), F32),
            dma((4,)),
            pltpu.VMEM((CHIPS, 4 * G, CB), F32),
            pltpu.VMEM((CHIPS, 4 * G, CB), F32),
            pltpu.VMEM((COLS, 4 * G, CB), F32),
            pltpu.VMEM((ROWS, 8, BLK // 2), F32),
            pltpu.VMEM((ROWS, 8, BLK // 2), F32),
            pltpu.VMEM((2 * CB, ROWS * BLK), BF16),
            pltpu.VMEM((COLS * 2 * G, 2 * CB), BF16),
            pltpu.VMEM((COLS * 2 * G, 2 * CB), BF16),
            pltpu.VMEM((ROWS, 8, BLK // 2), F32),
            pltpu.VMEM((G, BLK), F32),
            pltpu.VMEM((G, BLK), F32),
            pltpu.VMEM((CHIPS, 8, CB), F32),
            pltpu.VMEM((COLS, CB, BLK), F32),
            pltpu.VMEM((BLK, BLK), BF16),
            pltpu.VMEM((BLK, BLK), BF16),
            pltpu.VMEM((BLK, BLK), BF16),
            pltpu.VMEM((BLK, BLK), BF16),
            dma, dma, dma, dma, dma,
            dma((ROWS,)),
            dma((ROWS,)),
            dma,
            dma((32,)),
            dma((COLS, CHUNKS)),
            dma,
            dma,
            pltpu.SemaphoreType.REGULAR((4,)),
        ],
        compiler_params=pltpu.CompilerParams(
            collective_id=0, has_side_effects=True, vmem_limit_bytes=55200 * 1024
        ),
    )(
        rhs,
        pivots.reshape(1, ROWS * BLK),
        factor.reshape(BLK, CB),
        diag_inv.reshape(BLK, BLK),
    )
    return out.reshape(NRHS, 1, 1, CB)


def solution(mesh):
    return jax.shard_map(
        per_device,
        mesh=mesh,
        in_specs=(P(None, ("row", "col")), P(), P("row", None, "col", None), P("row", None, None)),
        out_specs=P(None, None, "col", None),
        check_vma=False,
    )
```
